256 devices in a mesh: dom: 64 (over x, z, core), rep: 4 (over y).
Axes of the slice: x: 4, y: 4, z: 8, core: 2. Of those that a mesh axis runs over, the one named last changes fastest.
Arguments:
- features: bfloat16 [524288, 128], P('dom'), may hold values from -6 to 6
- partition_map: int32 [524288], replicated, may hold values from 0 to 524287, as said below
- seed_ids: int32 [16384], P(('dom', 'rep')), may hold values from 0 to 524287, as said below
- hop1_ids: int32 [16384, 15], P(('dom', 'rep')), may hold values from 0 to 524287, as said below
- hop2_ids: int32 [16384, 15, 10], P(('dom', 'rep')), may hold values from 0 to 524287, as said below
- labels: int32 [16384], P(('dom', 'rep')), may hold values from 0 to 171
- self_one: bfloat16 [128, 256], replicated, may hold values from -0.5 to 0.5
- neigh_one: bfloat16 [128, 256], replicated, may hold values from -0.5 to 0.5
- bias_one: float32 [256], replicated, may hold values from -3 to 3
- self_two: bfloat16 [256, 172], replicated, may hold values from -0.375 to 0.375
- neigh_two: bfloat16 [256, 172], replicated, may hold values from -0.375 to 0.375
- bias_two: float32 [172], replicated, may hold values from -2 to 112, as said below
Outputs:
- seed_loss: float32 [16384], P(('dom', 'rep'))
- grad_self_one: float32 [128, 256], replicated
- grad_neigh_one: float32 [128, 256], replicated
- grad_bias_one: float32 [256], replicated
- grad_self_two: float32 [256, 172], replicated
- grad_neigh_two: float32 [256, 172], replicated
- grad_bias_two: float32 [172], replicated
The draws below stay inside these ranges and needn't reach their ends.
Inputs may be any that keep to these rules, and one draw needn't show every extreme that they name: A permutation of 0 to 524287: node v is stored at position p = partition_map[v], in partition p // 8192, row p % 8192. Rows below 256 of each partition hold hub nodes. `seed_ids`: node ids. `hop1_ids`: node ids. `hop2_ids`: take one device's 64 seeds (an aligned block of seeds) with all their hop-1 and hop-2 ids, 10624 ids with repeats counted, and map them through partition_map: at most 607 positions fall in any one partition, and at most 83 fall in rows 256 and above of any one partition. Every device reaches both bounds. `bias_two`: class biases; in one draw all 172 lie within a window of width 4 (about -2 to 2, or about 108 to 112).
All inputs are finite; a program needn't handle non-finite values.
Results may differ from the reference program's by a relative error of at most 0.003.
Values may be sent and summed in bfloat16 or wider, within the bound.
A program may use at most 128 MiB of HBM per device.

```python
import jax
import jax.numpy as jnp
from jax import lax

FEAT = 128
HID = 256
CLASSES = 172
FAN1 = 15
FAN2 = 10
HOT_DEV = 256
SEEDS_DEV = 64
NODE_DEV = 8192
TREE = 166
COLD_CAP = 83
LOW_HOT = 20
HIGH_HOT = 524
HUBS = 8
NODES = 524288
SEEDS_ALL = 16384
N_DOM = 64
N_REP = 4


def sample_plan(key):
    folded = jax.random.fold_in(key, 4242)
    key_map, key_hub, key_dev = jax.random.split(folded, 3)
    part_map = jax.random.permutation(key_map, NODES).astype(jnp.int32)
    hub_order = jax.random.permutation(key_hub, N_DOM).astype(jnp.int32)
    total_rows = SEEDS_DEV * TREE
    cold_total = N_DOM * COLD_CAP
    hub_total = HUBS * HIGH_HOT

    def one_device(dev_key):
        key_cold, key_hot, key_mix = jax.random.split(dev_key, 3)
        row_index = jnp.arange(total_rows, dtype=jnp.int32)
        is_cold = row_index < cold_total
        cold_owner = jnp.minimum(row_index // COLD_CAP, N_DOM - 1)
        hot_index = jnp.maximum(row_index - cold_total, 0)
        owner_rank = jnp.where(hot_index < hub_total, hot_index // HIGH_HOT, HUBS + (hot_index - hub_total) // LOW_HOT)
        hot_owner = hub_order[jnp.clip(owner_rank, 0, N_DOM - 1)]
        owners = jnp.where(is_cold, cold_owner, hot_owner)
        cold_row = jax.random.randint(key_cold, (total_rows,), HOT_DEV, NODE_DEV, dtype=jnp.int32)
        hot_row = jax.random.randint(key_hot, (total_rows,), 0, HOT_DEV, dtype=jnp.int32)
        store_place = owners * NODE_DEV + jnp.where(is_cold, cold_row, hot_row)
        return store_place[jax.random.permutation(key_mix, total_rows)]
    places = jax.vmap(one_device)(jax.random.split(key_dev, N_DOM * N_REP))
    inverse = jnp.zeros((NODES,), jnp.int32).at[part_map].set(jnp.arange(NODES, dtype=jnp.int32))
    return (part_map, inverse[places])


def draw_partition_map(key, part):
    part_map, node_ids = sample_plan(key)
    return part_map


def draw_seed_ids(key, part):
    part_map, node_ids = sample_plan(key)
    return node_ids[:, :SEEDS_DEV].reshape(-1)


def draw_hop1_ids(key, part):
    part_map, node_ids = sample_plan(key)
    return node_ids[:, SEEDS_DEV:SEEDS_DEV * (1 + FAN1)].reshape(N_DOM * N_REP * SEEDS_DEV, FAN1)


def draw_hop2_ids(key, part):
    part_map, node_ids = sample_plan(key)
    return node_ids[:, SEEDS_DEV * (1 + FAN1):].reshape(N_DOM * N_REP * SEEDS_DEV, FAN1, FAN2)


def draw_bias_two(key, part):
    centred = 0.5 * jax.random.truncated_normal(key, -4.0, 4.0, (CLASSES,), jnp.float32)
    return centred


def set_ends(result, key, low, high):
    shape = result.shape
    index_at = [jax.random.randint(jax.random.fold_in(key, axis), (), 0, shape[axis]) for axis in range(len(shape))]
    result = result.at[tuple(index_at)].set(low)
    longest = shape.index(max(shape))
    index_at[longest] = (index_at[longest] + 1) % shape[longest]
    return result.at[tuple(index_at)].set(high)


def shard_levels(stream_key, dims, cuts, smallest, largest):
    loudness = 1.0
    for axis_at, parts in cuts:
        heights = jax.random.uniform(jax.random.fold_in(jax.random.fold_in(stream_key, 6), axis_at), (parts,), jnp.float32, smallest / len(cuts), largest / len(cuts))
        loudness = loudness * jnp.repeat(jnp.exp(heights), dims[axis_at] // parts).reshape((-1,) + (1,) * (len(dims) - 1 - axis_at))
    return loudness


def noise(stream_key, dims, scale, reach, cuts=(), kind=jnp.bfloat16):
    drawn = scale * jax.random.normal(stream_key, dims, jnp.float32)
    if cuts:
        drawn = drawn * shard_levels(stream_key, dims, cuts, -0.22, 0.18)
    return jnp.clip(drawn, -reach, reach).astype(kind)


def setup_inputs(seed: int = 0) -> dict:
    key_list = jax.random.split(jax.random.key(seed), 13)
    features = noise(key_list[0], (NODES, FEAT), 1.0, 6.0, ((0, 64),))
    partition_map = draw_partition_map(jax.random.fold_in(key_list[12], 71), 0)
    seed_ids = draw_seed_ids(jax.random.fold_in(key_list[12], 71), 0)
    hop1_ids = draw_hop1_ids(jax.random.fold_in(key_list[12], 71), 0)
    hop2_ids = draw_hop2_ids(jax.random.fold_in(key_list[12], 71), 0)
    labels = set_ends(jax.random.randint(key_list[5], (SEEDS_ALL,), 0, CLASSES), jax.random.fold_in(key_list[5], 1), 0, CLASSES - 1).astype(jnp.int32)
    self_one = noise(key_list[6], (FEAT, HID), FEAT ** -0.5, 0.5)
    neigh_one = noise(key_list[7], (FEAT, HID), FEAT ** -0.5, 0.5)
    bias_one = noise(key_list[8], (HID,), 0.5, 3.0, (), jnp.float32)
    self_two = noise(key_list[9], (HID, CLASSES), HID ** -0.5, 0.375)
    neigh_two = noise(key_list[10], (HID, CLASSES), HID ** -0.5, 0.375)
    bias_two = draw_bias_two(jax.random.fold_in(key_list[12], 71), 0)
    return {"features": features, "partition_map": partition_map, "seed_ids": seed_ids, "hop1_ids": hop1_ids, "hop2_ids": hop2_ids, "labels": labels, "self_one": self_one, "neigh_one": neigh_one, "bias_one": bias_one, "self_two": self_two, "neigh_two": neigh_two, "bias_two": bias_two}


def activate(values):
    return jax.nn.gelu(values, approximate=True)

def sage_terms(seed_rows, hop_rows, far_rows, labels, self_one, neigh_one, bias_one, self_two, neigh_two, bias_two):
    seed_count = seed_rows.shape[0]
    fan_one = hop_rows.shape[0] // seed_count
    feat_width = seed_rows.shape[1]
    hidden = self_one.shape[1]
    seed_mean = lax.optimization_barrier(jnp.mean(hop_rows.reshape(seed_count, fan_one, feat_width), axis=1, dtype=jnp.float32)).astype(jnp.bfloat16)
    far_mean = lax.optimization_barrier(jnp.mean(far_rows, axis=1, dtype=jnp.float32)).astype(jnp.bfloat16)
    pre_seed = jnp.dot(seed_rows, self_one, preferred_element_type=jnp.float32) + jnp.dot(seed_mean, neigh_one, preferred_element_type=jnp.float32) + bias_one
    pre_hop = jnp.dot(hop_rows, self_one, preferred_element_type=jnp.float32) + jnp.dot(far_mean, neigh_one, preferred_element_type=jnp.float32) + bias_one
    act_seed, back_seed = jax.vjp(activate, pre_seed)
    act_hop, back_hop = jax.vjp(activate, pre_hop)
    hid_seed = act_seed.astype(jnp.bfloat16)
    hid_hop = act_hop.astype(jnp.bfloat16)
    hop_mean = lax.optimization_barrier(jnp.mean(hid_hop.reshape(seed_count, fan_one, hidden), axis=1, dtype=jnp.float32)).astype(jnp.bfloat16)
    logits = jnp.dot(hid_seed, self_two, preferred_element_type=jnp.float32) + jnp.dot(hop_mean, neigh_two, preferred_element_type=jnp.float32) + bias_two
    peak_value = lax.optimization_barrier(jnp.max(logits, axis=1, keepdims=True))
    shifted = logits - peak_value
    log_total = jnp.log(lax.optimization_barrier(jnp.sum(jnp.exp(shifted), axis=1, keepdims=True)))
    log_probs = shifted - log_total
    class_iota = lax.broadcasted_iota(jnp.int32, logits.shape, 1)
    target = (labels[:, None] == class_iota).astype(jnp.float32)
    seed_loss = -lax.optimization_barrier(jnp.sum(log_probs * target, axis=1))
    d_logits = ((jnp.exp(log_probs) - target) / seed_count).astype(jnp.bfloat16)
    grad_self_two = jnp.dot(hid_seed.T, d_logits, preferred_element_type=jnp.float32)
    grad_neigh_two = jnp.dot(hop_mean.T, d_logits, preferred_element_type=jnp.float32)
    grad_bias_two = lax.optimization_barrier(jnp.sum(d_logits.astype(jnp.float32), axis=0))
    d_hid_seed = jnp.dot(d_logits, self_two.T, preferred_element_type=jnp.float32)
    d_hop_mean = jnp.dot(d_logits, neigh_two.T, preferred_element_type=jnp.float32)
    d_pre_seed = back_seed(d_hid_seed)[0].astype(jnp.bfloat16)
    spread = jnp.broadcast_to((d_hop_mean / fan_one)[:, None, :], (seed_count, fan_one, hidden)).reshape(seed_count * fan_one, hidden)
    d_pre_hop = back_hop(spread)[0].astype(jnp.bfloat16)
    grad_self_one = jnp.dot(seed_rows.T, d_pre_seed, preferred_element_type=jnp.float32) + jnp.dot(hop_rows.T, d_pre_hop, preferred_element_type=jnp.float32)
    grad_neigh_one = jnp.dot(seed_mean.T, d_pre_seed, preferred_element_type=jnp.float32) + jnp.dot(far_mean.T, d_pre_hop, preferred_element_type=jnp.float32)
    grad_bias_one = lax.optimization_barrier(jnp.sum(d_pre_seed.astype(jnp.float32), axis=0)) + lax.optimization_barrier(jnp.sum(d_pre_hop.astype(jnp.float32), axis=0))
    return (seed_loss, (grad_self_one, grad_neigh_one, grad_bias_one, grad_self_two, grad_neigh_two, grad_bias_two))

def reference(features, partition_map, seed_ids, hop1_ids, hop2_ids, labels, self_one, neigh_one, bias_one, self_two, neigh_two, bias_two):
    devices = N_DOM * N_REP
    seed_blocks = seed_ids.reshape(devices, SEEDS_DEV)
    hop_blocks = hop1_ids.reshape(devices, SEEDS_DEV * FAN1)
    far_blocks = hop2_ids.reshape(devices, SEEDS_DEV * FAN1, FAN2)
    label_blocks = labels.reshape(devices, SEEDS_DEV)
    initial = (jnp.zeros((FEAT, HID), jnp.float32), jnp.zeros((FEAT, HID), jnp.float32), jnp.zeros((HID,), jnp.float32), jnp.zeros((HID, CLASSES), jnp.float32), jnp.zeros((HID, CLASSES), jnp.float32), jnp.zeros((CLASSES,), jnp.float32))

    def one_block(totals, pieces):
        seeds_here, hops_here, far_here, labels_here = pieces
        seed_rows = features[partition_map[seeds_here]]
        hop_rows = features[partition_map[hops_here]]
        far_rows = features[partition_map[far_here]]
        seed_loss, grads = sage_terms(seed_rows, hop_rows, far_rows, labels_here, self_one, neigh_one, bias_one, self_two, neigh_two, bias_two)
        return (jax.tree.map(jnp.add, totals, grads), seed_loss)
    totals, losses = lax.scan(one_block, initial, (seed_blocks, hop_blocks, far_blocks, label_blocks))
    return (losses.reshape(-1), totals[0], totals[1], totals[2], totals[3], totals[4], totals[5])
```

```python
import jax
import jax.numpy as jnp
from jax import lax
from jax.experimental import pallas as pl
from jax.experimental.pallas import tpu as pltpu
from jax.sharding import PartitionSpec as P

MESH = pl.DeviceIdType.MESH

HOT_DEV = 256


def activate(values):
    return jax.nn.gelu(values, approximate=True)


def sage_terms(
    seed_rows,
    hop_rows,
    far_rows,
    labels,
    self_one,
    neigh_one,
    bias_one,
    self_two,
    neigh_two,
    bias_two,
):
    seed_count = seed_rows.shape[0]
    fan_one = hop_rows.shape[0] // seed_count
    feat_width = seed_rows.shape[1]
    hidden = self_one.shape[1]
    seed_mean = jnp.mean(
        hop_rows.reshape(seed_count, fan_one, feat_width), axis=1, dtype=jnp.float32
    ).astype(jnp.bfloat16)
    far_mean = jnp.mean(far_rows, axis=1, dtype=jnp.float32).astype(jnp.bfloat16)
    pre_seed = (
        jnp.dot(seed_rows, self_one, preferred_element_type=jnp.float32)
        + jnp.dot(seed_mean, neigh_one, preferred_element_type=jnp.float32)
        + bias_one
    )
    pre_hop = (
        jnp.dot(hop_rows, self_one, preferred_element_type=jnp.float32)
        + jnp.dot(far_mean, neigh_one, preferred_element_type=jnp.float32)
        + bias_one
    )
    act_seed, back_seed = jax.vjp(activate, pre_seed)
    act_hop, back_hop = jax.vjp(activate, pre_hop)
    hid_seed = act_seed.astype(jnp.bfloat16)
    hid_hop = act_hop.astype(jnp.bfloat16)
    hop_mean = jnp.mean(
        hid_hop.reshape(seed_count, fan_one, hidden), axis=1, dtype=jnp.float32
    ).astype(jnp.bfloat16)
    logits = (
        jnp.dot(hid_seed, self_two, preferred_element_type=jnp.float32)
        + jnp.dot(hop_mean, neigh_two, preferred_element_type=jnp.float32)
        + bias_two
    )
    peak_value = jnp.max(logits, axis=1, keepdims=True)
    shifted = logits - peak_value
    log_total = jnp.log(jnp.sum(jnp.exp(shifted), axis=1, keepdims=True))
    log_probs = shifted - log_total
    class_iota = lax.broadcasted_iota(jnp.int32, logits.shape, 1)
    target = (labels[:, None] == class_iota).astype(jnp.float32)
    seed_loss = -jnp.sum(log_probs * target, axis=1)
    d_logits = ((jnp.exp(log_probs) - target) / seed_count).astype(jnp.bfloat16)
    grad_self_two = jnp.dot(hid_seed.T, d_logits, preferred_element_type=jnp.float32)
    grad_neigh_two = jnp.dot(hop_mean.T, d_logits, preferred_element_type=jnp.float32)
    grad_bias_two = jnp.sum(d_logits.astype(jnp.float32), axis=0)
    d_hid_seed = jnp.dot(d_logits, self_two.T, preferred_element_type=jnp.float32)
    d_hop_mean = jnp.dot(d_logits, neigh_two.T, preferred_element_type=jnp.float32)
    d_pre_seed = back_seed(d_hid_seed)[0].astype(jnp.bfloat16)
    spread = jnp.broadcast_to(
        (d_hop_mean / fan_one)[:, None, :], (seed_count, fan_one, hidden)
    ).reshape(seed_count * fan_one, hidden)
    d_pre_hop = back_hop(spread)[0].astype(jnp.bfloat16)
    grad_self_one = jnp.dot(seed_rows.T, d_pre_seed, preferred_element_type=jnp.float32) + jnp.dot(
        hop_rows.T, d_pre_hop, preferred_element_type=jnp.float32
    )
    grad_neigh_one = jnp.dot(seed_mean.T, d_pre_seed, preferred_element_type=jnp.float32) + jnp.dot(
        far_mean.T, d_pre_hop, preferred_element_type=jnp.float32
    )
    grad_bias_one = jnp.sum(d_pre_seed.astype(jnp.float32), axis=0) + jnp.sum(
        d_pre_hop.astype(jnp.float32), axis=0
    )
    return (
        seed_loss,
        (
            grad_self_one,
            grad_neigh_one,
            grad_bias_one,
            grad_self_two,
            grad_neigh_two,
            grad_bias_two,
        ),
    )


def bucket_slots(owners, chosen, part_count):
    columns = lax.broadcasted_iota(jnp.int32, (owners.shape[0], part_count), 1)
    member = ((owners[:, None] == columns) & chosen[:, None]).astype(jnp.int32)
    running = jnp.cumsum(member, axis=0)
    return jnp.sum(running * member, axis=1) - 1


def request_table(owners, slots, local_rows, part_count, capacity):
    target_slot = jnp.where(slots >= 0, slots, capacity)
    table = jnp.zeros((part_count, capacity), jnp.int32)
    return table.at[owners, target_slot].set(local_rows, mode="drop")


def shards(
    features,
    partition_map,
    seed_ids,
    hop1_ids,
    hop2_ids,
    labels,
    self_one,
    neigh_one,
    bias_one,
    self_two,
    neigh_two,
    bias_two,
):
    part_count = lax.axis_size("dom")
    seed_count = seed_ids.shape[0]
    fan_one = hop1_ids.shape[1]
    fan_two = hop2_ids.shape[2]
    node_rows = features.shape[0]
    feat_width = features.shape[1]
    tree_rows = 1 + fan_one + fan_one * fan_two
    seed_unit = seed_count // part_count
    cold_cap = tree_rows // 2 * seed_unit
    wanted = jnp.concatenate([seed_ids, hop1_ids.reshape(-1), hop2_ids.reshape(-1)])
    position = partition_map[wanted]
    owners = position // node_rows
    local_rows = position % node_rows
    is_cold = local_rows >= HOT_DEV
    slots = bucket_slots(owners, is_cold, part_count)
    request = request_table(owners, slots, local_rows, part_count, cold_cap)
    arrived = lax.all_to_all(request, "dom", split_axis=0, concat_axis=0, tiled=True)
    returned = lax.all_to_all(features[arrived], "dom", split_axis=0, concat_axis=0, tiled=True)
    hub_rows = lax.all_gather(features[:HOT_DEV], "dom", axis=0, tiled=True)
    from_far = returned[owners, jnp.maximum(slots, 0)]
    from_hub = hub_rows[owners * HOT_DEV + jnp.minimum(local_rows, HOT_DEV - 1)]
    fetched = jnp.where(is_cold[:, None], from_far, from_hub)
    seed_rows = fetched[:seed_count]
    hop_rows = fetched[seed_count : seed_count * (1 + fan_one)]
    far_rows = fetched[seed_count * (1 + fan_one) :].reshape(
        seed_count * fan_one, fan_two, feat_width
    )
    seed_loss, grads = sage_terms(
        seed_rows,
        hop_rows,
        far_rows,
        labels,
        self_one,
        neigh_one,
        bias_one,
        self_two,
        neigh_two,
        bias_two,
    )
    summed = unpack(sum_all(pack(grads)))
    return (seed_loss, summed[0], summed[1], summed[2], summed[3], summed[4], summed[5])


PIECE = 80


def sum_kernel(mine, total, other, send_z, recv_z, send_p, recv_p, core_send, core_recv,
               z_send, z_recv, p_send, p_recv, g_send, g_recv, h_send, h_recv):
    dom = lax.axis_index("dom")
    y = lax.axis_index("rep")
    core = lax.rem(dom, 2)
    z = lax.rem(lax.div(dom, 2), 8)
    x = lax.div(dom, 16)

    def device(to_x, to_y, to_z, to_core):
        return ((to_x * 8 + to_z) * 2 + to_core, to_y)

    partner = device(x, y, z, 1 - core)

    def z_peer(step):
        return device(x, y, lax.rem(z + step, 8), core)

    def plane_peer(step):
        place = lax.rem(x * 4 + y + step, 16)
        return device(lax.div(place, 4), lax.rem(place, 4), z, core)

    barrier = pltpu.get_barrier_semaphore()
    pl.semaphore_signal(barrier, inc=1, device_id=partner, device_id_type=MESH)

    @pl.loop(1, 8)
    def _(step):
        pl.semaphore_signal(barrier, inc=1, device_id=z_peer(step), device_id_type=MESH)

    @pl.loop(1, 16)
    def _(step):
        pl.semaphore_signal(barrier, inc=1, device_id=plane_peer(step), device_id_type=MESH)

    pl.semaphore_wait(barrier, 23)

    swap = pltpu.make_async_remote_copy(
        src_ref=mine.at[1 - core], dst_ref=other, send_sem=core_send, recv_sem=core_recv,
        device_id=partner, device_id_type=MESH,
    )
    swap.start()
    swap.wait()

    @pl.loop(0, 8)
    def _(part):
        send_z[part] = (mine[core, part] + other[part]).astype(jnp.bfloat16)

    def z_copy(step):
        to_z = lax.rem(z + step, 8)
        return pltpu.make_async_remote_copy(
            src_ref=send_z.at[to_z], dst_ref=recv_z.at[step], send_sem=z_send.at[step],
            recv_sem=z_recv.at[step], device_id=z_peer(step), device_id_type=MESH,
        )

    @pl.loop(1, 8)
    def _(step):
        z_copy(step).start()

    kept = mine[core, z] + other[z]

    @pl.loop(1, 8)
    def _(step):
        z_copy(step).wait()

    def add_z(step, value):
        return value + recv_z[step].astype(jnp.float32)

    kept = lax.fori_loop(1, 8, add_z, kept)
    send_p[...] = kept.astype(jnp.bfloat16)

    def plane_copy(step):
        return pltpu.make_async_remote_copy(
            src_ref=send_p, dst_ref=recv_p.at[step], send_sem=p_send.at[step],
            recv_sem=p_recv.at[step], device_id=plane_peer(step), device_id_type=MESH,
        )

    @pl.loop(1, 16)
    def _(step):
        plane_copy(step).start()

    recv_p[0] = send_p[...]

    @pl.loop(1, 16)
    def _(step):
        plane_copy(step).wait()

    def add_plane(place, value):
        step = lax.rem(x * 4 + y - place + 16, 16)
        return value + recv_p[step].astype(jnp.float32)

    total[core, z] = lax.fori_loop(0, 16, add_plane, jnp.zeros_like(kept))

    def z_back(step):
        return pltpu.make_async_remote_copy(
            src_ref=total.at[core, z], dst_ref=total.at[core, z], send_sem=g_send.at[step],
            recv_sem=g_recv.at[step], device_id=z_peer(step), device_id_type=MESH,
        )

    def hand_on(step):
        of_z = lax.rem(z - step + 8, 8)
        return pltpu.make_async_remote_copy(
            src_ref=total.at[core, of_z], dst_ref=total.at[core, of_z], send_sem=h_send.at[step],
            recv_sem=h_recv.at[step], device_id=partner, device_id_type=MESH,
        )

    @pl.loop(1, 8)
    def _(step):
        z_back(step).start()

    hand_on(0).start()

    @pl.loop(1, 8)
    def _(step):
        z_back(step).wait()
        hand_on(step).start()

    @pl.loop(0, 8)
    def _(step):
        hand_on(step).wait()


def sum_all(packed):
    vmem = pl.BlockSpec(memory_space=pltpu.VMEM)
    dma = pltpu.SemaphoreType.DMA
    return pl.pallas_call(
        sum_kernel,
        out_shape=jax.ShapeDtypeStruct((2, 8, PIECE, 128), jnp.float32),
        in_specs=[vmem],
        out_specs=vmem,
        scratch_shapes=[
            pltpu.VMEM((8, PIECE, 128), jnp.float32),
            pltpu.VMEM((8, PIECE, 128), jnp.bfloat16),
            pltpu.VMEM((8, PIECE, 128), jnp.bfloat16),
            pltpu.VMEM((PIECE, 128), jnp.bfloat16),
            pltpu.VMEM((16, PIECE, 128), jnp.bfloat16),
            dma, dma, dma((8,)), dma((8,)), dma((16,)), dma((16,)),
            dma((8,)), dma((8,)), dma((8,)), dma((8,)),
        ],
        compiler_params=pltpu.CompilerParams(collective_id=1, has_side_effects=True),
        name="sum_all",
    )(packed)


def pack(grads):
    self_one, neigh_one, bias_one, self_two, neigh_two, bias_two = grads
    rest = jnp.concatenate(
        [
            self_two[:, 128:],
            bias_one[:, None],
            jnp.pad(bias_two, (0, 84))[:, None],
            jnp.zeros((256, 18), jnp.float32),
            neigh_two[:, 128:],
            jnp.zeros((256, 20), jnp.float32),
        ],
        axis=1,
    )
    return jnp.concatenate(
        [
            self_one[:, :128],
            self_one[:, 128:],
            neigh_one[:, :128],
            neigh_one[:, 128:],
            self_two[:, :128],
            neigh_two[:, :128],
            rest,
        ],
        axis=0,
    ).reshape(2, 8, PIECE, 128)


def unpack_kernel(packed, self_one, neigh_one, self_two, neigh_two):
    self_one[:, :128] = packed[0:128]
    self_one[:, 128:] = packed[128:256]
    neigh_one[:, :128] = packed[256:384]
    neigh_one[:, 128:] = packed[384:512]
    self_two[:, :128] = packed[512:768]
    self_two[:, 128:] = packed[1024:1280, 0:44]
    neigh_two[:, :128] = packed[768:1024]
    neigh_two[:, 128:] = packed[1024:1280, 64:108]


def unpack(total):
    flat = total.reshape(16 * PIECE, 128)
    shapes = ((128, 256), (128, 256), (256, 172), (256, 172))
    self_one, neigh_one, self_two, neigh_two = pl.pallas_call(
        unpack_kernel,
        out_shape=[jax.ShapeDtypeStruct(shape, jnp.float32) for shape in shapes],
        name="unpack",
    )(flat)
    return self_one, neigh_one, flat[1024:1280, 44], self_two, neigh_two, flat[1024:1196, 45]


def solution(mesh):
    return jax.shard_map(
        shards,
        mesh=mesh,
        in_specs=(
            P("dom", None),
            P(),
            P(("dom", "rep")),
            P(("dom", "rep"), None),
            P(("dom", "rep"), None, None),
            P(("dom", "rep")),
            P(),
            P(),
            P(),
            P(),
            P(),
            P(),
        ),
        out_specs=(P(("dom", "rep")), P(), P(), P(), P(), P(), P()),
        check_vma=False,
    )
```

```python
import functools

import jax
import jax.numpy as jnp
from jax import lax
from jax.experimental import pallas as pl
from jax.experimental.pallas import tpu as pltpu
from jax.sharding import PartitionSpec as P

MESH = pl.DeviceIdType.MESH
HOT_DEV = 256
NODE_DEV = 8192
OWNERS = 64
CAP = 83
SEEDS = 64
FAN1 = 15
FAN2 = 10
HOPS = SEEDS * FAN1
CLASSES = 172
BLOCK = 128
GROUP = 4
CHUNK = 16
ROWS = 1280
PIECE = ROWS // 16
VMEM_LIMIT = 60 * 1024 * 1024


def plan_kernel(blocks, lines, ids, table, request_out, place_out, found, kept_place, request):
    square_row = lax.broadcasted_iota(jnp.int32, (BLOCK, BLOCK), 0)
    square_col = lax.broadcasted_iota(jnp.int32, (BLOCK, BLOCK), 1)
    diagonal = square_row == square_col
    before = jnp.concatenate(
        [(square_row < square_col).astype(jnp.bfloat16), jnp.ones((BLOCK, BLOCK), jnp.bfloat16)],
        axis=1,
    )
    owner_row = lax.broadcasted_iota(jnp.int32, (OWNERS, BLOCK), 0)
    groups = ids.shape[0] // GROUP
    found[...] = jnp.zeros_like(found)
    kept_place[...] = jnp.zeros_like(kept_place)
    request[...] = jnp.zeros_like(request)

    def spread(position, valid):
        owner = lax.shift_right_logical(position, 13)
        row = position & (NODE_DEV - 1)
        cold = (row >= HOT_DEV) & valid
        member = ((owner_row == owner) & cold).astype(jnp.float32)
        return owner, row, cold, member

    def step(group, base):
        old = [kept_place[pl.ds(8 * g, 2)] for g in range(GROUP)]
        rows = [found[BLOCK * g : BLOCK * (g + 1)] for g in range(GROUP)]
        from_row = jnp.minimum(group, groups - 1) * GROUP
        for g in range(GROUP):
            for at in range(BLOCK):
                found[pl.ds(BLOCK * g + at, 1)] = table[lines[from_row + g, at]]
        last_row = jnp.maximum(group - 1, 0) * GROUP
        ids_row = jnp.minimum(last_row, (groups - 1) * GROUP)
        for g in range(GROUP):
            valid = (group >= 1) & (last_row + g < blocks)
            lane_row = (ids[pl.ds(ids_row + g, 1)] & 127).astype(jnp.float32)
            lane = jnp.sum(jnp.where(diagonal, lane_row, 0.0), axis=1, keepdims=True)
            kept = jnp.where(square_col == lane.astype(jnp.int32), rows[g], 0)
            total = jnp.sum(kept.astype(jnp.float32), axis=1, keepdims=True)
            position = jnp.sum(jnp.where(diagonal, total, 0.0), axis=0, keepdims=True)
            position = position.astype(jnp.int32)
            owner, row, cold, member = spread(position, valid)
            counted = jnp.dot(
                member.astype(jnp.bfloat16), before, preferred_element_type=jnp.float32
            )
            rank = jnp.sum((counted[:, :BLOCK] + base) * member, axis=0, keepdims=True)
            slot = jnp.minimum(rank.astype(jnp.int32), CAP - 1)
            place = jnp.where(
                cold,
                owner * CAP + slot,
                OWNERS * CAP + owner * HOT_DEV + jnp.minimum(row, HOT_DEV - 1),
            )
            place_out[pl.ds(last_row + g, 1)] = place
            kept_place[pl.ds(8 * g, 1)] = position
            kept_place[pl.ds(8 * g + 1, 1)] = slot
            base = base + counted[:, BLOCK:]
        old_group = (group - 2) * GROUP
        update = request[...]
        for g in range(GROUP):
            valid = (group >= 2) & (old_group + g < blocks)
            _, row, _, member = spread(old[g][0:1], valid)
            pick = (square_row == old[g][1:2]).astype(jnp.bfloat16)
            high = member * lax.shift_right_logical(row, 8).astype(jnp.float32)
            low = member * (row & 255).astype(jnp.float32)
            both = jnp.concatenate([high, low], axis=0).astype(jnp.bfloat16)
            update = update + lax.dot_general(
                both, pick, (((1,), (1,)), ((), ())), preferred_element_type=jnp.float32
            )
        request[...] = update
        return base

    lax.fori_loop(0, groups + 2, step, jnp.zeros((OWNERS, BLOCK), jnp.float32))
    table_out = request[0:OWNERS] * 256.0 + request[OWNERS:]
    request_out[...] = table_out.astype(jnp.int32)


def plan(ids, partition_map):
    blocks = ids.shape[0] * ids.shape[1] // BLOCK
    padded = -(-blocks // GROUP) * GROUP
    ids = jnp.pad(ids.reshape(blocks, BLOCK), ((0, padded - blocks), (0, 0)))
    lines = lax.shift_right_logical(ids, 7)
    return pl.pallas_call(
        functools.partial(plan_kernel, blocks),
        out_shape=[
            jax.ShapeDtypeStruct((OWNERS, BLOCK), jnp.int32),
            jax.ShapeDtypeStruct((padded + GROUP, BLOCK), jnp.int32),
        ],
        in_specs=[
            pl.BlockSpec(memory_space=pltpu.SMEM),
            pl.BlockSpec(memory_space=pltpu.VMEM),
            pl.BlockSpec(memory_space=pltpu.VMEM),
        ],
        out_specs=[pl.BlockSpec(memory_space=pltpu.VMEM)] * 2,
        scratch_shapes=[
            pltpu.VMEM((GROUP * BLOCK, BLOCK), jnp.int32),
            pltpu.VMEM((GROUP * 8, BLOCK), jnp.int32),
            pltpu.VMEM((BLOCK, BLOCK), jnp.float32),
        ],
        compiler_params=pltpu.CompilerParams(vmem_limit_bytes=VMEM_LIMIT),
        name="plan",
    )(lines, ids, partition_map.reshape(-1, 1, BLOCK))


def serve_kernel(wanted, features, out, wide, picked):
    wide[...] = features[...].astype(jnp.float32)

    @pl.loop(0, OWNERS)
    def _(asker):
        for at in range(CAP):
            picked[pl.ds(at, 1)] = wide[pl.ds(wanted[asker, at], 1)]
        out[asker] = picked[0:CAP].astype(jnp.bfloat16)


def serve(wanted, features):
    return pl.pallas_call(
        serve_kernel,
        out_shape=jax.ShapeDtypeStruct((OWNERS, CAP, 128), jnp.bfloat16),
        in_specs=[
            pl.BlockSpec(memory_space=pltpu.SMEM),
            pl.BlockSpec(memory_space=pltpu.VMEM),
        ],
        out_specs=pl.BlockSpec(memory_space=pltpu.VMEM),
        scratch_shapes=[
            pltpu.VMEM(features.shape, jnp.float32),
            pltpu.VMEM((88, 128), jnp.float32),
        ],
        compiler_params=pltpu.CompilerParams(vmem_limit_bytes=VMEM_LIMIT),
        name="serve",
    )(wanted, features)


def dot(a, b, dims):
    return lax.dot_general(a, b, (dims, ((), ())), preferred_element_type=jnp.float32)


def gelu_parts(x):
    scale = 0.7978845608028654
    square = x * x
    t = jnp.tanh(scale * x * (1.0 + 0.044715 * square))
    half = 0.5 * (1.0 + t)
    slope = half + 0.5 * x * (1.0 - t * t) * (scale * (1.0 + 3.0 * 0.044715 * square))
    return x * half, slope


def sage_kernel(place, returned, hubs, labels, self_one, neigh_one, bias_one, self_two, neigh_two,
                bias_two, loss_out, packed, table, rows, far):
    for owner in range(OWNERS):
        table[CAP * owner : CAP * (owner + 1)] = returned[owner].astype(jnp.float32)
    table[CAP * OWNERS :] = hubs[...].astype(jnp.float32)

    @pl.loop(0, (SEEDS + HOPS) // 64)
    def _(block):
        first = pl.multiple_of(block * 64, 64)
        for at in range(64):
            rows[pl.ds(first + at, 1)] = table[pl.ds(place[first + at], 1)]

    @pl.loop(0, HOPS // CHUNK)
    def _(block):
        first = pl.multiple_of(block * CHUNK, CHUNK)
        for at in range(CHUNK):
            value = None
            for k in range(FAN2):
                row = table[pl.ds(place[first + (SEEDS + HOPS + k * HOPS + at)], 1)]
                value = row if value is None else value + row
            far[pl.ds(first + at, 1)] = value

    seed_rows = rows[0:SEEDS].astype(jnp.bfloat16)
    hop_rows = rows[SEEDS:].astype(jnp.bfloat16)
    far_mean = (far[...] * (1.0 / FAN2)).astype(jnp.bfloat16)
    seed_sum = rows[SEEDS : 2 * SEEDS]
    for f in range(1, FAN1):
        seed_sum = seed_sum + rows[SEEDS * (f + 1) : SEEDS * (f + 2)]
    seed_mean = (seed_sum * (1.0 / FAN1)).astype(jnp.bfloat16)

    own = jnp.concatenate([seed_rows, hop_rows], axis=0)
    near = jnp.concatenate([seed_mean, far_mean], axis=0)
    both = jnp.concatenate([own, near], axis=1)
    weight = jnp.concatenate([self_one[...], neigh_one[...]], axis=0)
    pre = dot(both, weight, ((1,), (0,))) + bias_one[...]
    act, slope = gelu_parts(pre)
    hid_seed = act[0:SEEDS].astype(jnp.bfloat16)
    hop_sum = act[SEEDS : 2 * SEEDS]
    for f in range(1, FAN1):
        hop_sum = hop_sum + act[SEEDS * (f + 1) : SEEDS * (f + 2)]
    hop_mean = (hop_sum * (1.0 / FAN1)).astype(jnp.bfloat16)

    logits = (
        dot(hid_seed, self_two[...], ((1,), (1,)))
        + dot(hop_mean, neigh_two[...], ((1,), (1,)))
        + bias_two[...]
    )
    shifted = logits - jnp.max(logits, axis=1, keepdims=True)
    exps = jnp.exp(shifted)
    sums = jnp.sum(exps, axis=1, keepdims=True)
    log_probs = shifted - jnp.log(sums)
    small_row = lax.broadcasted_iota(jnp.int32, (SEEDS, SEEDS), 0)
    small_col = lax.broadcasted_iota(jnp.int32, (SEEDS, SEEDS), 1)
    label = jnp.sum(
        jnp.where(small_row == small_col, labels[...].astype(jnp.float32), 0.0),
        axis=1, keepdims=True,
    ).astype(jnp.int32)
    target = lax.broadcasted_iota(jnp.int32, (SEEDS, CLASSES), 1) == label
    picked = jnp.sum(jnp.where(target, log_probs, 0.0), axis=1, keepdims=True)
    loss_out[...] = -jnp.sum(
        jnp.where(small_row == small_col, picked, 0.0), axis=0, keepdims=True
    )
    d_logits32 = (jnp.exp(log_probs) - target.astype(jnp.float32)) * (1.0 / SEEDS)
    d_logits = d_logits32.astype(jnp.bfloat16)

    zeros = jnp.zeros((8, 128), jnp.float32)
    packed[512 + 168 : 512 + 176] = zeros
    packed[688 + 168 : 688 + 176] = zeros
    packed[864 + 168 : 864 + 176] = zeros
    packed[1040 + 168 : 1040 + 176] = zeros
    packed[1216:] = jnp.zeros((ROWS - 1216, 128), jnp.float32)
    grad_self_two = dot(d_logits, hid_seed, ((0,), (0,)))
    packed[512:684] = grad_self_two[:, :128]
    packed[688:860] = grad_self_two[:, 128:]
    grad_neigh_two = dot(d_logits, hop_mean, ((0,), (0,)))
    packed[864:1036] = grad_neigh_two[:, :128]
    packed[1040:1212] = grad_neigh_two[:, 128:]
    grad_bias_two = jnp.sum(d_logits32, axis=0, keepdims=True)
    packed[1218:1219] = grad_bias_two[:, :128]
    packed[1219:1220, 0 : CLASSES - 128] = grad_bias_two[:, 128:]

    d_hid_seed = dot(d_logits, self_two[...], ((1,), (0,)))
    d_hop_mean = dot(d_logits, neigh_two[...], ((1,), (0,))) * (1.0 / FAN1)
    d_hid = jnp.concatenate([d_hid_seed] + [d_hop_mean] * FAN1, axis=0)
    d_pre32 = d_hid * slope
    d_pre = d_pre32.astype(jnp.bfloat16)
    grad_one = dot(both, d_pre, ((0,), (0,)))
    packed[0:128] = grad_one[0:128, :128]
    packed[128:256] = grad_one[0:128, 128:]
    packed[256:384] = grad_one[128:256, :128]
    packed[384:512] = grad_one[128:256, 128:]
    grad_bias_one = jnp.sum(d_pre32, axis=0, keepdims=True)
    packed[1216:1217] = grad_bias_one[:, :128]
    packed[1217:1218] = grad_bias_one[:, 128:]


def sage(place, returned, hubs, labels, self_one, neigh_one, bias_one, self_two, neigh_two, bias_two):
    vmem = pl.BlockSpec(memory_space=pltpu.VMEM)
    loss, packed = pl.pallas_call(
        sage_kernel,
        out_shape=[
            jax.ShapeDtypeStruct((1, SEEDS), jnp.float32),
            jax.ShapeDtypeStruct((ROWS, 128), jnp.float32),
        ],
        in_specs=[pl.BlockSpec(memory_space=pltpu.SMEM)] + [vmem] * 9,
        out_specs=[vmem, vmem],
        scratch_shapes=[
            pltpu.VMEM((OWNERS * (CAP + HOT_DEV), 128), jnp.float32),
            pltpu.VMEM((SEEDS + HOPS, 128), jnp.float32),
            pltpu.VMEM((HOPS, 128), jnp.float32),
        ],
        compiler_params=pltpu.CompilerParams(vmem_limit_bytes=VMEM_LIMIT),
        name="sage",
    )(
        place.reshape(-1), returned, hubs, labels[None, :], self_one, neigh_one, bias_one[None, :],
        self_two.T, neigh_two.T, bias_two[None, :],
    )
    return loss.reshape(-1), packed


def unpack_kernel(packed, self_one, neigh_one, bias_one, self_two, neigh_two, bias_two):
    self_one[:, :128] = packed[0:128]
    self_one[:, 128:] = packed[128:256]
    neigh_one[:, :128] = packed[256:384]
    neigh_one[:, 128:] = packed[384:512]
    self_two[:, :128] = packed[512:684]
    self_two[:, 128:] = packed[688:860]
    neigh_two[:, :128] = packed[864:1036]
    neigh_two[:, 128:] = packed[1040:1212]
    bias_one[:, :128] = packed[1216:1217]
    bias_one[:, 128:] = packed[1217:1218]
    bias_two[:, :128] = packed[1218:1219]
    bias_two[:, 128:] = packed[1219:1220, 0 : CLASSES - 128]


def unpack(packed):
    shapes = ((128, 256), (128, 256), (1, 256), (CLASSES, 256), (CLASSES, 256), (1, CLASSES))
    self_one, neigh_one, bias_one, self_two, neigh_two, bias_two = pl.pallas_call(
        unpack_kernel,
        out_shape=[jax.ShapeDtypeStruct(shape, jnp.float32) for shape in shapes],
        name="unpack",
    )(packed)
    return self_one, neigh_one, bias_one.reshape(-1), self_two.T, neigh_two.T, bias_two.reshape(-1)


def sum_kernel(mine, total, other, send_z, recv_z, send_p, recv_p, core_send, core_recv,
               z_send, z_recv, p_send, p_recv, g_send, g_recv, h_send, h_recv):
    dom = lax.axis_index("dom")
    y = lax.axis_index("rep")
    core = lax.rem(dom, 2)
    z = lax.rem(lax.div(dom, 2), 8)
    x = lax.div(dom, 16)

    def device(to_x, to_y, to_z, to_core):
        return ((to_x * 8 + to_z) * 2 + to_core, to_y)

    partner = device(x, y, z, 1 - core)

    def z_peer(step):
        return device(x, y, lax.rem(z + step, 8), core)

    def plane_peer(step):
        place = lax.rem(x * 4 + y + step, 16)
        return device(lax.div(place, 4), lax.rem(place, 4), z, core)

    barrier = pltpu.get_barrier_semaphore()
    pl.semaphore_signal(barrier, inc=1, device_id=partner, device_id_type=MESH)

    @pl.loop(1, 8)
    def _(step):
        pl.semaphore_signal(barrier, inc=1, device_id=z_peer(step), device_id_type=MESH)

    @pl.loop(1, 16)
    def _(step):
        pl.semaphore_signal(barrier, inc=1, device_id=plane_peer(step), device_id_type=MESH)

    pl.semaphore_wait(barrier, 23)

    swap = pltpu.make_async_remote_copy(
        src_ref=mine.at[1 - core], dst_ref=other, send_sem=core_send, recv_sem=core_recv,
        device_id=partner, device_id_type=MESH,
    )
    swap.start()
    swap.wait()

    @pl.loop(0, 8)
    def _(part):
        send_z[part] = (mine[core, part] + other[part]).astype(jnp.bfloat16)

    def z_copy(step):
        to_z = lax.rem(z + step, 8)
        return pltpu.make_async_remote_copy(
            src_ref=send_z.at[to_z], dst_ref=recv_z.at[step], send_sem=z_send.at[step],
            recv_sem=z_recv.at[step], device_id=z_peer(step), device_id_type=MESH,
        )

    @pl.loop(1, 8)
    def _(step):
        z_copy(step).start()

    kept = mine[core, z] + other[z]

    @pl.loop(1, 8)
    def _(step):
        z_copy(step).wait()

    def add_z(step, value):
        return value + recv_z[step].astype(jnp.float32)

    kept = lax.fori_loop(1, 8, add_z, kept)
    send_p[...] = kept.astype(jnp.bfloat16)

    def plane_copy(step):
        return pltpu.make_async_remote_copy(
            src_ref=send_p, dst_ref=recv_p.at[step], send_sem=p_send.at[step],
            recv_sem=p_recv.at[step], device_id=plane_peer(step), device_id_type=MESH,
        )

    @pl.loop(1, 16)
    def _(step):
        plane_copy(step).start()

    recv_p[0] = send_p[...]

    @pl.loop(1, 16)
    def _(step):
        plane_copy(step).wait()

    def add_plane(place, value):
        step = lax.rem(x * 4 + y - place + 16, 16)
        return value + recv_p[step].astype(jnp.float32)

    total[core, z] = lax.fori_loop(0, 16, add_plane, jnp.zeros_like(kept))

    def z_back(step):
        return pltpu.make_async_remote_copy(
            src_ref=total.at[core, z], dst_ref=total.at[core, z], send_sem=g_send.at[step],
            recv_sem=g_recv.at[step], device_id=z_peer(step), device_id_type=MESH,
        )

    def hand_on(step):
        of_z = lax.rem(z - step + 8, 8)
        return pltpu.make_async_remote_copy(
            src_ref=total.at[core, of_z], dst_ref=total.at[core, of_z], send_sem=h_send.at[step],
            recv_sem=h_recv.at[step], device_id=partner, device_id_type=MESH,
        )

    @pl.loop(1, 8)
    def _(step):
        z_back(step).start()

    hand_on(0).start()

    @pl.loop(1, 8)
    def _(step):
        z_back(step).wait()
        hand_on(step).start()

    @pl.loop(0, 8)
    def _(step):
        hand_on(step).wait()


def sum_all(packed):
    vmem = pl.BlockSpec(memory_space=pltpu.VMEM)
    dma = pltpu.SemaphoreType.DMA
    return pl.pallas_call(
        sum_kernel,
        out_shape=jax.ShapeDtypeStruct((2, 8, PIECE, 128), jnp.float32),
        in_specs=[vmem],
        out_specs=vmem,
        scratch_shapes=[
            pltpu.VMEM((8, PIECE, 128), jnp.float32),
            pltpu.VMEM((8, PIECE, 128), jnp.bfloat16),
            pltpu.VMEM((8, PIECE, 128), jnp.bfloat16),
            pltpu.VMEM((PIECE, 128), jnp.bfloat16),
            pltpu.VMEM((16, PIECE, 128), jnp.bfloat16),
            dma, dma, dma((8,)), dma((8,)), dma((16,)), dma((16,)),
            dma((8,)), dma((8,)), dma((8,)), dma((8,)),
        ],
        compiler_params=pltpu.CompilerParams(collective_id=1, has_side_effects=True),
        name="sum_all",
    )(packed)


def shards(
    features,
    partition_map,
    seed_ids,
    hop1_ids,
    hop2_ids,
    labels,
    self_one,
    neigh_one,
    bias_one,
    self_two,
    neigh_two,
    bias_two,
):
    ids = jnp.concatenate(
        [
            seed_ids[None, :],
            hop1_ids.T,
            hop2_ids.transpose(2, 1, 0).reshape(FAN2 * FAN1, SEEDS),
        ],
        axis=0,
    )
    hubs = lax.all_gather(features[:HOT_DEV], "dom", axis=0, tiled=True)
    request, place = plan(ids, partition_map)
    wanted = lax.all_to_all(request, "dom", split_axis=0, concat_axis=0, tiled=True)
    returned = lax.all_to_all(serve(wanted, features), "dom", split_axis=0, concat_axis=0, tiled=True)
    seed_loss, packed = sage(
        place, returned, hubs, labels, self_one, neigh_one, bias_one, self_two, neigh_two, bias_two
    )
    total = sum_all(packed.reshape(2, 8, PIECE, 128))
    return (seed_loss, *unpack(total.reshape(ROWS, 128)))


def solution(mesh):
    return jax.shard_map(
        shards,
        mesh=mesh,
        in_specs=(
            P("dom", None),
            P(),
            P(("dom", "rep")),
            P(("dom", "rep"), None),
            P(("dom", "rep"), None, None),
            P(("dom", "rep")),
            P(),
            P(),
            P(),
            P(),
            P(),
            P(),
        ),
        out_specs=(P(("dom", "rep")), P(), P(), P(), P(), P(), P()),
        check_vma=False,
    )
```

```python
import functools

import jax
import jax.numpy as jnp
from jax import lax
from jax.experimental import pallas as pl
from jax.experimental.pallas import tpu as pltpu
from jax.sharding import PartitionSpec as P

MESH = pl.DeviceIdType.MESH
HOT_DEV = 256
NODE_DEV = 8192
OWNERS = 64
CAP = 83
SEEDS = 64
FAN1 = 15
FAN2 = 10
HOPS = SEEDS * FAN1
CLASSES = 172
BLOCK = 128
GROUP = 4
CHUNK = 16
ROWS = 1280
PIECE = ROWS // 16
VMEM_LIMIT = 60 * 1024 * 1024


def plan_kernel(blocks, lines, ids, table, request_out, place_out, found, kept_place, request):
    square_row = lax.broadcasted_iota(jnp.int32, (BLOCK, BLOCK), 0)
    square_col = lax.broadcasted_iota(jnp.int32, (BLOCK, BLOCK), 1)
    diagonal = square_row == square_col
    before = jnp.concatenate(
        [(square_row < square_col).astype(jnp.bfloat16), jnp.ones((BLOCK, BLOCK), jnp.bfloat16)],
        axis=1,
    )
    owner_row = lax.broadcasted_iota(jnp.int32, (OWNERS, BLOCK), 0)
    groups = ids.shape[0] // GROUP
    found[...] = jnp.zeros_like(found)
    kept_place[...] = jnp.zeros_like(kept_place)
    request[...] = jnp.zeros_like(request)

    def spread(position, valid):
        owner = lax.shift_right_logical(position, 13)
        row = position & (NODE_DEV - 1)
        cold = (row >= HOT_DEV) & valid
        member = ((owner_row == owner) & cold).astype(jnp.float32)
        return owner, row, cold, member

    def step(group, base):
        old = [kept_place[pl.ds(8 * g, 2)] for g in range(GROUP)]
        rows = [found[BLOCK * g : BLOCK * (g + 1)] for g in range(GROUP)]
        from_row = jnp.minimum(group, groups - 1) * GROUP
        for g in range(GROUP):
            for at in range(BLOCK):
                found[pl.ds(BLOCK * g + at, 1)] = table[lines[from_row + g, at]]
        last_row = jnp.maximum(group - 1, 0) * GROUP
        ids_row = jnp.minimum(last_row, (groups - 1) * GROUP)
        for g in range(GROUP):
            valid = (group >= 1) & (last_row + g < blocks)
            lane_row = (ids[pl.ds(ids_row + g, 1)] & 127).astype(jnp.float32)
            lane = jnp.sum(jnp.where(diagonal, lane_row, 0.0), axis=1, keepdims=True)
            kept = jnp.where(square_col == lane.astype(jnp.int32), rows[g], 0)
            total = jnp.sum(kept.astype(jnp.float32), axis=1, keepdims=True)
            position = jnp.sum(jnp.where(diagonal, total, 0.0), axis=0, keepdims=True)
            position = position.astype(jnp.int32)
            owner, row, cold, member = spread(position, valid)
            counted = jnp.dot(
                member.astype(jnp.bfloat16), before, preferred_element_type=jnp.float32
            )
            rank = jnp.sum((counted[:, :BLOCK] + base) * member, axis=0, keepdims=True)
            slot = jnp.minimum(rank.astype(jnp.int32), CAP - 1)
            place = jnp.where(
                cold,
                owner * CAP + slot,
                OWNERS * CAP + owner * HOT_DEV + jnp.minimum(row, HOT_DEV - 1),
            )
            place_out[pl.ds(last_row + g, 1)] = place
            kept_place[pl.ds(8 * g, 1)] = position
            kept_place[pl.ds(8 * g + 1, 1)] = slot
            base = base + counted[:, BLOCK:]
        old_group = (group - 2) * GROUP
        update = request[...]
        for g in range(GROUP):
            valid = (group >= 2) & (old_group + g < blocks)
            _, row, _, member = spread(old[g][0:1], valid)
            pick = (square_row == old[g][1:2]).astype(jnp.bfloat16)
            high = member * lax.shift_right_logical(row, 8).astype(jnp.float32)
            low = member * (row & 255).astype(jnp.float32)
            both = jnp.concatenate([high, low], axis=0).astype(jnp.bfloat16)
            update = update + lax.dot_general(
                both, pick, (((1,), (1,)), ((), ())), preferred_element_type=jnp.float32
            )
        request[...] = update
        return base

    lax.fori_loop(0, groups + 2, step, jnp.zeros((OWNERS, BLOCK), jnp.float32))
    table_out = request[0:OWNERS] * 256.0 + request[OWNERS:]
    request_out[...] = table_out.astype(jnp.int32)


def plan(ids, partition_map):
    blocks = ids.shape[0] * ids.shape[1] // BLOCK
    padded = -(-blocks // GROUP) * GROUP
    ids = jnp.pad(ids.reshape(blocks, BLOCK), ((0, padded - blocks), (0, 0)))
    lines = lax.shift_right_logical(ids, 7)
    return pl.pallas_call(
        functools.partial(plan_kernel, blocks),
        out_shape=[
            jax.ShapeDtypeStruct((OWNERS, BLOCK), jnp.int32),
            jax.ShapeDtypeStruct((padded + GROUP, BLOCK), jnp.int32),
        ],
        in_specs=[
            pl.BlockSpec(memory_space=pltpu.SMEM),
            pl.BlockSpec(memory_space=pltpu.VMEM),
            pl.BlockSpec(memory_space=pltpu.VMEM),
        ],
        out_specs=[pl.BlockSpec(memory_space=pltpu.VMEM)] * 2,
        scratch_shapes=[
            pltpu.VMEM((GROUP * BLOCK, BLOCK), jnp.int32),
            pltpu.VMEM((GROUP * 8, BLOCK), jnp.int32),
            pltpu.VMEM((BLOCK, BLOCK), jnp.float32),
        ],
        compiler_params=pltpu.CompilerParams(vmem_limit_bytes=VMEM_LIMIT),
        name="plan",
    )(lines, ids, partition_map.reshape(-1, 1, BLOCK))


def fetch_kernel(request, features, returned, wide, picked, sending, arrived, wanted,
                 ask_send, ask_recv, row_send, row_recv, local_sem):
    dom = lax.axis_index("dom")
    y = lax.axis_index("rep")

    def peer(step):
        return lax.rem(dom + step, OWNERS)

    barrier = pltpu.get_barrier_semaphore()

    @pl.loop(1, OWNERS)
    def _(step):
        pl.semaphore_signal(barrier, inc=1, device_id=(peer(step), y), device_id_type=MESH)

    wide[...] = features[...].astype(jnp.float32)
    pl.semaphore_wait(barrier, OWNERS - 1)

    def ask(step):
        return pltpu.make_async_remote_copy(
            src_ref=request.at[peer(step)], dst_ref=arrived.at[step], send_sem=ask_send.at[step],
            recv_sem=ask_recv.at[step], device_id=(peer(step), y), device_id_type=MESH,
        )

    @pl.loop(1, OWNERS)
    def _(step):
        ask(step).start()

    arrived[0] = request[dom]

    @pl.loop(1, OWNERS)
    def _(step):
        ask(step).wait()

    down = pltpu.make_async_copy(arrived, wanted, local_sem)
    down.start()
    down.wait()

    def asker(step):
        return lax.rem(dom - step + OWNERS, OWNERS)

    def gather(step):
        for at in range(CAP):
            picked[pl.ds(at, 1)] = wide[pl.ds(wanted[step, 0, at], 1)]
        return picked[0:CAP].astype(jnp.bfloat16)

    def answer(step):
        return pltpu.make_async_remote_copy(
            src_ref=sending.at[step], dst_ref=returned.at[dom], send_sem=row_send.at[step],
            recv_sem=row_recv.at[step], device_id=(asker(step), y), device_id_type=MESH,
        )

    sending[1] = gather(1)

    @pl.loop(2, OWNERS)
    def _(step):
        sending[step] = gather(step)
        answer(step - 1).start()

    returned[dom] = gather(0)
    answer(OWNERS - 1).start()

    @pl.loop(1, OWNERS)
    def _(step):
        answer(step).wait()


def fetch(request, features):
    vmem = pl.BlockSpec(memory_space=pltpu.VMEM)
    dma = pltpu.SemaphoreType.DMA
    return pl.pallas_call(
        fetch_kernel,
        out_shape=jax.ShapeDtypeStruct((OWNERS, CAP, 128), jnp.bfloat16),
        in_specs=[vmem, vmem],
        out_specs=vmem,
        scratch_shapes=[
            pltpu.VMEM(features.shape, jnp.float32),
            pltpu.VMEM((88, 128), jnp.float32),
            pltpu.VMEM((OWNERS, CAP, 128), jnp.bfloat16),
            pltpu.VMEM((OWNERS, 1, BLOCK), jnp.int32),
            pltpu.SMEM((OWNERS, 1, BLOCK), jnp.int32),
            dma((OWNERS,)), dma((OWNERS,)), dma((OWNERS,)), dma((OWNERS,)), dma,
        ],
        compiler_params=pltpu.CompilerParams(
            collective_id=2, has_side_effects=True, vmem_limit_bytes=VMEM_LIMIT
        ),
        name="fetch",
    )(request.reshape(OWNERS, 1, BLOCK), features)


def dot(a, b, dims):
    return lax.dot_general(a, b, (dims, ((), ())), preferred_element_type=jnp.float32)


def gelu_parts(x):
    scale = 0.7978845608028654
    square = x * x
    t = jnp.tanh(scale * x * (1.0 + 0.044715 * square))
    half = 0.5 * (1.0 + t)
    slope = half + 0.5 * x * (1.0 - t * t) * (scale * (1.0 + 3.0 * 0.044715 * square))
    return x * half, slope


def sage_kernel(place, returned, hubs, labels, self_one, neigh_one, bias_one, self_two, neigh_two,
                bias_two, loss_out, packed, table, rows, far):
    for owner in range(OWNERS):
        table[CAP * owner : CAP * (owner + 1)] = returned[owner].astype(jnp.float32)
    table[CAP * OWNERS :] = hubs[...].astype(jnp.float32)

    @pl.loop(0, (SEEDS + HOPS) // 64)
    def _(block):
        first = pl.multiple_of(block * 64, 64)
        for at in range(64):
            rows[pl.ds(first + at, 1)] = table[pl.ds(place[first + at], 1)]

    @pl.loop(0, HOPS // CHUNK)
    def _(block):
        first = pl.multiple_of(block * CHUNK, CHUNK)
        for at in range(CHUNK):
            value = None
            for k in range(FAN2):
                row = table[pl.ds(place[first + (SEEDS + HOPS + k * HOPS + at)], 1)]
                value = row if value is None else value + row
            far[pl.ds(first + at, 1)] = value

    seed_rows = rows[0:SEEDS].astype(jnp.bfloat16)
    hop_rows = rows[SEEDS:].astype(jnp.bfloat16)
    far_mean = (far[...] * (1.0 / FAN2)).astype(jnp.bfloat16)
    seed_sum = rows[SEEDS : 2 * SEEDS]
    for f in range(1, FAN1):
        seed_sum = seed_sum + rows[SEEDS * (f + 1) : SEEDS * (f + 2)]
    seed_mean = (seed_sum * (1.0 / FAN1)).astype(jnp.bfloat16)

    own = jnp.concatenate([seed_rows, hop_rows], axis=0)
    near = jnp.concatenate([seed_mean, far_mean], axis=0)
    both = jnp.concatenate([own, near], axis=1)
    weight = jnp.concatenate([self_one[...], neigh_one[...]], axis=0)
    pre = dot(both, weight, ((1,), (0,))) + bias_one[...]
    act, slope = gelu_parts(pre)
    hid_seed = act[0:SEEDS].astype(jnp.bfloat16)
    hop_sum = act[SEEDS : 2 * SEEDS]
    for f in range(1, FAN1):
        hop_sum = hop_sum + act[SEEDS * (f + 1) : SEEDS * (f + 2)]
    hop_mean = (hop_sum * (1.0 / FAN1)).astype(jnp.bfloat16)

    logits = (
        dot(hid_seed, self_two[...], ((1,), (1,)))
        + dot(hop_mean, neigh_two[...], ((1,), (1,)))
        + bias_two[...]
    )
    shifted = logits - jnp.max(logits, axis=1, keepdims=True)
    exps = jnp.exp(shifted)
    sums = jnp.sum(exps, axis=1, keepdims=True)
    log_probs = shifted - jnp.log(sums)
    small_row = lax.broadcasted_iota(jnp.int32, (SEEDS, SEEDS), 0)
    small_col = lax.broadcasted_iota(jnp.int32, (SEEDS, SEEDS), 1)
    label = jnp.sum(
        jnp.where(small_row == small_col, labels[...].astype(jnp.float32), 0.0),
        axis=1, keepdims=True,
    ).astype(jnp.int32)
    target = lax.broadcasted_iota(jnp.int32, (SEEDS, CLASSES), 1) == label
    picked = jnp.sum(jnp.where(target, log_probs, 0.0), axis=1, keepdims=True)
    loss_out[...] = -jnp.sum(
        jnp.where(small_row == small_col, picked, 0.0), axis=0, keepdims=True
    )
    d_logits32 = (jnp.exp(log_probs) - target.astype(jnp.float32)) * (1.0 / SEEDS)
    d_logits = d_logits32.astype(jnp.bfloat16)

    zeros = jnp.zeros((8, 128), jnp.float32)
    packed[512 + 168 : 512 + 176] = zeros
    packed[688 + 168 : 688 + 176] = zeros
    packed[864 + 168 : 864 + 176] = zeros
    packed[1040 + 168 : 1040 + 176] = zeros
    packed[1216:] = jnp.zeros((ROWS - 1216, 128), jnp.float32)
    grad_self_two = dot(d_logits, hid_seed, ((0,), (0,)))
    packed[512:684] = grad_self_two[:, :128]
    packed[688:860] = grad_self_two[:, 128:]
    grad_neigh_two = dot(d_logits, hop_mean, ((0,), (0,)))
    packed[864:1036] = grad_neigh_two[:, :128]
    packed[1040:1212] = grad_neigh_two[:, 128:]
    grad_bias_two = jnp.sum(d_logits32, axis=0, keepdims=True)
    packed[1218:1219] = grad_bias_two[:, :128]
    packed[1219:1220, 0 : CLASSES - 128] = grad_bias_two[:, 128:]

    d_hid_seed = dot(d_logits, self_two[...], ((1,), (0,)))
    d_hop_mean = dot(d_logits, neigh_two[...], ((1,), (0,))) * (1.0 / FAN1)
    d_hid = jnp.concatenate([d_hid_seed] + [d_hop_mean] * FAN1, axis=0)
    d_pre32 = d_hid * slope
    d_pre = d_pre32.astype(jnp.bfloat16)
    grad_one = dot(both, d_pre, ((0,), (0,)))
    packed[0:128] = grad_one[0:128, :128]
    packed[128:256] = grad_one[0:128, 128:]
    packed[256:384] = grad_one[128:256, :128]
    packed[384:512] = grad_one[128:256, 128:]
    grad_bias_one = jnp.sum(d_pre32, axis=0, keepdims=True)
    packed[1216:1217] = grad_bias_one[:, :128]
    packed[1217:1218] = grad_bias_one[:, 128:]


def sage(place, returned, hubs, labels, self_one, neigh_one, bias_one, self_two, neigh_two, bias_two):
    vmem = pl.BlockSpec(memory_space=pltpu.VMEM)
    loss, packed = pl.pallas_call(
        sage_kernel,
        out_shape=[
            jax.ShapeDtypeStruct((1, SEEDS), jnp.float32),
            jax.ShapeDtypeStruct((ROWS, 128), jnp.float32),
        ],
        in_specs=[pl.BlockSpec(memory_space=pltpu.SMEM)] + [vmem] * 9,
        out_specs=[vmem, vmem],
        scratch_shapes=[
            pltpu.VMEM((OWNERS * (CAP + HOT_DEV), 128), jnp.float32),
            pltpu.VMEM((SEEDS + HOPS, 128), jnp.float32),
            pltpu.VMEM((HOPS, 128), jnp.float32),
        ],
        compiler_params=pltpu.CompilerParams(vmem_limit_bytes=VMEM_LIMIT),
        name="sage",
    )(
        place.reshape(-1), returned, hubs, labels[None, :], self_one, neigh_one, bias_one[None, :],
        self_two.T, neigh_two.T, bias_two[None, :],
    )
    return loss.reshape(-1), packed


def unpack_kernel(packed, self_one, neigh_one, bias_one, self_two, neigh_two, bias_two):
    self_one[:, :128] = packed[0:128]
    self_one[:, 128:] = packed[128:256]
    neigh_one[:, :128] = packed[256:384]
    neigh_one[:, 128:] = packed[384:512]
    self_two[:, :128] = packed[512:684]
    self_two[:, 128:] = packed[688:860]
    neigh_two[:, :128] = packed[864:1036]
    neigh_two[:, 128:] = packed[1040:1212]
    bias_one[:, :128] = packed[1216:1217]
    bias_one[:, 128:] = packed[1217:1218]
    bias_two[:, :128] = packed[1218:1219]
    bias_two[:, 128:] = packed[1219:1220, 0 : CLASSES - 128]


def unpack(packed):
    shapes = ((128, 256), (128, 256), (1, 256), (CLASSES, 256), (CLASSES, 256), (1, CLASSES))
    self_one, neigh_one, bias_one, self_two, neigh_two, bias_two = pl.pallas_call(
        unpack_kernel,
        out_shape=[jax.ShapeDtypeStruct(shape, jnp.float32) for shape in shapes],
        name="unpack",
    )(packed)
    return self_one, neigh_one, bias_one.reshape(-1), self_two.T, neigh_two.T, bias_two.reshape(-1)


def sum_kernel(mine, total, other, send_z, recv_z, send_p, recv_p, core_send, core_recv,
               z_send, z_recv, p_send, p_recv, g_send, g_recv, h_send, h_recv):
    dom = lax.axis_index("dom")
    y = lax.axis_index("rep")
    core = lax.rem(dom, 2)
    z = lax.rem(lax.div(dom, 2), 8)
    x = lax.div(dom, 16)

    def device(to_x, to_y, to_z, to_core):
        return ((to_x * 8 + to_z) * 2 + to_core, to_y)

    partner = device(x, y, z, 1 - core)

    def z_peer(step):
        return device(x, y, lax.rem(z + step, 8), core)

    def plane_peer(step):
        place = lax.rem(x * 4 + y + step, 16)
        return device(lax.div(place, 4), lax.rem(place, 4), z, core)

    barrier = pltpu.get_barrier_semaphore()
    pl.semaphore_signal(barrier, inc=1, device_id=partner, device_id_type=MESH)

    @pl.loop(1, 8)
    def _(step):
        pl.semaphore_signal(barrier, inc=1, device_id=z_peer(step), device_id_type=MESH)

    @pl.loop(1, 16)
    def _(step):
        pl.semaphore_signal(barrier, inc=1, device_id=plane_peer(step), device_id_type=MESH)

    pl.semaphore_wait(barrier, 23)

    swap = pltpu.make_async_remote_copy(
        src_ref=mine.at[1 - core], dst_ref=other, send_sem=core_send, recv_sem=core_recv,
        device_id=partner, device_id_type=MESH,
    )
    swap.start()
    swap.wait()

    @pl.loop(0, 8)
    def _(part):
        send_z[part] = (mine[core, part] + other[part]).astype(jnp.bfloat16)

    def z_copy(step):
        to_z = lax.rem(z + step, 8)
        return pltpu.make_async_remote_copy(
            src_ref=send_z.at[to_z], dst_ref=recv_z.at[step], send_sem=z_send.at[step],
            recv_sem=z_recv.at[step], device_id=z_peer(step), device_id_type=MESH,
        )

    @pl.loop(1, 8)
    def _(step):
        z_copy(step).start()

    kept = mine[core, z] + other[z]

    @pl.loop(1, 8)
    def _(step):
        z_copy(step).wait()

    def add_z(step, value):
        return value + recv_z[step].astype(jnp.float32)

    kept = lax.fori_loop(1, 8, add_z, kept)
    send_p[...] = kept.astype(jnp.bfloat16)

    def plane_copy(step):
        return pltpu.make_async_remote_copy(
            src_ref=send_p, dst_ref=recv_p.at[step], send_sem=p_send.at[step],
            recv_sem=p_recv.at[step], device_id=plane_peer(step), device_id_type=MESH,
        )

    @pl.loop(1, 16)
    def _(step):
        plane_copy(step).start()

    recv_p[0] = send_p[...]

    @pl.loop(1, 16)
    def _(step):
        plane_copy(step).wait()

    def add_plane(place, value):
        step = lax.rem(x * 4 + y - place + 16, 16)
        return value + recv_p[step].astype(jnp.float32)

    total[core, z] = lax.fori_loop(0, 16, add_plane, jnp.zeros_like(kept))

    def z_back(step):
        return pltpu.make_async_remote_copy(
            src_ref=total.at[core, z], dst_ref=total.at[core, z], send_sem=g_send.at[step],
            recv_sem=g_recv.at[step], device_id=z_peer(step), device_id_type=MESH,
        )

    def hand_on(step):
        of_z = lax.rem(z - step + 8, 8)
        return pltpu.make_async_remote_copy(
            src_ref=total.at[core, of_z], dst_ref=total.at[core, of_z], send_sem=h_send.at[step],
            recv_sem=h_recv.at[step], device_id=partner, device_id_type=MESH,
        )

    @pl.loop(1, 8)
    def _(step):
        z_back(step).start()

    hand_on(0).start()

    @pl.loop(1, 8)
    def _(step):
        z_back(step).wait()
        hand_on(step).start()

    @pl.loop(0, 8)
    def _(step):
        hand_on(step).wait()


def sum_all(packed):
    vmem = pl.BlockSpec(memory_space=pltpu.VMEM)
    dma = pltpu.SemaphoreType.DMA
    return pl.pallas_call(
        sum_kernel,
        out_shape=jax.ShapeDtypeStruct((2, 8, PIECE, 128), jnp.float32),
        in_specs=[vmem],
        out_specs=vmem,
        scratch_shapes=[
            pltpu.VMEM((8, PIECE, 128), jnp.float32),
            pltpu.VMEM((8, PIECE, 128), jnp.bfloat16),
            pltpu.VMEM((8, PIECE, 128), jnp.bfloat16),
            pltpu.VMEM((PIECE, 128), jnp.bfloat16),
            pltpu.VMEM((16, PIECE, 128), jnp.bfloat16),
            dma, dma, dma((8,)), dma((8,)), dma((16,)), dma((16,)),
            dma((8,)), dma((8,)), dma((8,)), dma((8,)),
        ],
        compiler_params=pltpu.CompilerParams(collective_id=1, has_side_effects=True),
        name="sum_all",
    )(packed)


def shards(
    features,
    partition_map,
    seed_ids,
    hop1_ids,
    hop2_ids,
    labels,
    self_one,
    neigh_one,
    bias_one,
    self_two,
    neigh_two,
    bias_two,
):
    ids = jnp.concatenate(
        [
            seed_ids[None, :],
            hop1_ids.T,
            hop2_ids.transpose(2, 1, 0).reshape(FAN2 * FAN1, SEEDS),
        ],
        axis=0,
    )
    hubs = lax.all_gather(features[:HOT_DEV], "dom", axis=0, tiled=True)
    request, place = plan(ids, partition_map)
    returned = fetch(request, features)
    seed_loss, packed = sage(
        place, returned, hubs, labels, self_one, neigh_one, bias_one, self_two, neigh_two, bias_two
    )
    total = sum_all(packed.reshape(2, 8, PIECE, 128))
    return (seed_loss, *unpack(total.reshape(ROWS, 128)))


def solution(mesh):
    return jax.shard_map(
        shards,
        mesh=mesh,
        in_specs=(
            P("dom", None),
            P(),
            P(("dom", "rep")),
            P(("dom", "rep"), None),
            P(("dom", "rep"), None, None),
            P(("dom", "rep")),
            P(),
            P(),
            P(),
            P(),
            P(),
            P(),
        ),
        out_specs=(P(("dom", "rep")), P(), P(), P(), P(), P(), P()),
        check_vma=False,
    )
```

```python
import functools

import jax
import jax.numpy as jnp
from jax import lax
from jax.experimental import pallas as pl
from jax.experimental.pallas import tpu as pltpu
from jax.sharding import PartitionSpec as P

MESH = pl.DeviceIdType.MESH
HOT_DEV = 256
NODE_DEV = 8192
OWNERS = 64
CAP = 83
SEEDS = 64
FAN1 = 15
FAN2 = 10
HOPS = SEEDS * FAN1
CLASSES = 172
BLOCK = 128
GROUP = 4
CHUNK = 16
ROWS = 1280
PIECE = ROWS // 16
VMEM_LIMIT = 60 * 1024 * 1024


def plan_kernel(blocks, lines, ids, table, request_out, place_out, found, kept_place, request):
    square_row = lax.broadcasted_iota(jnp.int32, (BLOCK, BLOCK), 0)
    square_col = lax.broadcasted_iota(jnp.int32, (BLOCK, BLOCK), 1)
    diagonal = square_row == square_col
    before = jnp.concatenate(
        [(square_row < square_col).astype(jnp.bfloat16), jnp.ones((BLOCK, BLOCK), jnp.bfloat16)],
        axis=1,
    )
    owner_row = lax.broadcasted_iota(jnp.int32, (OWNERS, BLOCK), 0)
    groups = ids.shape[0] // GROUP
    found[...] = jnp.zeros_like(found)
    kept_place[...] = jnp.zeros_like(kept_place)
    request[...] = jnp.zeros_like(request)

    def spread(position, valid):
        owner = lax.shift_right_logical(position, 13)
        row = position & (NODE_DEV - 1)
        cold = (row >= HOT_DEV) & valid
        member = ((owner_row == owner) & cold).astype(jnp.float32)
        return owner, row, cold, member

    def step(group, base):
        old = [kept_place[pl.ds(8 * g, 2)] for g in range(GROUP)]
        rows = [found[BLOCK * g : BLOCK * (g + 1)] for g in range(GROUP)]
        from_row = jnp.minimum(group, groups - 1) * GROUP
        for g in range(GROUP):
            for at in range(BLOCK):
                found[pl.ds(BLOCK * g + at, 1)] = table[lines[from_row + g, at]]
        last_row = jnp.maximum(group - 1, 0) * GROUP
        ids_row = jnp.minimum(last_row, (groups - 1) * GROUP)
        for g in range(GROUP):
            valid = (group >= 1) & (last_row + g < blocks)
            lane_row = (ids[pl.ds(ids_row + g, 1)] & 127).astype(jnp.float32)
            lane = jnp.sum(jnp.where(diagonal, lane_row, 0.0), axis=1, keepdims=True)
            kept = jnp.where(square_col == lane.astype(jnp.int32), rows[g], 0)
            total = jnp.sum(kept.astype(jnp.float32), axis=1, keepdims=True)
            position = jnp.sum(jnp.where(diagonal, total, 0.0), axis=0, keepdims=True)
            position = position.astype(jnp.int32)
            owner, row, cold, member = spread(position, valid)
            counted = jnp.dot(
                member.astype(jnp.bfloat16), before, preferred_element_type=jnp.float32
            )
            rank = jnp.sum((counted[:, :BLOCK] + base) * member, axis=0, keepdims=True)
            slot = jnp.minimum(rank.astype(jnp.int32), CAP - 1)
            hub_place = (
                (owner & 1) * (OWNERS // 2 * HOT_DEV)
                + lax.shift_right_logical(owner, 1) * HOT_DEV
                + jnp.minimum(row, HOT_DEV - 1)
            )
            place = jnp.where(cold, owner * CAP + slot, OWNERS * CAP + hub_place)
            place_out[pl.ds(last_row + g, 1)] = place
            kept_place[pl.ds(8 * g, 1)] = position
            kept_place[pl.ds(8 * g + 1, 1)] = slot
            base = base + counted[:, BLOCK:]
        old_group = (group - 2) * GROUP
        update = request[...]
        for g in range(GROUP):
            valid = (group >= 2) & (old_group + g < blocks)
            _, row, _, member = spread(old[g][0:1], valid)
            pick = (square_row == old[g][1:2]).astype(jnp.bfloat16)
            high = member * lax.shift_right_logical(row, 8).astype(jnp.float32)
            low = member * (row & 255).astype(jnp.float32)
            both = jnp.concatenate([high, low], axis=0).astype(jnp.bfloat16)
            update = update + lax.dot_general(
                both, pick, (((1,), (1,)), ((), ())), preferred_element_type=jnp.float32
            )
        request[...] = update
        return base

    lax.fori_loop(0, groups + 2, step, jnp.zeros((OWNERS, BLOCK), jnp.float32))
    table_out = request[0:OWNERS] * 256.0 + request[OWNERS:]
    request_out[...] = table_out.astype(jnp.int32)


def plan(ids, partition_map):
    blocks = ids.shape[0] * ids.shape[1] // BLOCK
    padded = -(-blocks // GROUP) * GROUP
    ids = jnp.pad(ids.reshape(blocks, BLOCK), ((0, padded - blocks), (0, 0)))
    lines = lax.shift_right_logical(ids, 7)
    return pl.pallas_call(
        functools.partial(plan_kernel, blocks),
        out_shape=[
            jax.ShapeDtypeStruct((OWNERS, BLOCK), jnp.int32),
            jax.ShapeDtypeStruct((padded + GROUP, BLOCK), jnp.int32),
        ],
        in_specs=[
            pl.BlockSpec(memory_space=pltpu.SMEM),
            pl.BlockSpec(memory_space=pltpu.VMEM),
            pl.BlockSpec(memory_space=pltpu.VMEM),
        ],
        out_specs=[pl.BlockSpec(memory_space=pltpu.VMEM)] * 2,
        scratch_shapes=[
            pltpu.VMEM((GROUP * BLOCK, BLOCK), jnp.int32),
            pltpu.VMEM((GROUP * 8, BLOCK), jnp.int32),
            pltpu.VMEM((BLOCK, BLOCK), jnp.float32),
        ],
        compiler_params=pltpu.CompilerParams(vmem_limit_bytes=VMEM_LIMIT),
        name="plan",
    )(lines, ids, partition_map.reshape(-1, 1, BLOCK))


def fetch_kernel(request, features, returned, hubs, wide, picked, sending, arrived, wanted,
                 ask_send, ask_recv, row_send, row_recv, local_sem, z_send, z_recv, x_send, x_recv,
                 core_send, core_recv):
    dom = lax.axis_index("dom")
    y = lax.axis_index("rep")
    core = lax.rem(dom, 2)
    z = lax.rem(lax.div(dom, 2), 8)
    x = lax.div(dom, 16)

    def peer(step):
        return lax.rem(dom + step, OWNERS)

    def at_z(offset):
        return lax.rem(z + offset + 8, 8)

    def at_x(offset):
        return lax.rem(x + offset + 4, 4)

    barrier = pltpu.get_barrier_semaphore()

    @pl.loop(1, OWNERS)
    def _(step):
        pl.semaphore_signal(barrier, inc=1, device_id=(peer(step), y), device_id_type=MESH)

    hubs[core, x, z] = features[0:HOT_DEV]
    wide[...] = features[...].astype(jnp.float32)
    pl.semaphore_wait(barrier, OWNERS - 1)

    def ask(step):
        return pltpu.make_async_remote_copy(
            src_ref=request.at[peer(step)], dst_ref=arrived.at[step], send_sem=ask_send.at[step],
            recv_sem=ask_recv.at[step], device_id=(peer(step), y), device_id_type=MESH,
        )

    def hub_z(step, way):
        place = hubs.at[core, x, at_z(-way * (step - 1))]
        if step == 4:
            place = place.at[pl.ds(0 if way > 0 else HOT_DEV // 2, HOT_DEV // 2)]
        slot = step - 1 + (0 if way > 0 else 4)
        return pltpu.make_async_remote_copy(
            src_ref=place, dst_ref=place, send_sem=z_send.at[slot], recv_sem=z_recv.at[slot],
            device_id=((x * 8 + at_z(way)) * 2 + core, y), device_id_type=MESH,
        )

    def hub_x(offset, way, hop):
        place = hubs.at[core, at_x(-way * hop), at_z(offset)]
        slot = (offset + 3) + (0 if way > 0 else 8) + 16 * hop
        return pltpu.make_async_remote_copy(
            src_ref=place, dst_ref=place, send_sem=x_send.at[slot], recv_sem=x_recv.at[slot],
            device_id=((at_x(way) * 8 + z) * 2 + core, y), device_id_type=MESH,
        )

    def hub_core(offset):
        place = hubs.at[core, at_x(offset)]
        return pltpu.make_async_remote_copy(
            src_ref=place, dst_ref=place, send_sem=core_send.at[offset + 1],
            recv_sem=core_recv.at[offset + 1],
            device_id=((x * 8 + z) * 2 + 1 - core, y), device_id_type=MESH,
        )

    def turn(step):
        for way in (1, -1):
            hub_z(step, way).wait()
        if step < 4:
            for way in (1, -1):
                hub_z(step + 1, way).start()
        for offset in (-step, step) if step < 4 else (4,):
            for way in (1, -1):
                hub_x(offset, way, 0).start()

    @pl.loop(1, OWNERS)
    def _(step):
        ask(step).start()

    for way in (1, -1):
        hub_z(1, way).start()
    for way in (1, -1):
        hub_x(0, way, 0).start()

    arrived[0] = request[dom]

    @pl.loop(1, OWNERS)
    def _(step):
        ask(step).wait()

    down = pltpu.make_async_copy(arrived, wanted, local_sem)
    down.start()
    turn(1)
    down.wait()

    def asker(step):
        return lax.rem(dom - step + OWNERS, OWNERS)

    def gather(step):
        for at in range(CAP):
            picked[pl.ds(at, 1)] = wide[pl.ds(wanted[step, 0, at], 1)]
        return picked[0:CAP].astype(jnp.bfloat16)

    def answer(step):
        return pltpu.make_async_remote_copy(
            src_ref=sending.at[step], dst_ref=returned.at[dom], send_sem=row_send.at[step],
            recv_sem=row_recv.at[step], device_id=(asker(step), y), device_id_type=MESH,
        )

    sending[1] = gather(1)

    def answers(first, last):
        @pl.loop(first, last)
        def _(step):
            sending[step] = gather(step)
            answer(step - 1).start()

    answers(2, 16)
    turn(2)
    answers(16, 32)
    turn(3)
    answers(32, 48)
    turn(4)
    answers(48, OWNERS)
    returned[dom] = gather(0)
    answer(OWNERS - 1).start()

    hub_core(0).start()
    order = (0, -1, 1, -2, 2, -3, 3, 4)
    for offset in order:
        for way in (1, -1):
            hub_x(offset, way, 0).wait()
        hub_x(offset, 1 if offset <= 0 else -1, 1).start()
    hub_core(-1).start()
    hub_core(1).start()
    for offset in order:
        hub_x(offset, 1 if offset <= 0 else -1, 1).wait()
    hub_core(2).start()

    @pl.loop(1, OWNERS)
    def _(step):
        answer(step).wait()

    for offset in (0, -1, 1, 2):
        hub_core(offset).wait()


def fetch(request, features):
    vmem = pl.BlockSpec(memory_space=pltpu.VMEM)
    dma = pltpu.SemaphoreType.DMA
    return pl.pallas_call(
        fetch_kernel,
        out_shape=[
            jax.ShapeDtypeStruct((OWNERS, CAP, 128), jnp.bfloat16),
            jax.ShapeDtypeStruct((2, 4, 8, HOT_DEV, 128), jnp.bfloat16),
        ],
        in_specs=[vmem, vmem],
        out_specs=[vmem, vmem],
        scratch_shapes=[
            pltpu.VMEM(features.shape, jnp.float32),
            pltpu.VMEM((88, 128), jnp.float32),
            pltpu.VMEM((OWNERS, CAP, 128), jnp.bfloat16),
            pltpu.VMEM((OWNERS, 1, BLOCK), jnp.int32),
            pltpu.SMEM((OWNERS, 1, BLOCK), jnp.int32),
            dma((OWNERS,)), dma((OWNERS,)), dma((OWNERS,)), dma((OWNERS,)), dma,
            dma((8,)), dma((8,)), dma((32,)), dma((32,)), dma((4,)), dma((4,)),
        ],
        compiler_params=pltpu.CompilerParams(
            collective_id=2, has_side_effects=True, vmem_limit_bytes=VMEM_LIMIT
        ),
        name="fetch",
    )(request.reshape(OWNERS, 1, BLOCK), features)


def dot(a, b, dims):
    return lax.dot_general(a, b, (dims, ((), ())), preferred_element_type=jnp.float32)


def gelu_parts(x):
    scale = 0.7978845608028654
    square = x * x
    t = jnp.tanh(scale * x * (1.0 + 0.044715 * square))
    half = 0.5 * (1.0 + t)
    slope = half + 0.5 * x * (1.0 - t * t) * (scale * (1.0 + 3.0 * 0.044715 * square))
    return x * half, slope


def sage_kernel(place, returned, hubs, labels, self_one, neigh_one, bias_one, self_two, neigh_two,
                bias_two, loss_out, packed, table, rows, far):
    for owner in range(OWNERS):
        table[CAP * owner : CAP * (owner + 1)] = returned[owner].astype(jnp.float32)
    table[CAP * OWNERS :] = hubs[...].astype(jnp.float32)

    @pl.loop(0, (SEEDS + HOPS) // 64)
    def _(block):
        first = pl.multiple_of(block * 64, 64)
        for at in range(64):
            rows[pl.ds(first + at, 1)] = table[pl.ds(place[first + at], 1)]

    @pl.loop(0, HOPS // CHUNK)
    def _(block):
        first = pl.multiple_of(block * CHUNK, CHUNK)
        for at in range(CHUNK):
            value = None
            for k in range(FAN2):
                row = table[pl.ds(place[first + (SEEDS + HOPS + k * HOPS + at)], 1)]
                value = row if value is None else value + row
            far[pl.ds(first + at, 1)] = value

    seed_rows = rows[0:SEEDS].astype(jnp.bfloat16)
    hop_rows = rows[SEEDS:].astype(jnp.bfloat16)
    far_mean = (far[...] * (1.0 / FAN2)).astype(jnp.bfloat16)
    seed_sum = rows[SEEDS : 2 * SEEDS]
    for f in range(1, FAN1):
        seed_sum = seed_sum + rows[SEEDS * (f + 1) : SEEDS * (f + 2)]
    seed_mean = (seed_sum * (1.0 / FAN1)).astype(jnp.bfloat16)

    own = jnp.concatenate([seed_rows, hop_rows], axis=0)
    near = jnp.concatenate([seed_mean, far_mean], axis=0)
    both = jnp.concatenate([own, near], axis=1)
    weight = jnp.concatenate([self_one[...], neigh_one[...]], axis=0)
    pre = dot(both, weight, ((1,), (0,))) + bias_one[...]
    act, slope = gelu_parts(pre)
    hid_seed = act[0:SEEDS].astype(jnp.bfloat16)
    hop_sum = act[SEEDS : 2 * SEEDS]
    for f in range(1, FAN1):
        hop_sum = hop_sum + act[SEEDS * (f + 1) : SEEDS * (f + 2)]
    hop_mean = (hop_sum * (1.0 / FAN1)).astype(jnp.bfloat16)

    logits = (
        dot(hid_seed, self_two[...], ((1,), (1,)))
        + dot(hop_mean, neigh_two[...], ((1,), (1,)))
        + bias_two[...]
    )
    shifted = logits - jnp.max(logits, axis=1, keepdims=True)
    exps = jnp.exp(shifted)
    sums = jnp.sum(exps, axis=1, keepdims=True)
    log_probs = shifted - jnp.log(sums)
    small_row = lax.broadcasted_iota(jnp.int32, (SEEDS, SEEDS), 0)
    small_col = lax.broadcasted_iota(jnp.int32, (SEEDS, SEEDS), 1)
    label = jnp.sum(
        jnp.where(small_row == small_col, labels[...].astype(jnp.float32), 0.0),
        axis=1, keepdims=True,
    ).astype(jnp.int32)
    target = lax.broadcasted_iota(jnp.int32, (SEEDS, CLASSES), 1) == label
    picked = jnp.sum(jnp.where(target, log_probs, 0.0), axis=1, keepdims=True)
    loss_out[...] = -jnp.sum(
        jnp.where(small_row == small_col, picked, 0.0), axis=0, keepdims=True
    )
    d_logits32 = (jnp.exp(log_probs) - target.astype(jnp.float32)) * (1.0 / SEEDS)
    d_logits = d_logits32.astype(jnp.bfloat16)

    zeros = jnp.zeros((8, 128), jnp.float32)
    packed[512 + 168 : 512 + 176] = zeros
    packed[688 + 168 : 688 + 176] = zeros
    packed[864 + 168 : 864 + 176] = zeros
    packed[1040 + 168 : 1040 + 176] = zeros
    packed[1216:] = jnp.zeros((ROWS - 1216, 128), jnp.float32)
    grad_self_two = dot(d_logits, hid_seed, ((0,), (0,)))
    packed[512:684] = grad_self_two[:, :128]
    packed[688:860] = grad_self_two[:, 128:]
    grad_neigh_two = dot(d_logits, hop_mean, ((0,), (0,)))
    packed[864:1036] = grad_neigh_two[:, :128]
    packed[1040:1212] = grad_neigh_two[:, 128:]
    grad_bias_two = jnp.sum(d_logits32, axis=0, keepdims=True)
    packed[1218:1219] = grad_bias_two[:, :128]
    packed[1219:1220, 0 : CLASSES - 128] = grad_bias_two[:, 128:]

    d_hid_seed = dot(d_logits, self_two[...], ((1,), (0,)))
    d_hop_mean = dot(d_logits, neigh_two[...], ((1,), (0,))) * (1.0 / FAN1)
    d_hid = jnp.concatenate([d_hid_seed] + [d_hop_mean] * FAN1, axis=0)
    d_pre32 = d_hid * slope
    d_pre = d_pre32.astype(jnp.bfloat16)
    grad_one = dot(both, d_pre, ((0,), (0,)))
    packed[0:128] = grad_one[0:128, :128]
    packed[128:256] = grad_one[0:128, 128:]
    packed[256:384] = grad_one[128:256, :128]
    packed[384:512] = grad_one[128:256, 128:]
    grad_bias_one = jnp.sum(d_pre32, axis=0, keepdims=True)
    packed[1216:1217] = grad_bias_one[:, :128]
    packed[1217:1218] = grad_bias_one[:, 128:]


def sage(place, returned, hubs, labels, self_one, neigh_one, bias_one, self_two, neigh_two, bias_two):
    vmem = pl.BlockSpec(memory_space=pltpu.VMEM)
    loss, packed = pl.pallas_call(
        sage_kernel,
        out_shape=[
            jax.ShapeDtypeStruct((1, SEEDS), jnp.float32),
            jax.ShapeDtypeStruct((ROWS, 128), jnp.float32),
        ],
        in_specs=[pl.BlockSpec(memory_space=pltpu.SMEM)] + [vmem] * 9,
        out_specs=[vmem, vmem],
        scratch_shapes=[
            pltpu.VMEM((OWNERS * (CAP + HOT_DEV), 128), jnp.float32),
            pltpu.VMEM((SEEDS + HOPS, 128), jnp.float32),
            pltpu.VMEM((HOPS, 128), jnp.float32),
        ],
        compiler_params=pltpu.CompilerParams(vmem_limit_bytes=VMEM_LIMIT),
        name="sage",
    )(
        place.reshape(-1), returned, hubs, labels[None, :], self_one, neigh_one, bias_one[None, :],
        self_two.T, neigh_two.T, bias_two[None, :],
    )
    return loss.reshape(-1), packed


def unpack_kernel(packed, self_one, neigh_one, bias_one, self_two, neigh_two, bias_two):
    self_one[:, :128] = packed[0:128]
    self_one[:, 128:] = packed[128:256]
    neigh_one[:, :128] = packed[256:384]
    neigh_one[:, 128:] = packed[384:512]
    self_two[:, :128] = packed[512:684]
    self_two[:, 128:] = packed[688:860]
    neigh_two[:, :128] = packed[864:1036]
    neigh_two[:, 128:] = packed[1040:1212]
    bias_one[:, :128] = packed[1216:1217]
    bias_one[:, 128:] = packed[1217:1218]
    bias_two[:, :128] = packed[1218:1219]
    bias_two[:, 128:] = packed[1219:1220, 0 : CLASSES - 128]


def unpack(packed):
    shapes = ((128, 256), (128, 256), (1, 256), (CLASSES, 256), (CLASSES, 256), (1, CLASSES))
    self_one, neigh_one, bias_one, self_two, neigh_two, bias_two = pl.pallas_call(
        unpack_kernel,
        out_shape=[jax.ShapeDtypeStruct(shape, jnp.float32) for shape in shapes],
        name="unpack",
    )(packed)
    return self_one, neigh_one, bias_one.reshape(-1), self_two.T, neigh_two.T, bias_two.reshape(-1)


def sum_kernel(mine, total, other, send_z, recv_z, send_p, recv_p, core_send, core_recv,
               z_send, z_recv, p_send, p_recv, g_send, g_recv, h_send, h_recv):
    dom = lax.axis_index("dom")
    y = lax.axis_index("rep")
    core = lax.rem(dom, 2)
    z = lax.rem(lax.div(dom, 2), 8)
    x = lax.div(dom, 16)

    def device(to_x, to_y, to_z, to_core):
        return ((to_x * 8 + to_z) * 2 + to_core, to_y)

    partner = device(x, y, z, 1 - core)

    def z_peer(step):
        return device(x, y, lax.rem(z + step, 8), core)

    def plane_peer(step):
        place = lax.rem(x * 4 + y + step, 16)
        return device(lax.div(place, 4), lax.rem(place, 4), z, core)

    barrier = pltpu.get_barrier_semaphore()
    pl.semaphore_signal(barrier, inc=1, device_id=partner, device_id_type=MESH)

    @pl.loop(1, 8)
    def _(step):
        pl.semaphore_signal(barrier, inc=1, device_id=z_peer(step), device_id_type=MESH)

    @pl.loop(1, 16)
    def _(step):
        pl.semaphore_signal(barrier, inc=1, device_id=plane_peer(step), device_id_type=MESH)

    pl.semaphore_wait(barrier, 23)

    swap = pltpu.make_async_remote_copy(
        src_ref=mine.at[1 - core], dst_ref=other, send_sem=core_send, recv_sem=core_recv,
        device_id=partner, device_id_type=MESH,
    )
    swap.start()
    swap.wait()

    @pl.loop(0, 8)
    def _(part):
        send_z[part] = (mine[core, part] + other[part]).astype(jnp.bfloat16)

    def z_copy(step):
        to_z = lax.rem(z + step, 8)
        return pltpu.make_async_remote_copy(
            src_ref=send_z.at[to_z], dst_ref=recv_z.at[step], send_sem=z_send.at[step],
            recv_sem=z_recv.at[step], device_id=z_peer(step), device_id_type=MESH,
        )

    @pl.loop(1, 8)
    def _(step):
        z_copy(step).start()

    kept = mine[core, z] + other[z]

    @pl.loop(1, 8)
    def _(step):
        z_copy(step).wait()

    def add_z(step, value):
        return value + recv_z[step].astype(jnp.float32)

    kept = lax.fori_loop(1, 8, add_z, kept)
    send_p[...] = kept.astype(jnp.bfloat16)

    def plane_copy(step):
        return pltpu.make_async_remote_copy(
            src_ref=send_p, dst_ref=recv_p.at[step], send_sem=p_send.at[step],
            recv_sem=p_recv.at[step], device_id=plane_peer(step), device_id_type=MESH,
        )

    @pl.loop(1, 16)
    def _(step):
        plane_copy(step).start()

    recv_p[0] = send_p[...]

    @pl.loop(1, 16)
    def _(step):
        plane_copy(step).wait()

    def add_plane(place, value):
        step = lax.rem(x * 4 + y - place + 16, 16)
        return value + recv_p[step].astype(jnp.float32)

    total[core, z] = lax.fori_loop(0, 16, add_plane, jnp.zeros_like(kept))

    def z_back(step):
        return pltpu.make_async_remote_copy(
            src_ref=total.at[core, z], dst_ref=total.at[core, z], send_sem=g_send.at[step],
            recv_sem=g_recv.at[step], device_id=z_peer(step), device_id_type=MESH,
        )

    def hand_on(step):
        of_z = lax.rem(z - step + 8, 8)
        return pltpu.make_async_remote_copy(
            src_ref=total.at[core, of_z], dst_ref=total.at[core, of_z], send_sem=h_send.at[step],
            recv_sem=h_recv.at[step], device_id=partner, device_id_type=MESH,
        )

    @pl.loop(1, 8)
    def _(step):
        z_back(step).start()

    hand_on(0).start()

    @pl.loop(1, 8)
    def _(step):
        z_back(step).wait()
        hand_on(step).start()

    @pl.loop(0, 8)
    def _(step):
        hand_on(step).wait()


def sum_all(packed):
    vmem = pl.BlockSpec(memory_space=pltpu.VMEM)
    dma = pltpu.SemaphoreType.DMA
    return pl.pallas_call(
        sum_kernel,
        out_shape=jax.ShapeDtypeStruct((2, 8, PIECE, 128), jnp.float32),
        in_specs=[vmem],
        out_specs=vmem,
        scratch_shapes=[
            pltpu.VMEM((8, PIECE, 128), jnp.float32),
            pltpu.VMEM((8, PIECE, 128), jnp.bfloat16),
            pltpu.VMEM((8, PIECE, 128), jnp.bfloat16),
            pltpu.VMEM((PIECE, 128), jnp.bfloat16),
            pltpu.VMEM((16, PIECE, 128), jnp.bfloat16),
            dma, dma, dma((8,)), dma((8,)), dma((16,)), dma((16,)),
            dma((8,)), dma((8,)), dma((8,)), dma((8,)),
        ],
        compiler_params=pltpu.CompilerParams(collective_id=1, has_side_effects=True),
        name="sum_all",
    )(packed)


def shards(
    features,
    partition_map,
    seed_ids,
    hop1_ids,
    hop2_ids,
    labels,
    self_one,
    neigh_one,
    bias_one,
    self_two,
    neigh_two,
    bias_two,
):
    ids = jnp.concatenate(
        [
            seed_ids[None, :],
            hop1_ids.T,
            hop2_ids.transpose(2, 1, 0).reshape(FAN2 * FAN1, SEEDS),
        ],
        axis=0,
    )
    request, place = plan(ids, partition_map)
    returned, hubs = fetch(request, features)
    hubs = hubs.reshape(OWNERS * HOT_DEV, 128)
    seed_loss, packed = sage(
        place, returned, hubs, labels, self_one, neigh_one, bias_one, self_two, neigh_two, bias_two
    )
    total = sum_all(packed.reshape(2, 8, PIECE, 128))
    return (seed_loss, *unpack(total.reshape(ROWS, 128)))


def solution(mesh):
    return jax.shard_map(
        shards,
        mesh=mesh,
        in_specs=(
            P("dom", None),
            P(),
            P(("dom", "rep")),
            P(("dom", "rep"), None),
            P(("dom", "rep"), None, None),
            P(("dom", "rep")),
            P(),
            P(),
            P(),
            P(),
            P(),
            P(),
        ),
        out_specs=(P(("dom", "rep")), P(), P(), P(), P(), P(), P()),
        check_vma=False,
    )
```

```python
import functools

import jax
import jax.numpy as jnp
from jax import lax
from jax.experimental import pallas as pl
from jax.experimental.pallas import tpu as pltpu
from jax.sharding import PartitionSpec as P

MESH = pl.DeviceIdType.MESH
HOT_DEV = 256
NODE_DEV = 8192
OWNERS = 64
CAP = 83
SEEDS = 64
FAN1 = 15
FAN2 = 10
HOPS = SEEDS * FAN1
CLASSES = 172
BLOCK = 128
GROUP = 4
CHUNK = 16
ROWS = 1280
PIECE = ROWS // 32
VMEM_LIMIT = 60 * 1024 * 1024


def fetch_kernel(blocks, lines, ids, table, features, place_out, returned, hubs, found, kept_place,
                 counts, request, wide, picked, sending, arrived, wanted, ask_send, ask_recv, row_send,
                 row_recv, local_sem, z_send, z_recv, x_send, x_recv, core_send, core_recv):
    dom = lax.axis_index("dom")
    y = lax.axis_index("rep")
    core = lax.rem(dom, 2)
    z = lax.rem(lax.div(dom, 2), 8)
    x = lax.div(dom, 16)

    def peer(step):
        return lax.rem(dom + step, OWNERS)

    def at_z(offset):
        return lax.rem(z + offset + 8, 8)

    def at_x(offset):
        return lax.rem(x + offset + 4, 4)

    barrier = pltpu.get_barrier_semaphore()

    @pl.loop(1, OWNERS)
    def _(step):
        pl.semaphore_signal(barrier, inc=1, device_id=(peer(step), y), device_id_type=MESH)

    def hub_z(step, way):
        place = hubs.at[core, x, at_z(-way * (step - 1))]
        if step == 4:
            place = place.at[pl.ds(0 if way > 0 else HOT_DEV // 2, HOT_DEV // 2)]
        slot = step - 1 + (0 if way > 0 else 4)
        return pltpu.make_async_remote_copy(
            src_ref=place, dst_ref=place, send_sem=z_send.at[slot], recv_sem=z_recv.at[slot],
            device_id=((x * 8 + at_z(way)) * 2 + core, y), device_id_type=MESH,
        )

    def hub_x(offset, way, hop):
        place = hubs.at[core, at_x(-way * hop), at_z(offset)]
        slot = (offset + 3) + (0 if way > 0 else 8) + 16 * hop
        return pltpu.make_async_remote_copy(
            src_ref=place, dst_ref=place, send_sem=x_send.at[slot], recv_sem=x_recv.at[slot],
            device_id=((at_x(way) * 8 + z) * 2 + core, y), device_id_type=MESH,
        )

    def hub_core(offset):
        place = hubs.at[core, at_x(offset)]
        return pltpu.make_async_remote_copy(
            src_ref=place, dst_ref=place, send_sem=core_send.at[offset + 1],
            recv_sem=core_recv.at[offset + 1],
            device_id=((x * 8 + z) * 2 + 1 - core, y), device_id_type=MESH,
        )

    def turn(step):
        if step == 0:
            pl.semaphore_wait(barrier, OWNERS - 1)
        else:
            for way in (1, -1):
                hub_z(step, way).wait()
        if step < 4:
            for way in (1, -1):
                hub_z(step + 1, way).start()
        for offset in (0,) if step == 0 else (-step, step) if step < 4 else (4,):
            for way in (1, -1):
                hub_x(offset, way, 0).start()
        if step == 4:
            hub_core(0).start()

    hubs[core, x, z] = features[0:HOT_DEV]
    wide[...] = features[...].astype(jnp.float32)

    square_row = lax.broadcasted_iota(jnp.int32, (BLOCK, BLOCK), 0)
    square_col = lax.broadcasted_iota(jnp.int32, (BLOCK, BLOCK), 1)
    diagonal = square_row == square_col
    before = jnp.concatenate(
        [(square_row < square_col).astype(jnp.bfloat16), jnp.ones((BLOCK, BLOCK), jnp.bfloat16)],
        axis=1,
    )
    owner_row = lax.broadcasted_iota(jnp.int32, (OWNERS, BLOCK), 0)
    groups = ids.shape[0] // GROUP
    found[...] = jnp.zeros_like(found)
    kept_place[...] = jnp.zeros_like(kept_place)
    counts[...] = jnp.zeros_like(counts)

    def spread(position, valid):
        owner = lax.shift_right_logical(position, 13)
        row = position & (NODE_DEV - 1)
        cold = (row >= HOT_DEV) & valid
        member = ((owner_row == owner) & cold).astype(jnp.float32)
        return owner, row, cold, member

    def step(group, base):
        old = [kept_place[pl.ds(8 * g, 2)] for g in range(GROUP)]
        rows = [found[BLOCK * g : BLOCK * (g + 1)] for g in range(GROUP)]
        from_row = jnp.minimum(group, groups - 1) * GROUP
        for g in range(GROUP):
            for at in range(BLOCK):
                found[pl.ds(BLOCK * g + at, 1)] = table[lines[from_row + g, at]]
        last_row = jnp.maximum(group - 1, 0) * GROUP
        ids_row = jnp.minimum(last_row, (groups - 1) * GROUP)
        for g in range(GROUP):
            valid = (group >= 1) & (last_row + g < blocks)
            lane_row = (ids[pl.ds(ids_row + g, 1)] & 127).astype(jnp.float32)
            lane = jnp.sum(jnp.where(diagonal, lane_row, 0.0), axis=1, keepdims=True)
            kept = jnp.where(square_col == lane.astype(jnp.int32), rows[g], 0)
            total = jnp.sum(kept.astype(jnp.float32), axis=1, keepdims=True)
            position = jnp.sum(jnp.where(diagonal, total, 0.0), axis=0, keepdims=True)
            position = position.astype(jnp.int32)
            owner, row, cold, member = spread(position, valid)
            counted = jnp.dot(
                member.astype(jnp.bfloat16), before, preferred_element_type=jnp.float32
            )
            rank = jnp.sum((counted[:, :BLOCK] + base) * member, axis=0, keepdims=True)
            slot = jnp.minimum(rank.astype(jnp.int32), CAP - 1)
            hub_place = (
                (owner & 1) * (OWNERS // 2 * HOT_DEV)
                + lax.shift_right_logical(owner, 1) * HOT_DEV
                + jnp.minimum(row, HOT_DEV - 1)
            )
            place = jnp.where(cold, owner * CAP + slot, OWNERS * CAP + hub_place)
            place_out[pl.ds(last_row + g, 1)] = place
            kept_place[pl.ds(8 * g, 1)] = position
            kept_place[pl.ds(8 * g + 1, 1)] = slot
            base = base + counted[:, BLOCK:]
        old_group = (group - 2) * GROUP
        update = counts[...]
        for g in range(GROUP):
            valid = (group >= 2) & (old_group + g < blocks)
            _, row, _, member = spread(old[g][0:1], valid)
            pick = (square_row == old[g][1:2]).astype(jnp.bfloat16)
            high = member * lax.shift_right_logical(row, 8).astype(jnp.float32)
            low = member * (row & 255).astype(jnp.float32)
            both = jnp.concatenate([high, low], axis=0).astype(jnp.bfloat16)
            update = update + lax.dot_general(
                both, pick, (((1,), (1,)), ((), ())), preferred_element_type=jnp.float32
            )
        counts[...] = update
        for at in range(5):
            pl.when(group == 3 + 4 * at)(functools.partial(turn, at))
        return base

    lax.fori_loop(0, groups + 2, step, jnp.zeros((OWNERS, BLOCK), jnp.float32))
    flat = (counts[0:OWNERS] * 256.0 + counts[OWNERS:]).astype(jnp.int32) & (NODE_DEV - 1)
    for owner in range(OWNERS):
        request[owner] = flat[owner : owner + 1]

    def ask(step):
        return pltpu.make_async_remote_copy(
            src_ref=request.at[peer(step)], dst_ref=arrived.at[step], send_sem=ask_send.at[step],
            recv_sem=ask_recv.at[step], device_id=(peer(step), y), device_id_type=MESH,
        )

    @pl.loop(1, OWNERS)
    def _(step):
        ask(step).start()

    arrived[0] = request[dom]
    order = (0, -1, 1, -2, 2, -3, 3, 4)
    for offset in order:
        for way in (1, -1):
            hub_x(offset, way, 0).wait()
        hub_x(offset, 1 if offset <= 0 else -1, 1).start()

    @pl.loop(1, OWNERS)
    def _(step):
        ask(step).wait()

    down = pltpu.make_async_copy(arrived, wanted, local_sem)
    down.start()
    hub_core(-1).start()
    hub_core(1).start()
    down.wait()

    def asker(step):
        return lax.rem(dom - step + OWNERS, OWNERS)

    def gather(step):
        for at in range(CAP):
            picked[pl.ds(at, 1)] = wide[pl.ds(wanted[step, 0, at], 1)]
        return picked[0:CAP].astype(jnp.bfloat16)

    def answer(step):
        return pltpu.make_async_remote_copy(
            src_ref=sending.at[step], dst_ref=returned.at[dom], send_sem=row_send.at[step],
            recv_sem=row_recv.at[step], device_id=(asker(step), y), device_id_type=MESH,
        )

    sending[1] = gather(1)

    @pl.loop(2, OWNERS)
    def _(step):
        sending[step] = gather(step)
        answer(step - 1).start()

    returned[dom] = gather(0)
    answer(OWNERS - 1).start()

    for offset in order:
        hub_x(offset, 1 if offset <= 0 else -1, 1).wait()
    hub_core(2).start()

    @pl.loop(1, OWNERS)
    def _(step):
        answer(step).wait()

    for offset in (0, -1, 1, 2):
        hub_core(offset).wait()


def fetch(ids, partition_map, features):
    blocks = ids.shape[0] * ids.shape[1] // BLOCK
    padded = -(-blocks // GROUP) * GROUP
    ids = jnp.pad(ids.reshape(blocks, BLOCK), ((0, padded - blocks), (0, 0)))
    lines = lax.shift_right_logical(ids, 7)
    vmem = pl.BlockSpec(memory_space=pltpu.VMEM)
    dma = pltpu.SemaphoreType.DMA
    return pl.pallas_call(
        functools.partial(fetch_kernel, blocks),
        out_shape=[
            jax.ShapeDtypeStruct((padded + GROUP, BLOCK), jnp.int32),
            jax.ShapeDtypeStruct((OWNERS, CAP, 128), jnp.bfloat16),
            jax.ShapeDtypeStruct((2, 4, 8, HOT_DEV, 128), jnp.bfloat16),
        ],
        in_specs=[pl.BlockSpec(memory_space=pltpu.SMEM), vmem, vmem, vmem],
        out_specs=[vmem, vmem, vmem],
        scratch_shapes=[
            pltpu.VMEM((GROUP * BLOCK, BLOCK), jnp.int32),
            pltpu.VMEM((GROUP * 8, BLOCK), jnp.int32),
            pltpu.VMEM((BLOCK, BLOCK), jnp.float32),
            pltpu.VMEM((OWNERS, 1, BLOCK), jnp.int32),
            pltpu.VMEM(features.shape, jnp.float32),
            pltpu.VMEM((88, 128), jnp.float32),
            pltpu.VMEM((OWNERS, CAP, 128), jnp.bfloat16),
            pltpu.VMEM((OWNERS, 1, BLOCK), jnp.int32),
            pltpu.SMEM((OWNERS, 1, BLOCK), jnp.int32),
            dma((OWNERS,)), dma((OWNERS,)), dma((OWNERS,)), dma((OWNERS,)), dma,
            dma((8,)), dma((8,)), dma((32,)), dma((32,)), dma((4,)), dma((4,)),
        ],
        compiler_params=pltpu.CompilerParams(
            collective_id=2, has_side_effects=True, vmem_limit_bytes=VMEM_LIMIT
        ),
        name="fetch",
    )(lines, ids, partition_map.reshape(-1, 1, BLOCK), features)


def dot(a, b, dims):
    return lax.dot_general(a, b, (dims, ((), ())), preferred_element_type=jnp.float32)


def gelu_parts(x):
    scale = 0.7978845608028654
    square = x * x
    t = jnp.tanh(scale * x * (1.0 + 0.044715 * square))
    half = 0.5 * (1.0 + t)
    slope = half + 0.5 * x * (1.0 - t * t) * (scale * (1.0 + 3.0 * 0.044715 * square))
    return x * half, slope


def sage_kernel(place, returned, hubs, labels, self_one, neigh_one, bias_one, self_two, neigh_two,
                bias_two, loss_out, packed, table, rows, far):
    for owner in range(OWNERS):
        table[CAP * owner : CAP * (owner + 1)] = returned[owner].astype(jnp.float32)
    table[CAP * OWNERS :] = hubs[...].astype(jnp.float32)

    @pl.loop(0, (SEEDS + HOPS) // 64)
    def _(block):
        first = pl.multiple_of(block * 64, 64)
        for at in range(64):
            rows[pl.ds(first + at, 1)] = table[pl.ds(place[first + at], 1)]

    @pl.loop(0, HOPS // CHUNK)
    def _(block):
        first = pl.multiple_of(block * CHUNK, CHUNK)
        for at in range(CHUNK):
            value = None
            for k in range(FAN2):
                row = table[pl.ds(place[first + (SEEDS + HOPS + k * HOPS + at)], 1)]
                value = row if value is None else value + row
            far[pl.ds(first + at, 1)] = value

    seed_rows = rows[0:SEEDS].astype(jnp.bfloat16)
    hop_rows = rows[SEEDS:].astype(jnp.bfloat16)
    far_mean = (far[...] * (1.0 / FAN2)).astype(jnp.bfloat16)
    seed_sum = rows[SEEDS : 2 * SEEDS]
    for f in range(1, FAN1):
        seed_sum = seed_sum + rows[SEEDS * (f + 1) : SEEDS * (f + 2)]
    seed_mean = (seed_sum * (1.0 / FAN1)).astype(jnp.bfloat16)

    own = jnp.concatenate([seed_rows, hop_rows], axis=0)
    near = jnp.concatenate([seed_mean, far_mean], axis=0)
    both = jnp.concatenate([own, near], axis=1)
    weight = jnp.concatenate([self_one[...], neigh_one[...]], axis=0)
    pre = dot(both, weight, ((1,), (0,))) + bias_one[...]
    act, slope = gelu_parts(pre)
    hid_seed = act[0:SEEDS].astype(jnp.bfloat16)
    hop_sum = act[SEEDS : 2 * SEEDS]
    for f in range(1, FAN1):
        hop_sum = hop_sum + act[SEEDS * (f + 1) : SEEDS * (f + 2)]
    hop_mean = (hop_sum * (1.0 / FAN1)).astype(jnp.bfloat16)

    logits = (
        dot(hid_seed, self_two[...], ((1,), (1,)))
        + dot(hop_mean, neigh_two[...], ((1,), (1,)))
        + bias_two[...]
    )
    shifted = logits - jnp.max(logits, axis=1, keepdims=True)
    exps = jnp.exp(shifted)
    sums = jnp.sum(exps, axis=1, keepdims=True)
    log_probs = shifted - jnp.log(sums)
    small_row = lax.broadcasted_iota(jnp.int32, (SEEDS, SEEDS), 0)
    small_col = lax.broadcasted_iota(jnp.int32, (SEEDS, SEEDS), 1)
    label = jnp.sum(
        jnp.where(small_row == small_col, labels[...].astype(jnp.float32), 0.0),
        axis=1, keepdims=True,
    ).astype(jnp.int32)
    target = lax.broadcasted_iota(jnp.int32, (SEEDS, CLASSES), 1) == label
    picked = jnp.sum(jnp.where(target, log_probs, 0.0), axis=1, keepdims=True)
    loss_out[...] = -jnp.sum(
        jnp.where(small_row == small_col, picked, 0.0), axis=0, keepdims=True
    )
    d_logits32 = (jnp.exp(log_probs) - target.astype(jnp.float32)) * (1.0 / SEEDS)
    d_logits = d_logits32.astype(jnp.bfloat16)

    zeros = jnp.zeros((8, 128), jnp.float32)
    packed[512 + 168 : 512 + 176] = zeros
    packed[688 + 168 : 688 + 176] = zeros
    packed[864 + 168 : 864 + 176] = zeros
    packed[1040 + 168 : 1040 + 176] = zeros
    packed[1216:] = jnp.zeros((ROWS - 1216, 128), jnp.float32)
    grad_self_two = dot(d_logits, hid_seed, ((0,), (0,)))
    packed[512:684] = grad_self_two[:, :128]
    packed[688:860] = grad_self_two[:, 128:]
    grad_neigh_two = dot(d_logits, hop_mean, ((0,), (0,)))
    packed[864:1036] = grad_neigh_two[:, :128]
    packed[1040:1212] = grad_neigh_two[:, 128:]
    grad_bias_two = jnp.sum(d_logits32, axis=0, keepdims=True)
    packed[1218:1219] = grad_bias_two[:, :128]
    packed[1219:1220, 0 : CLASSES - 128] = grad_bias_two[:, 128:]

    d_hid_seed = dot(d_logits, self_two[...], ((1,), (0,)))
    d_hop_mean = dot(d_logits, neigh_two[...], ((1,), (0,))) * (1.0 / FAN1)
    d_hid = jnp.concatenate([d_hid_seed] + [d_hop_mean] * FAN1, axis=0)
    d_pre32 = d_hid * slope
    d_pre = d_pre32.astype(jnp.bfloat16)
    grad_one = dot(both, d_pre, ((0,), (0,)))
    packed[0:128] = grad_one[0:128, :128]
    packed[128:256] = grad_one[0:128, 128:]
    packed[256:384] = grad_one[128:256, :128]
    packed[384:512] = grad_one[128:256, 128:]
    grad_bias_one = jnp.sum(d_pre32, axis=0, keepdims=True)
    packed[1216:1217] = grad_bias_one[:, :128]
    packed[1217:1218] = grad_bias_one[:, 128:]


def sage(place, returned, hubs, labels, self_one, neigh_one, bias_one, self_two, neigh_two, bias_two):
    vmem = pl.BlockSpec(memory_space=pltpu.VMEM)
    loss, packed = pl.pallas_call(
        sage_kernel,
        out_shape=[
            jax.ShapeDtypeStruct((1, SEEDS), jnp.float32),
            jax.ShapeDtypeStruct((ROWS, 128), jnp.float32),
        ],
        in_specs=[pl.BlockSpec(memory_space=pltpu.SMEM)] + [vmem] * 9,
        out_specs=[vmem, vmem],
        scratch_shapes=[
            pltpu.VMEM((OWNERS * (CAP + HOT_DEV), 128), jnp.float32),
            pltpu.VMEM((SEEDS + HOPS, 128), jnp.float32),
            pltpu.VMEM((HOPS, 128), jnp.float32),
        ],
        compiler_params=pltpu.CompilerParams(vmem_limit_bytes=VMEM_LIMIT),
        name="sage",
    )(
        place.reshape(-1), returned, hubs, labels[None, :], self_one, neigh_one, bias_one[None, :],
        self_two.T, neigh_two.T, bias_two[None, :],
    )
    return loss.reshape(-1), packed


def unpack_kernel(packed, self_one, neigh_one, bias_one, self_two, neigh_two, bias_two):
    self_one[:, :128] = packed[0:128]
    self_one[:, 128:] = packed[128:256]
    neigh_one[:, :128] = packed[256:384]
    neigh_one[:, 128:] = packed[384:512]
    self_two[:, :128] = packed[512:684]
    self_two[:, 128:] = packed[688:860]
    neigh_two[:, :128] = packed[864:1036]
    neigh_two[:, 128:] = packed[1040:1212]
    bias_one[:, :128] = packed[1216:1217]
    bias_one[:, 128:] = packed[1217:1218]
    bias_two[:, :128] = packed[1218:1219]
    bias_two[:, 128:] = packed[1219:1220, 0 : CLASSES - 128]


def unpack(packed):
    shapes = ((128, 256), (128, 256), (1, 256), (CLASSES, 256), (CLASSES, 256), (1, CLASSES))
    self_one, neigh_one, bias_one, self_two, neigh_two, bias_two = pl.pallas_call(
        unpack_kernel,
        out_shape=[jax.ShapeDtypeStruct(shape, jnp.float32) for shape in shapes],
        name="unpack",
    )(packed)
    return self_one, neigh_one, bias_one.reshape(-1), self_two.T, neigh_two.T, bias_two.reshape(-1)


def sum_kernel(mine, total, other, send_p, recv_p, send_z, recv_z, core_send, core_recv,
               p_send, p_recv, z_send, z_recv, g_send, g_recv, h_send, h_recv):
    dom = lax.axis_index("dom")
    y = lax.axis_index("rep")
    core = lax.rem(dom, 2)
    z = lax.rem(lax.div(dom, 2), 8)
    x = lax.div(dom, 16)
    place = x * 4 + y

    def device(at, to_z, to_core):
        return ((lax.div(at, 4) * 8 + to_z) * 2 + to_core, lax.rem(at, 4))

    partner = device(place, z, 1 - core)

    def above(step):
        return lax.rem(place + step, 16)

    def below(step):
        return lax.rem(place - step + 16, 16)

    def z_peer(step):
        return device(place, lax.rem(z + step, 8), core)

    barrier = pltpu.get_barrier_semaphore()
    pl.semaphore_signal(barrier, inc=1, device_id=partner, device_id_type=MESH)

    @pl.loop(1, 16)
    def _(step):
        pl.semaphore_signal(
            barrier, inc=1, device_id=device(above(step), z, core), device_id_type=MESH
        )

    @pl.loop(1, 8)
    def _(step):
        pl.semaphore_signal(barrier, inc=1, device_id=z_peer(step), device_id_type=MESH)

    pl.semaphore_wait(barrier, 23)

    swap = pltpu.make_async_remote_copy(
        src_ref=mine.at[1 - core], dst_ref=other, send_sem=core_send, recv_sem=core_recv,
        device_id=partner, device_id_type=MESH,
    )
    swap.start()
    swap.wait()

    @pl.loop(0, 16)
    def _(part):
        send_p[part] = (mine[core, part] + other[part]).astype(jnp.bfloat16)

    def plane_copy(step):
        return pltpu.make_async_remote_copy(
            src_ref=send_p.at[above(step)], dst_ref=recv_p.at[step], send_sem=p_send.at[step],
            recv_sem=p_recv.at[step], device_id=device(above(step), z, core), device_id_type=MESH,
        )

    @pl.loop(1, 16)
    def _(step):
        plane_copy(step).start()

    kept = mine[core, place] + other[place]

    @pl.loop(1, 16)
    def _(step):
        plane_copy(step).wait()

    def add_plane(step, value):
        return value + recv_p[step].astype(jnp.float32)

    send_z[...] = lax.fori_loop(1, 16, add_plane, kept).astype(jnp.bfloat16)

    def z_copy(step):
        return pltpu.make_async_remote_copy(
            src_ref=send_z, dst_ref=recv_z.at[step], send_sem=z_send.at[step],
            recv_sem=z_recv.at[step], device_id=z_peer(step), device_id_type=MESH,
        )

    @pl.loop(1, 8)
    def _(step):
        z_copy(step).start()

    recv_z[0] = send_z[...]

    @pl.loop(1, 8)
    def _(step):
        z_copy(step).wait()

    def add_z(of_z, value):
        step = lax.rem(z - of_z + 8, 8)
        return value + recv_z[step].astype(jnp.float32)

    total[core, place] = lax.fori_loop(0, 8, add_z, jnp.zeros_like(kept))

    def plane_back(step):
        return pltpu.make_async_remote_copy(
            src_ref=total.at[core, place], dst_ref=total.at[core, place], send_sem=g_send.at[step],
            recv_sem=g_recv.at[step], device_id=device(above(step), z, core), device_id_type=MESH,
        )

    def hand_on(step):
        return pltpu.make_async_remote_copy(
            src_ref=total.at[core, below(step)], dst_ref=total.at[core, below(step)],
            send_sem=h_send.at[step], recv_sem=h_recv.at[step], device_id=partner,
            device_id_type=MESH,
        )

    @pl.loop(1, 16)
    def _(step):
        plane_back(step).start()

    hand_on(0).start()

    @pl.loop(1, 16)
    def _(step):
        plane_back(step).wait()
        hand_on(step).start()

    @pl.loop(0, 16)
    def _(step):
        hand_on(step).wait()


def sum_all(packed):
    vmem = pl.BlockSpec(memory_space=pltpu.VMEM)
    dma = pltpu.SemaphoreType.DMA
    return pl.pallas_call(
        sum_kernel,
        out_shape=jax.ShapeDtypeStruct((2, 16, PIECE, 128), jnp.float32),
        in_specs=[vmem],
        out_specs=vmem,
        scratch_shapes=[
            pltpu.VMEM((16, PIECE, 128), jnp.float32),
            pltpu.VMEM((16, PIECE, 128), jnp.bfloat16),
            pltpu.VMEM((16, PIECE, 128), jnp.bfloat16),
            pltpu.VMEM((PIECE, 128), jnp.bfloat16),
            pltpu.VMEM((8, PIECE, 128), jnp.bfloat16),
            dma, dma, dma((16,)), dma((16,)), dma((8,)), dma((8,)),
            dma((16,)), dma((16,)), dma((16,)), dma((16,)),
        ],
        compiler_params=pltpu.CompilerParams(collective_id=1, has_side_effects=True),
        name="sum_all",
    )(packed)


def shards(
    features,
    partition_map,
    seed_ids,
    hop1_ids,
    hop2_ids,
    labels,
    self_one,
    neigh_one,
    bias_one,
    self_two,
    neigh_two,
    bias_two,
):
    ids = jnp.concatenate(
        [
            seed_ids[None, :],
            hop1_ids.T,
            hop2_ids.transpose(2, 1, 0).reshape(FAN2 * FAN1, SEEDS),
        ],
        axis=0,
    )
    place, returned, hubs = fetch(ids, partition_map, features)
    hubs = hubs.reshape(OWNERS * HOT_DEV, 128)
    seed_loss, packed = sage(
        place, returned, hubs, labels, self_one, neigh_one, bias_one, self_two, neigh_two, bias_two
    )
    total = sum_all(packed.reshape(2, 16, PIECE, 128))
    return (seed_loss, *unpack(total.reshape(ROWS, 128)))


def solution(mesh):
    return jax.shard_map(
        shards,
        mesh=mesh,
        in_specs=(
            P("dom", None),
            P(),
            P(("dom", "rep")),
            P(("dom", "rep"), None),
            P(("dom", "rep"), None, None),
            P(("dom", "rep")),
            P(),
            P(),
            P(),
            P(),
            P(),
            P(),
        ),
        out_specs=(P(("dom", "rep")), P(), P(), P(), P(), P(), P()),
        check_vma=False,
    )
```

```python
import functools

import jax
import jax.numpy as jnp
from jax import lax
from jax.experimental import pallas as pl
from jax.experimental.pallas import tpu as pltpu
from jax.sharding import PartitionSpec as P

MESH = pl.DeviceIdType.MESH
HOT_DEV = 256
NODE_DEV = 8192
OWNERS = 64
CAP = 83
SEEDS = 64
FAN1 = 15
FAN2 = 10
HOPS = SEEDS * FAN1
CLASSES = 172
BLOCK = 128
GROUP = 4
CHUNK = 16
ROWS = 1280
PIECE = ROWS // 32
VMEM_LIMIT = 60 * 1024 * 1024


def fetch_kernel(blocks, lines, ids, table, features, place_out, returned, hubs, found, kept_place,
                 counts, request, wide, picked, sending, arrived, wanted, ask_send, ask_recv, row_send,
                 row_recv, local_sem, z_send, z_recv, x_send, x_recv, core_send, core_recv):
    dom = lax.axis_index("dom")
    y = lax.axis_index("rep")
    core = lax.rem(dom, 2)
    z = lax.rem(lax.div(dom, 2), 8)
    x = lax.div(dom, 16)

    def peer(step):
        return lax.rem(dom + step, OWNERS)

    def at_z(offset):
        return lax.rem(z + offset + 8, 8)

    def at_x(offset):
        return lax.rem(x + offset + 4, 4)

    barrier = pltpu.get_barrier_semaphore()

    @pl.loop(1, OWNERS)
    def _(step):
        pl.semaphore_signal(barrier, inc=1, device_id=(peer(step), y), device_id_type=MESH)

    def hub_z(step, way):
        place = hubs.at[core, x, at_z(-way * (step - 1))]
        if step == 4:
            place = place.at[pl.ds(0 if way > 0 else HOT_DEV // 2, HOT_DEV // 2)]
        slot = step - 1 + (0 if way > 0 else 4)
        return pltpu.make_async_remote_copy(
            src_ref=place, dst_ref=place, send_sem=z_send.at[slot], recv_sem=z_recv.at[slot],
            device_id=((x * 8 + at_z(way)) * 2 + core, y), device_id_type=MESH,
        )

    def hub_x(offset, way, hop):
        place = hubs.at[core, at_x(-way * hop), at_z(offset)]
        slot = (offset + 3) + (0 if way > 0 else 8) + 16 * hop
        return pltpu.make_async_remote_copy(
            src_ref=place, dst_ref=place, send_sem=x_send.at[slot], recv_sem=x_recv.at[slot],
            device_id=((at_x(way) * 8 + z) * 2 + core, y), device_id_type=MESH,
        )

    def hub_core(offset):
        place = hubs.at[core, at_x(offset)]
        return pltpu.make_async_remote_copy(
            src_ref=place, dst_ref=place, send_sem=core_send.at[offset + 1],
            recv_sem=core_recv.at[offset + 1],
            device_id=((x * 8 + z) * 2 + 1 - core, y), device_id_type=MESH,
        )

    def turn(step):
        if step == 0:
            pl.semaphore_wait(barrier, OWNERS - 1)
        else:
            for way in (1, -1):
                hub_z(step, way).wait()
        if step < 4:
            for way in (1, -1):
                hub_z(step + 1, way).start()
        for offset in (0,) if step == 0 else (-step, step) if step < 4 else (4,):
            for way in (1, -1):
                hub_x(offset, way, 0).start()
        if step == 4:
            hub_core(0).start()

    hubs[core, x, z] = features[0:HOT_DEV]
    wide[...] = features[...].astype(jnp.float32)

    square_row = lax.broadcasted_iota(jnp.int32, (BLOCK, BLOCK), 0)
    square_col = lax.broadcasted_iota(jnp.int32, (BLOCK, BLOCK), 1)
    diagonal = square_row == square_col
    before = jnp.concatenate(
        [(square_row < square_col).astype(jnp.bfloat16), jnp.ones((BLOCK, BLOCK), jnp.bfloat16)],
        axis=1,
    )
    owner_row = lax.broadcasted_iota(jnp.int32, (OWNERS, BLOCK), 0)
    groups = ids.shape[0] // GROUP
    found[...] = jnp.zeros_like(found)
    kept_place[...] = jnp.zeros_like(kept_place)
    counts[...] = jnp.zeros_like(counts)

    def spread(position, valid):
        owner = lax.shift_right_logical(position, 13)
        row = position & (NODE_DEV - 1)
        cold = (row >= HOT_DEV) & valid
        member = ((owner_row == owner) & cold).astype(jnp.float32)
        return owner, row, cold, member

    def step(group, base):
        old = [kept_place[pl.ds(8 * g, 2)] for g in range(GROUP)]
        rows = [found[BLOCK * g : BLOCK * (g + 1)] for g in range(GROUP)]
        from_row = jnp.minimum(group, groups - 1) * GROUP
        for g in range(GROUP):
            for at in range(BLOCK):
                found[pl.ds(BLOCK * g + at, 1)] = table[lines[from_row + g, at]]
        last_row = jnp.maximum(group - 1, 0) * GROUP
        ids_row = jnp.minimum(last_row, (groups - 1) * GROUP)
        for g in range(GROUP):
            valid = (group >= 1) & (last_row + g < blocks)
            lane_row = (ids[pl.ds(ids_row + g, 1)] & 127).astype(jnp.float32)
            lane = jnp.sum(jnp.where(diagonal, lane_row, 0.0), axis=1, keepdims=True)
            kept = jnp.where(square_col == lane.astype(jnp.int32), rows[g], 0)
            total = jnp.sum(kept.astype(jnp.float32), axis=1, keepdims=True)
            position = jnp.sum(jnp.where(diagonal, total, 0.0), axis=0, keepdims=True)
            position = position.astype(jnp.int32) & (OWNERS * NODE_DEV - 1)
            owner, row, cold, member = spread(position, valid)
            counted = jnp.dot(
                member.astype(jnp.bfloat16), before, preferred_element_type=jnp.float32
            )
            rank = jnp.sum((counted[:, :BLOCK] + base) * member, axis=0, keepdims=True)
            slot = jnp.clip(rank.astype(jnp.int32), 0, CAP - 1)
            hub_place = (
                (owner & 1) * (OWNERS // 2 * HOT_DEV)
                + lax.shift_right_logical(owner, 1) * HOT_DEV
                + jnp.minimum(row, HOT_DEV - 1)
            )
            place = jnp.where(cold, owner * CAP + slot, OWNERS * CAP + hub_place)
            place_out[pl.ds(last_row + g, 1)] = place
            kept_place[pl.ds(8 * g, 1)] = position
            kept_place[pl.ds(8 * g + 1, 1)] = slot
            base = base + counted[:, BLOCK:]
        old_group = (group - 2) * GROUP
        update = counts[...]
        for g in range(GROUP):
            valid = (group >= 2) & (old_group + g < blocks)
            _, row, _, member = spread(old[g][0:1], valid)
            pick = (square_row == old[g][1:2]).astype(jnp.bfloat16)
            high = member * lax.shift_right_logical(row, 8).astype(jnp.float32)
            low = member * (row & 255).astype(jnp.float32)
            both = jnp.concatenate([high, low], axis=0).astype(jnp.bfloat16)
            update = update + lax.dot_general(
                both, pick, (((1,), (1,)), ((), ())), preferred_element_type=jnp.float32
            )
        counts[...] = update
        for at in range(5):
            pl.when(group == 3 + 4 * at)(functools.partial(turn, at))
        return base

    lax.fori_loop(0, groups + 2, step, jnp.zeros((OWNERS, BLOCK), jnp.float32))
    flat = (counts[0:OWNERS] * 256.0 + counts[OWNERS:]).astype(jnp.int32) & (NODE_DEV - 1)
    for owner in range(OWNERS):
        request[owner] = flat[owner : owner + 1]

    def distance(slot):
        turn_z = lax.div(slot, 8)
        ahead = lax.div(turn_z + 1, 2)
        dz = jnp.where(lax.rem(turn_z, 2) == 1, ahead, 8 - ahead)
        return lax.div(lax.rem(slot, 8), 2), dz, lax.rem(slot, 2)

    def owner_at(slot):
        dx, dz, dc = distance(slot)
        return (lax.rem(x + dx, 4) * 8 + lax.rem(z + dz, 8)) * 2 + lax.rem(core + dc, 2)

    def asker_at(slot):
        dx, dz, dc = distance(slot)
        return (lax.rem(x - dx + 4, 4) * 8 + lax.rem(z - dz + 8, 8)) * 2 + lax.rem(core + dc, 2)

    def ask(slot):
        owner = owner_at(slot)
        return pltpu.make_async_remote_copy(
            src_ref=request.at[owner], dst_ref=arrived.at[slot], send_sem=ask_send.at[slot],
            recv_sem=ask_recv.at[slot], device_id=(owner, y), device_id_type=MESH,
        )

    @pl.loop(1, OWNERS)
    def _(slot):
        ask(slot).start()

    arrived[0] = request[dom]

    def down(near):
        first = near * 8
        return pltpu.make_async_copy(
            arrived.at[pl.ds(first, 8)], wanted.at[pl.ds(first, 8)], local_sem.at[near]
        )

    @pl.loop(1, 8)
    def _(slot):
        ask(slot).wait()

    down(0).start()
    order = (0, -1, 1, -2, 2, -3, 3, 4)

    def hub_on():
        for offset in order:
            for way in (1, -1):
                hub_x(offset, way, 0).wait()
            hub_x(offset, 1 if offset <= 0 else -1, 1).start()
        hub_core(-1).start()
        hub_core(1).start()

    def gather(slot):
        for at in range(CAP):
            picked[pl.ds(at, 1)] = wide[pl.ds(wanted[slot, 0, at], 1)]
        return picked[0:CAP].astype(jnp.bfloat16)

    def answer(slot):
        return pltpu.make_async_remote_copy(
            src_ref=sending.at[slot], dst_ref=returned.at[dom], send_sem=row_send.at[slot],
            recv_sem=row_recv.at[slot], device_id=(asker_at(slot), y), device_id_type=MESH,
        )

    @pl.loop(0, 8)
    def _(near):
        down(near).wait()

        @pl.when(near < 7)
        def _():
            @pl.loop(0, 8)
            def _(at):
                ask(near * 8 + 8 + at).wait()

            down(near + 1).start()

        @pl.loop(0, 8)
        def _(at):
            slot = near * 8 + at
            sending[slot] = gather(slot)

            @pl.when(slot >= 2)
            def _():
                answer(slot - 1).start()

        pl.when(near == 3)(hub_on)

    answer(OWNERS - 1).start()
    returned[dom] = sending[0]

    for offset in order:
        hub_x(offset, 1 if offset <= 0 else -1, 1).wait()
    hub_core(2).start()
    for offset in (0, -1, 1, 2):
        hub_core(offset).wait()

    @pl.loop(1, OWNERS)
    def _(slot):
        answer(slot).wait()


def fetch(ids, partition_map, features):
    blocks = ids.shape[0] * ids.shape[1] // BLOCK
    padded = -(-blocks // GROUP) * GROUP
    ids = jnp.pad(ids.reshape(blocks, BLOCK), ((0, padded - blocks), (0, 0)))
    lines = lax.shift_right_logical(ids, 7)
    vmem = pl.BlockSpec(memory_space=pltpu.VMEM)
    dma = pltpu.SemaphoreType.DMA
    return pl.pallas_call(
        functools.partial(fetch_kernel, blocks),
        out_shape=[
            jax.ShapeDtypeStruct((padded + GROUP, BLOCK), jnp.int32),
            jax.ShapeDtypeStruct((OWNERS, CAP, 128), jnp.bfloat16),
            jax.ShapeDtypeStruct((2, 4, 8, HOT_DEV, 128), jnp.bfloat16),
        ],
        in_specs=[pl.BlockSpec(memory_space=pltpu.SMEM), vmem, vmem, vmem],
        out_specs=[vmem, vmem, vmem],
        scratch_shapes=[
            pltpu.VMEM((GROUP * BLOCK, BLOCK), jnp.int32),
            pltpu.VMEM((GROUP * 8, BLOCK), jnp.int32),
            pltpu.VMEM((BLOCK, BLOCK), jnp.float32),
            pltpu.VMEM((OWNERS, 1, BLOCK), jnp.int32),
            pltpu.VMEM(features.shape, jnp.float32),
            pltpu.VMEM((88, 128), jnp.float32),
            pltpu.VMEM((OWNERS, CAP, 128), jnp.bfloat16),
            pltpu.VMEM((OWNERS, 1, BLOCK), jnp.int32),
            pltpu.SMEM((OWNERS, 1, BLOCK), jnp.int32),
            dma((OWNERS,)), dma((OWNERS,)), dma((OWNERS,)), dma((OWNERS,)), dma((8,)),
            dma((8,)), dma((8,)), dma((32,)), dma((32,)), dma((4,)), dma((4,)),
        ],
        compiler_params=pltpu.CompilerParams(
            collective_id=2, has_side_effects=True, vmem_limit_bytes=VMEM_LIMIT
        ),
        name="fetch",
    )(lines, ids, partition_map.reshape(-1, 1, BLOCK), features)


def dot(a, b, dims):
    return lax.dot_general(a, b, (dims, ((), ())), preferred_element_type=jnp.float32)


def gelu_parts(x):
    scale = 0.7978845608028654
    square = x * x
    t = jnp.tanh(scale * x * (1.0 + 0.044715 * square))
    half = 0.5 * (1.0 + t)
    slope = half + 0.5 * x * (1.0 - t * t) * (scale * (1.0 + 3.0 * 0.044715 * square))
    return x * half, slope


def sage_kernel(place, returned, hubs, labels, self_one, neigh_one, bias_one, self_two, neigh_two,
                bias_two, loss_out, packed, table, rows, far):
    for owner in range(OWNERS):
        table[CAP * owner : CAP * (owner + 1)] = returned[owner].astype(jnp.float32)
    table[CAP * OWNERS :] = hubs[...].astype(jnp.float32)

    @pl.loop(0, (SEEDS + HOPS) // 64)
    def _(block):
        first = pl.multiple_of(block * 64, 64)
        for at in range(64):
            rows[pl.ds(first + at, 1)] = table[pl.ds(place[first + at], 1)]

    @pl.loop(0, HOPS // CHUNK)
    def _(block):
        first = pl.multiple_of(block * CHUNK, CHUNK)
        for at in range(CHUNK):
            value = None
            for k in range(FAN2):
                row = table[pl.ds(place[first + (SEEDS + HOPS + k * HOPS + at)], 1)]
                value = row if value is None else value + row
            far[pl.ds(first + at, 1)] = value

    seed_rows = rows[0:SEEDS].astype(jnp.bfloat16)
    hop_rows = rows[SEEDS:].astype(jnp.bfloat16)
    far_mean = (far[...] * (1.0 / FAN2)).astype(jnp.bfloat16)
    seed_sum = rows[SEEDS : 2 * SEEDS]
    for f in range(1, FAN1):
        seed_sum = seed_sum + rows[SEEDS * (f + 1) : SEEDS * (f + 2)]
    seed_mean = (seed_sum * (1.0 / FAN1)).astype(jnp.bfloat16)

    own = jnp.concatenate([seed_rows, hop_rows], axis=0)
    near = jnp.concatenate([seed_mean, far_mean], axis=0)
    both = jnp.concatenate([own, near], axis=1)
    weight = jnp.concatenate([self_one[...], neigh_one[...]], axis=0)
    pre = dot(both, weight, ((1,), (0,))) + bias_one[...]
    act, slope = gelu_parts(pre)
    hid_seed = act[0:SEEDS].astype(jnp.bfloat16)
    hop_sum = act[SEEDS : 2 * SEEDS]
    for f in range(1, FAN1):
        hop_sum = hop_sum + act[SEEDS * (f + 1) : SEEDS * (f + 2)]
    hop_mean = (hop_sum * (1.0 / FAN1)).astype(jnp.bfloat16)

    logits = (
        dot(hid_seed, self_two[...], ((1,), (1,)))
        + dot(hop_mean, neigh_two[...], ((1,), (1,)))
        + bias_two[...]
    )
    shifted = logits - jnp.max(logits, axis=1, keepdims=True)
    exps = jnp.exp(shifted)
    sums = jnp.sum(exps, axis=1, keepdims=True)
    log_probs = shifted - jnp.log(sums)
    small_row = lax.broadcasted_iota(jnp.int32, (SEEDS, SEEDS), 0)
    small_col = lax.broadcasted_iota(jnp.int32, (SEEDS, SEEDS), 1)
    label = jnp.sum(
        jnp.where(small_row == small_col, labels[...].astype(jnp.float32), 0.0),
        axis=1, keepdims=True,
    ).astype(jnp.int32)
    target = lax.broadcasted_iota(jnp.int32, (SEEDS, CLASSES), 1) == label
    picked = jnp.sum(jnp.where(target, log_probs, 0.0), axis=1, keepdims=True)
    loss_out[...] = -jnp.sum(
        jnp.where(small_row == small_col, picked, 0.0), axis=0, keepdims=True
    )
    d_logits32 = (jnp.exp(log_probs) - target.astype(jnp.float32)) * (1.0 / SEEDS)
    d_logits = d_logits32.astype(jnp.bfloat16)

    zeros = jnp.zeros((8, 128), jnp.float32)
    packed[512 + 168 : 512 + 176] = zeros
    packed[688 + 168 : 688 + 176] = zeros
    packed[864 + 168 : 864 + 176] = zeros
    packed[1040 + 168 : 1040 + 176] = zeros
    packed[1216:] = jnp.zeros((ROWS - 1216, 128), jnp.float32)
    grad_self_two = dot(d_logits, hid_seed, ((0,), (0,)))
    packed[512:684] = grad_self_two[:, :128]
    packed[688:860] = grad_self_two[:, 128:]
    grad_neigh_two = dot(d_logits, hop_mean, ((0,), (0,)))
    packed[864:1036] = grad_neigh_two[:, :128]
    packed[1040:1212] = grad_neigh_two[:, 128:]
    grad_bias_two = jnp.sum(d_logits32, axis=0, keepdims=True)
    packed[1218:1219] = grad_bias_two[:, :128]
    packed[1219:1220, 0 : CLASSES - 128] = grad_bias_two[:, 128:]

    d_hid_seed = dot(d_logits, self_two[...], ((1,), (0,)))
    d_hop_mean = dot(d_logits, neigh_two[...], ((1,), (0,))) * (1.0 / FAN1)
    d_hid = jnp.concatenate([d_hid_seed] + [d_hop_mean] * FAN1, axis=0)
    d_pre32 = d_hid * slope
    d_pre = d_pre32.astype(jnp.bfloat16)
    grad_one = dot(both, d_pre, ((0,), (0,)))
    packed[0:128] = grad_one[0:128, :128]
    packed[128:256] = grad_one[0:128, 128:]
    packed[256:384] = grad_one[128:256, :128]
    packed[384:512] = grad_one[128:256, 128:]
    grad_bias_one = jnp.sum(d_pre32, axis=0, keepdims=True)
    packed[1216:1217] = grad_bias_one[:, :128]
    packed[1217:1218] = grad_bias_one[:, 128:]


def sage(place, returned, hubs, labels, self_one, neigh_one, bias_one, self_two, neigh_two, bias_two):
    vmem = pl.BlockSpec(memory_space=pltpu.VMEM)
    loss, packed = pl.pallas_call(
        sage_kernel,
        out_shape=[
            jax.ShapeDtypeStruct((1, SEEDS), jnp.float32),
            jax.ShapeDtypeStruct((ROWS, 128), jnp.float32),
        ],
        in_specs=[pl.BlockSpec(memory_space=pltpu.SMEM)] + [vmem] * 9,
        out_specs=[vmem, vmem],
        scratch_shapes=[
            pltpu.VMEM((OWNERS * (CAP + HOT_DEV), 128), jnp.float32),
            pltpu.VMEM((SEEDS + HOPS, 128), jnp.float32),
            pltpu.VMEM((HOPS, 128), jnp.float32),
        ],
        compiler_params=pltpu.CompilerParams(vmem_limit_bytes=VMEM_LIMIT),
        name="sage",
    )(
        place.reshape(-1), returned, hubs, labels[None, :], self_one, neigh_one, bias_one[None, :],
        self_two.T, neigh_two.T, bias_two[None, :],
    )
    return loss.reshape(-1), packed


def unpack_kernel(packed, self_one, neigh_one, bias_one, self_two, neigh_two, bias_two):
    self_one[:, :128] = packed[0:128]
    self_one[:, 128:] = packed[128:256]
    neigh_one[:, :128] = packed[256:384]
    neigh_one[:, 128:] = packed[384:512]
    self_two[:, :128] = packed[512:684]
    self_two[:, 128:] = packed[688:860]
    neigh_two[:, :128] = packed[864:1036]
    neigh_two[:, 128:] = packed[1040:1212]
    bias_one[:, :128] = packed[1216:1217]
    bias_one[:, 128:] = packed[1217:1218]
    bias_two[:, :128] = packed[1218:1219]
    bias_two[:, 128:] = packed[1219:1220, 0 : CLASSES - 128]


def unpack(packed):
    shapes = ((128, 256), (128, 256), (1, 256), (CLASSES, 256), (CLASSES, 256), (1, CLASSES))
    self_one, neigh_one, bias_one, self_two, neigh_two, bias_two = pl.pallas_call(
        unpack_kernel,
        out_shape=[jax.ShapeDtypeStruct(shape, jnp.float32) for shape in shapes],
        name="unpack",
    )(packed)
    return self_one, neigh_one, bias_one.reshape(-1), self_two.T, neigh_two.T, bias_two.reshape(-1)


def sum_kernel(mine, total, other, send_p, recv_p, send_z, recv_z, core_send, core_recv,
               p_send, p_recv, z_send, z_recv, g_send, g_recv, h_send, h_recv):
    dom = lax.axis_index("dom")
    y = lax.axis_index("rep")
    core = lax.rem(dom, 2)
    z = lax.rem(lax.div(dom, 2), 8)
    x = lax.div(dom, 16)
    place = x * 4 + y

    def device(at, to_z, to_core):
        return ((lax.div(at, 4) * 8 + to_z) * 2 + to_core, lax.rem(at, 4))

    partner = device(place, z, 1 - core)

    def above(step):
        return lax.rem(place + step, 16)

    def below(step):
        return lax.rem(place - step + 16, 16)

    def z_peer(step):
        return device(place, lax.rem(z + step, 8), core)

    barrier = pltpu.get_barrier_semaphore()
    pl.semaphore_signal(barrier, inc=1, device_id=partner, device_id_type=MESH)

    @pl.loop(1, 16)
    def _(step):
        pl.semaphore_signal(
            barrier, inc=1, device_id=device(above(step), z, core), device_id_type=MESH
        )

    @pl.loop(1, 8)
    def _(step):
        pl.semaphore_signal(barrier, inc=1, device_id=z_peer(step), device_id_type=MESH)

    pl.semaphore_wait(barrier, 23)

    swap = pltpu.make_async_remote_copy(
        src_ref=mine.at[1 - core], dst_ref=other, send_sem=core_send, recv_sem=core_recv,
        device_id=partner, device_id_type=MESH,
    )
    swap.start()
    swap.wait()

    @pl.loop(0, 16)
    def _(part):
        send_p[part] = (mine[core, part] + other[part]).astype(jnp.bfloat16)

    def plane_copy(step):
        return pltpu.make_async_remote_copy(
            src_ref=send_p.at[above(step)], dst_ref=recv_p.at[step], send_sem=p_send.at[step],
            recv_sem=p_recv.at[step], device_id=device(above(step), z, core), device_id_type=MESH,
        )

    @pl.loop(1, 16)
    def _(step):
        plane_copy(step).start()

    kept = mine[core, place] + other[place]

    @pl.loop(1, 16)
    def _(step):
        plane_copy(step).wait()

    def add_plane(step, value):
        return value + recv_p[step].astype(jnp.float32)

    send_z[...] = lax.fori_loop(1, 16, add_plane, kept).astype(jnp.bfloat16)

    def z_copy(step):
        return pltpu.make_async_remote_copy(
            src_ref=send_z, dst_ref=recv_z.at[step], send_sem=z_send.at[step],
            recv_sem=z_recv.at[step], device_id=z_peer(step), device_id_type=MESH,
        )

    @pl.loop(1, 8)
    def _(step):
        z_copy(step).start()

    recv_z[0] = send_z[...]

    @pl.loop(1, 8)
    def _(step):
        z_copy(step).wait()

    def add_z(of_z, value):
        step = lax.rem(z - of_z + 8, 8)
        return value + recv_z[step].astype(jnp.float32)

    total[core, place] = lax.fori_loop(0, 8, add_z, jnp.zeros_like(kept))

    def plane_back(step):
        return pltpu.make_async_remote_copy(
            src_ref=total.at[core, place], dst_ref=total.at[core, place], send_sem=g_send.at[step],
            recv_sem=g_recv.at[step], device_id=device(above(step), z, core), device_id_type=MESH,
        )

    def hand_on(step):
        return pltpu.make_async_remote_copy(
            src_ref=total.at[core, below(step)], dst_ref=total.at[core, below(step)],
            send_sem=h_send.at[step], recv_sem=h_recv.at[step], device_id=partner,
            device_id_type=MESH,
        )

    @pl.loop(1, 16)
    def _(step):
        plane_back(step).start()

    hand_on(0).start()

    @pl.loop(1, 16)
    def _(step):
        plane_back(step).wait()
        hand_on(step).start()

    @pl.loop(0, 16)
    def _(step):
        hand_on(step).wait()


def sum_all(packed):
    vmem = pl.BlockSpec(memory_space=pltpu.VMEM)
    dma = pltpu.SemaphoreType.DMA
    return pl.pallas_call(
        sum_kernel,
        out_shape=jax.ShapeDtypeStruct((2, 16, PIECE, 128), jnp.float32),
        in_specs=[vmem],
        out_specs=vmem,
        scratch_shapes=[
            pltpu.VMEM((16, PIECE, 128), jnp.float32),
            pltpu.VMEM((16, PIECE, 128), jnp.bfloat16),
            pltpu.VMEM((16, PIECE, 128), jnp.bfloat16),
            pltpu.VMEM((PIECE, 128), jnp.bfloat16),
            pltpu.VMEM((8, PIECE, 128), jnp.bfloat16),
            dma, dma, dma((16,)), dma((16,)), dma((8,)), dma((8,)),
            dma((16,)), dma((16,)), dma((16,)), dma((16,)),
        ],
        compiler_params=pltpu.CompilerParams(collective_id=1, has_side_effects=True),
        name="sum_all",
    )(packed)


def shards(
    features,
    partition_map,
    seed_ids,
    hop1_ids,
    hop2_ids,
    labels,
    self_one,
    neigh_one,
    bias_one,
    self_two,
    neigh_two,
    bias_two,
):
    ids = jnp.concatenate(
        [
            seed_ids[None, :],
            hop1_ids.T,
            hop2_ids.transpose(2, 1, 0).reshape(FAN2 * FAN1, SEEDS),
        ],
        axis=0,
    )
    place, returned, hubs = fetch(ids, partition_map, features)
    hubs = hubs.reshape(OWNERS * HOT_DEV, 128)
    seed_loss, packed = sage(
        place, returned, hubs, labels, self_one, neigh_one, bias_one, self_two, neigh_two, bias_two
    )
    total = sum_all(packed.reshape(2, 16, PIECE, 128))
    return (seed_loss, *unpack(total.reshape(ROWS, 128)))


def solution(mesh):
    return jax.shard_map(
        shards,
        mesh=mesh,
        in_specs=(
            P("dom", None),
            P(),
            P(("dom", "rep")),
            P(("dom", "rep"), None),
            P(("dom", "rep"), None, None),
            P(("dom", "rep")),
            P(),
            P(),
            P(),
            P(),
            P(),
            P(),
        ),
        out_specs=(P(("dom", "rep")), P(), P(), P(), P(), P(), P()),
        check_vma=False,
    )
```

```python
import functools

import jax
import jax.numpy as jnp
from jax import lax
from jax.experimental import pallas as pl
from jax.experimental.pallas import tpu as pltpu
from jax.sharding import PartitionSpec as P

MESH = pl.DeviceIdType.MESH
HOT_DEV = 256
NODE_DEV = 8192
OWNERS = 64
CAP = 83
SEEDS = 64
FAN1 = 15
FAN2 = 10
HOPS = SEEDS * FAN1
CLASSES = 172
BLOCK = 128
GROUP = 4
CHUNK = 16
ROWS = 1280
PIECE = ROWS // 32
VMEM_LIMIT = 30 * 1024 * 1024
SMALL_VMEM_LIMIT = 8 * 1024 * 1024


def fetch_kernel(blocks, lines, ids, table, features, place_out, returned, hubs, found, kept_place,
                 counts, request, wide, picked, sending, arrived, wanted, ask_send, ask_recv, row_send,
                 row_recv, local_sem, z_send, z_recv, x_send, x_recv, core_send, core_recv):
    dom = lax.axis_index("dom")
    y = lax.axis_index("rep")
    core = lax.rem(dom, 2)
    z = lax.rem(lax.div(dom, 2), 8)
    x = lax.div(dom, 16)

    def peer(step):
        return lax.rem(dom + step, OWNERS)

    def at_z(offset):
        return lax.rem(z + offset + 8, 8)

    def at_x(offset):
        return lax.rem(x + offset + 4, 4)

    barrier = pltpu.get_barrier_semaphore()

    @pl.loop(1, OWNERS)
    def _(step):
        pl.semaphore_signal(barrier, inc=1, device_id=(peer(step), y), device_id_type=MESH)

    def hub_z(step, way):
        place = hubs.at[core, x, at_z(-way * (step - 1))]
        if step == 4:
            place = place.at[pl.ds(0 if way > 0 else HOT_DEV // 2, HOT_DEV // 2)]
        slot = step - 1 + (0 if way > 0 else 4)
        return pltpu.make_async_remote_copy(
            src_ref=place, dst_ref=place, send_sem=z_send.at[slot], recv_sem=z_recv.at[slot],
            device_id=((x * 8 + at_z(way)) * 2 + core, y), device_id_type=MESH,
        )

    def hub_x(offset, way, hop):
        place = hubs.at[core, at_x(-way * hop), at_z(offset)]
        slot = (offset + 3) + (0 if way > 0 else 8) + 16 * hop
        return pltpu.make_async_remote_copy(
            src_ref=place, dst_ref=place, send_sem=x_send.at[slot], recv_sem=x_recv.at[slot],
            device_id=((at_x(way) * 8 + z) * 2 + core, y), device_id_type=MESH,
        )

    def hub_core(offset):
        place = hubs.at[core, at_x(offset)]
        return pltpu.make_async_remote_copy(
            src_ref=place, dst_ref=place, send_sem=core_send.at[offset + 1],
            recv_sem=core_recv.at[offset + 1],
            device_id=((x * 8 + z) * 2 + 1 - core, y), device_id_type=MESH,
        )

    def turn(step):
        if step == 0:
            pl.semaphore_wait(barrier, OWNERS - 1)
        else:
            for way in (1, -1):
                hub_z(step, way).wait()
        if step < 4:
            for way in (1, -1):
                hub_z(step + 1, way).start()
        for offset in (0,) if step == 0 else (-step, step) if step < 4 else (4,):
            for way in (1, -1):
                hub_x(offset, way, 0).start()
        if step == 4:
            hub_core(0).start()

    hubs[core, x, z] = features[0:HOT_DEV]
    wide[...] = features[...].astype(jnp.float32)

    square_row = lax.broadcasted_iota(jnp.int32, (BLOCK, BLOCK), 0)
    square_col = lax.broadcasted_iota(jnp.int32, (BLOCK, BLOCK), 1)
    diagonal = square_row == square_col
    before = jnp.concatenate(
        [(square_row < square_col).astype(jnp.bfloat16), jnp.ones((BLOCK, BLOCK), jnp.bfloat16)],
        axis=1,
    )
    owner_row = lax.broadcasted_iota(jnp.int32, (OWNERS, BLOCK), 0)
    groups = ids.shape[0] // GROUP
    found[...] = jnp.zeros_like(found)
    kept_place[...] = jnp.zeros_like(kept_place)
    counts[...] = jnp.zeros_like(counts)

    def spread(position, valid):
        owner = lax.shift_right_logical(position, 13)
        row = position & (NODE_DEV - 1)
        cold = (row >= HOT_DEV) & valid
        member = ((owner_row == owner) & cold).astype(jnp.float32)
        return owner, row, cold, member

    def step(group, base):
        old = [kept_place[pl.ds(8 * g, 2)] for g in range(GROUP)]
        rows = [found[BLOCK * g : BLOCK * (g + 1)] for g in range(GROUP)]
        from_row = jnp.minimum(group, groups - 1) * GROUP
        for g in range(GROUP):
            for at in range(BLOCK):
                found[pl.ds(BLOCK * g + at, 1)] = table[lines[from_row + g, at]]
        last_row = jnp.maximum(group - 1, 0) * GROUP
        ids_row = jnp.minimum(last_row, (groups - 1) * GROUP)
        spreads = []
        for g in range(GROUP):
            valid = (group >= 1) & (last_row + g < blocks)
            lane_row = ids[pl.ds(ids_row + g, 1)] & (BLOCK - 1)
            turned = rows[g].T
            position = jnp.sum(jnp.where(square_row == lane_row, turned, 0), axis=0, keepdims=True)
            spreads.append((position, *spread(position, valid)))
        members = jnp.concatenate([one[4].astype(jnp.bfloat16) for one in spreads], axis=0)
        counted_all = jnp.dot(members, before, preferred_element_type=jnp.float32)
        for g in range(GROUP):
            position, owner, row, cold, member = spreads[g]
            counted = counted_all[OWNERS * g : OWNERS * (g + 1)]
            rank = jnp.sum((counted[:, :BLOCK] + base) * member, axis=0, keepdims=True)
            slot = jnp.clip(rank.astype(jnp.int32), 0, CAP - 1)
            hub_place = (
                (owner & 1) * (OWNERS // 2 * HOT_DEV)
                + lax.shift_right_logical(owner, 1) * HOT_DEV
                + jnp.minimum(row, HOT_DEV - 1)
            )
            place = jnp.where(cold, owner * CAP + slot, OWNERS * CAP + hub_place)
            place_out[pl.ds(last_row + g, 1)] = place
            kept_place[pl.ds(8 * g, 1)] = position
            kept_place[pl.ds(8 * g + 1, 1)] = slot
            base = base + counted[:, BLOCK:]
        old_group = (group - 2) * GROUP
        boths = []
        picks = []
        for g in range(GROUP):
            valid = (group >= 2) & (old_group + g < blocks)
            _, row, _, member = spread(old[g][0:1], valid)
            picks.append((square_row == old[g][1:2]).astype(jnp.bfloat16))
            high = member * lax.shift_right_logical(row, 8).astype(jnp.float32)
            low = member * (row & 255).astype(jnp.float32)
            boths.append(jnp.concatenate([high, low], axis=0).astype(jnp.bfloat16))
        counts[...] += lax.dot_general(
            jnp.concatenate(boths, axis=1), jnp.concatenate(picks, axis=1),
            (((1,), (1,)), ((), ())), preferred_element_type=jnp.float32,
        )
        for at in range(5):
            pl.when(group == 3 + 4 * at)(functools.partial(turn, at))
        return base

    lax.fori_loop(0, groups + 2, step, jnp.zeros((OWNERS, BLOCK), jnp.float32))
    flat = (counts[0:OWNERS] * 256.0 + counts[OWNERS:]).astype(jnp.int32) & (NODE_DEV - 1)
    for owner in range(OWNERS):
        request[owner] = flat[owner : owner + 1]

    def distance(slot):
        turn_z = lax.div(slot, 8)
        ahead = lax.div(turn_z + 1, 2)
        dz = jnp.where(lax.rem(turn_z, 2) == 1, ahead, 8 - ahead)
        return lax.div(lax.rem(slot, 8), 2), dz, lax.rem(slot, 2)

    def owner_at(slot):
        dx, dz, dc = distance(slot)
        return (lax.rem(x + dx, 4) * 8 + lax.rem(z + dz, 8)) * 2 + lax.rem(core + dc, 2)

    def asker_at(slot):
        dx, dz, dc = distance(slot)
        return (lax.rem(x - dx + 4, 4) * 8 + lax.rem(z - dz + 8, 8)) * 2 + lax.rem(core + dc, 2)

    def ask(slot):
        owner = owner_at(slot)
        return pltpu.make_async_remote_copy(
            src_ref=request.at[owner], dst_ref=arrived.at[slot], send_sem=ask_send.at[slot],
            recv_sem=ask_recv.at[slot], device_id=(owner, y), device_id_type=MESH,
        )

    @pl.loop(1, OWNERS)
    def _(slot):
        ask(slot).start()

    arrived[0] = request[dom]

    def down(near):
        first = near * 8
        return pltpu.make_async_copy(
            arrived.at[pl.ds(first, 8)], wanted.at[pl.ds(first, 8)], local_sem.at[near]
        )

    @pl.loop(1, 8)
    def _(slot):
        ask(slot).wait()

    down(0).start()
    order = (0, -1, 1, -2, 2, -3, 3, 4)

    def hub_on():
        for offset in order:
            for way in (1, -1):
                hub_x(offset, way, 0).wait()
            hub_x(offset, 1 if offset <= 0 else -1, 1).start()
        hub_core(-1).start()
        hub_core(1).start()

    def gather(slot):
        for at in range(CAP):
            picked[pl.ds(at, 1)] = wide[pl.ds(wanted[slot, 0, at], 1)]
        return picked[0:CAP].astype(jnp.bfloat16)

    def answer(slot):
        return pltpu.make_async_remote_copy(
            src_ref=sending.at[slot], dst_ref=returned.at[dom], send_sem=row_send.at[slot],
            recv_sem=row_recv.at[slot], device_id=(asker_at(slot), y), device_id_type=MESH,
        )

    @pl.loop(0, 8)
    def _(near):
        down(near).wait()

        @pl.when(near < 7)
        def _():
            @pl.loop(0, 8)
            def _(at):
                ask(near * 8 + 8 + at).wait()

            down(near + 1).start()

        @pl.loop(0, 8)
        def _(at):
            slot = near * 8 + at
            sending[slot] = gather(slot)

            @pl.when(slot >= 2)
            def _():
                answer(slot - 1).start()

        pl.when(near == 6)(hub_on)

    answer(OWNERS - 1).start()
    returned[dom] = sending[0]

    for offset in order:
        hub_x(offset, 1 if offset <= 0 else -1, 1).wait()
    hub_core(2).start()
    for offset in (0, -1, 1, 2):
        hub_core(offset).wait()

    @pl.loop(1, OWNERS)
    def _(slot):
        answer(slot).wait()


def fetch(ids, partition_map, features):
    blocks = ids.shape[0] * ids.shape[1] // BLOCK
    padded = -(-blocks // GROUP) * GROUP
    ids = jnp.pad(ids.reshape(blocks, BLOCK), ((0, padded - blocks), (0, 0)))
    lines = lax.shift_right_logical(ids, 7)
    vmem = pl.BlockSpec(memory_space=pltpu.VMEM)
    dma = pltpu.SemaphoreType.DMA
    return pl.pallas_call(
        functools.partial(fetch_kernel, blocks),
        out_shape=[
            jax.ShapeDtypeStruct((padded + GROUP, BLOCK), jnp.int32),
            jax.ShapeDtypeStruct((OWNERS, CAP, 128), jnp.bfloat16),
            jax.ShapeDtypeStruct((2, 4, 8, HOT_DEV, 128), jnp.bfloat16),
        ],
        in_specs=[pl.BlockSpec(memory_space=pltpu.SMEM), vmem, vmem, vmem],
        out_specs=[vmem, vmem, vmem],
        scratch_shapes=[
            pltpu.VMEM((GROUP * BLOCK, BLOCK), jnp.int32),
            pltpu.VMEM((GROUP * 8, BLOCK), jnp.int32),
            pltpu.VMEM((BLOCK, BLOCK), jnp.float32),
            pltpu.VMEM((OWNERS, 1, BLOCK), jnp.int32),
            pltpu.VMEM(features.shape, jnp.float32),
            pltpu.VMEM((88, 128), jnp.float32),
            pltpu.VMEM((OWNERS, CAP, 128), jnp.bfloat16),
            pltpu.VMEM((OWNERS, 1, BLOCK), jnp.int32),
            pltpu.SMEM((OWNERS, 1, BLOCK), jnp.int32),
            dma((OWNERS,)), dma((OWNERS,)), dma((OWNERS,)), dma((OWNERS,)), dma((8,)),
            dma((8,)), dma((8,)), dma((32,)), dma((32,)), dma((4,)), dma((4,)),
        ],
        compiler_params=pltpu.CompilerParams(
            collective_id=2, has_side_effects=True, vmem_limit_bytes=VMEM_LIMIT
        ),
        name="fetch",
    )(lines, ids, partition_map.reshape(-1, 1, BLOCK), features)


def dot(a, b, dims):
    return lax.dot_general(a, b, (dims, ((), ())), preferred_element_type=jnp.float32)


def gelu_parts(x):
    scale = 0.7978845608028654
    square = x * x
    t = jnp.tanh(scale * x * (1.0 + 0.044715 * square))
    half = 0.5 * (1.0 + t)
    slope = half + 0.5 * x * (1.0 - t * t) * (scale * (1.0 + 3.0 * 0.044715 * square))
    return x * half, slope


def sage_kernel(place, returned, hubs, labels, self_one, neigh_one, bias_one, self_two, neigh_two,
                bias_two, loss_out, packed, table, rows, far):
    for owner in range(OWNERS):
        table[CAP * owner : CAP * (owner + 1)] = returned[owner].astype(jnp.float32)
    table[CAP * OWNERS :] = hubs[...].astype(jnp.float32)

    @pl.loop(0, (SEEDS + HOPS) // 64)
    def _(block):
        first = pl.multiple_of(block * 64, 64)
        for at in range(64):
            rows[pl.ds(first + at, 1)] = table[pl.ds(place[first + at], 1)]

    @pl.loop(0, HOPS // CHUNK)
    def _(block):
        first = pl.multiple_of(block * CHUNK, CHUNK)
        for at in range(CHUNK):
            value = None
            for k in range(FAN2):
                row = table[pl.ds(place[first + (SEEDS + HOPS + k * HOPS + at)], 1)]
                value = row if value is None else value + row
            far[pl.ds(first + at, 1)] = value

    seed_rows = rows[0:SEEDS].astype(jnp.bfloat16)
    hop_rows = rows[SEEDS:].astype(jnp.bfloat16)
    far_mean = (far[...] * (1.0 / FAN2)).astype(jnp.bfloat16)
    seed_sum = rows[SEEDS : 2 * SEEDS]
    for f in range(1, FAN1):
        seed_sum = seed_sum + rows[SEEDS * (f + 1) : SEEDS * (f + 2)]
    seed_mean = (seed_sum * (1.0 / FAN1)).astype(jnp.bfloat16)

    own = jnp.concatenate([seed_rows, hop_rows], axis=0)
    near = jnp.concatenate([seed_mean, far_mean], axis=0)
    both = jnp.concatenate([own, near], axis=1)
    weight = jnp.concatenate([self_one[...], neigh_one[...]], axis=0)
    pre = dot(both, weight, ((1,), (0,))) + bias_one[...]
    act, slope = gelu_parts(pre)
    hid_seed = act[0:SEEDS].astype(jnp.bfloat16)
    hop_sum = act[SEEDS : 2 * SEEDS]
    for f in range(1, FAN1):
        hop_sum = hop_sum + act[SEEDS * (f + 1) : SEEDS * (f + 2)]
    hop_mean = (hop_sum * (1.0 / FAN1)).astype(jnp.bfloat16)

    logits = (
        dot(hid_seed, self_two[...], ((1,), (1,)))
        + dot(hop_mean, neigh_two[...], ((1,), (1,)))
        + bias_two[...]
    )
    shifted = logits - jnp.max(logits, axis=1, keepdims=True)
    exps = jnp.exp(shifted)
    sums = jnp.sum(exps, axis=1, keepdims=True)
    log_probs = shifted - jnp.log(sums)
    small_row = lax.broadcasted_iota(jnp.int32, (SEEDS, SEEDS), 0)
    small_col = lax.broadcasted_iota(jnp.int32, (SEEDS, SEEDS), 1)
    label = jnp.sum(
        jnp.where(small_row == small_col, labels[...].astype(jnp.float32), 0.0),
        axis=1, keepdims=True,
    ).astype(jnp.int32)
    target = lax.broadcasted_iota(jnp.int32, (SEEDS, CLASSES), 1) == label
    picked = jnp.sum(jnp.where(target, log_probs, 0.0), axis=1, keepdims=True)
    loss_out[...] = -jnp.sum(
        jnp.where(small_row == small_col, picked, 0.0), axis=0, keepdims=True
    )
    d_logits32 = (jnp.exp(log_probs) - target.astype(jnp.float32)) * (1.0 / SEEDS)
    d_logits = d_logits32.astype(jnp.bfloat16)

    zeros = jnp.zeros((8, 128), jnp.float32)
    packed[512 + 168 : 512 + 176] = zeros
    packed[688 + 168 : 688 + 176] = zeros
    packed[864 + 168 : 864 + 176] = zeros
    packed[1040 + 168 : 1040 + 176] = zeros
    packed[1216:] = jnp.zeros((ROWS - 1216, 128), jnp.float32)
    grad_self_two = dot(d_logits, hid_seed, ((0,), (0,)))
    packed[512:684] = grad_self_two[:, :128]
    packed[688:860] = grad_self_two[:, 128:]
    grad_neigh_two = dot(d_logits, hop_mean, ((0,), (0,)))
    packed[864:1036] = grad_neigh_two[:, :128]
    packed[1040:1212] = grad_neigh_two[:, 128:]
    grad_bias_two = jnp.sum(d_logits32, axis=0, keepdims=True)
    packed[1218:1219] = grad_bias_two[:, :128]
    packed[1219:1220, 0 : CLASSES - 128] = grad_bias_two[:, 128:]

    d_hid_seed = dot(d_logits, self_two[...], ((1,), (0,)))
    d_hop_mean = dot(d_logits, neigh_two[...], ((1,), (0,))) * (1.0 / FAN1)
    d_hid = jnp.concatenate([d_hid_seed] + [d_hop_mean] * FAN1, axis=0)
    d_pre32 = d_hid * slope
    d_pre = d_pre32.astype(jnp.bfloat16)
    grad_one = dot(both, d_pre, ((0,), (0,)))
    packed[0:128] = grad_one[0:128, :128]
    packed[128:256] = grad_one[0:128, 128:]
    packed[256:384] = grad_one[128:256, :128]
    packed[384:512] = grad_one[128:256, 128:]
    grad_bias_one = jnp.sum(d_pre32, axis=0, keepdims=True)
    packed[1216:1217] = grad_bias_one[:, :128]
    packed[1217:1218] = grad_bias_one[:, 128:]


def sage(place, returned, hubs, labels, self_one, neigh_one, bias_one, self_two, neigh_two, bias_two):
    vmem = pl.BlockSpec(memory_space=pltpu.VMEM)
    loss, packed = pl.pallas_call(
        sage_kernel,
        out_shape=[
            jax.ShapeDtypeStruct((1, SEEDS), jnp.float32),
            jax.ShapeDtypeStruct((ROWS, 128), jnp.float32),
        ],
        in_specs=[pl.BlockSpec(memory_space=pltpu.SMEM)] + [vmem] * 9,
        out_specs=[vmem, vmem],
        scratch_shapes=[
            pltpu.VMEM((OWNERS * (CAP + HOT_DEV), 128), jnp.float32),
            pltpu.VMEM((SEEDS + HOPS, 128), jnp.float32),
            pltpu.VMEM((HOPS, 128), jnp.float32),
        ],
        compiler_params=pltpu.CompilerParams(vmem_limit_bytes=VMEM_LIMIT),
        name="sage",
    )(
        place.reshape(-1), returned, hubs, labels[None, :], self_one, neigh_one, bias_one[None, :],
        self_two.T, neigh_two.T, bias_two[None, :],
    )
    return loss.reshape(-1), packed


def unpack_kernel(packed, self_one, neigh_one, bias_one, self_two, neigh_two, bias_two):
    self_one[:, :128] = packed[0:128]
    self_one[:, 128:] = packed[128:256]
    neigh_one[:, :128] = packed[256:384]
    neigh_one[:, 128:] = packed[384:512]
    self_two[:, :128] = packed[512:684]
    self_two[:, 128:] = packed[688:860]
    neigh_two[:, :128] = packed[864:1036]
    neigh_two[:, 128:] = packed[1040:1212]
    bias_one[:, :128] = packed[1216:1217]
    bias_one[:, 128:] = packed[1217:1218]
    bias_two[:, :128] = packed[1218:1219]
    bias_two[:, 128:] = packed[1219:1220, 0 : CLASSES - 128]


def unpack(packed):
    shapes = ((128, 256), (128, 256), (1, 256), (CLASSES, 256), (CLASSES, 256), (1, CLASSES))
    self_one, neigh_one, bias_one, self_two, neigh_two, bias_two = pl.pallas_call(
        unpack_kernel,
        out_shape=[jax.ShapeDtypeStruct(shape, jnp.float32) for shape in shapes],
        compiler_params=pltpu.CompilerParams(vmem_limit_bytes=SMALL_VMEM_LIMIT),
        name="unpack",
    )(packed)
    return self_one, neigh_one, bias_one.reshape(-1), self_two.T, neigh_two.T, bias_two.reshape(-1)


def sum_kernel(mine, total, other, send_p, recv_p, send_z, recv_z, core_send, core_recv,
               p_send, p_recv, z_send, z_recv, g_send, g_recv, h_send, h_recv):
    dom = lax.axis_index("dom")
    y = lax.axis_index("rep")
    core = lax.rem(dom, 2)
    z = lax.rem(lax.div(dom, 2), 8)
    x = lax.div(dom, 16)
    place = x * 4 + y

    def device(at, to_z, to_core):
        return ((lax.div(at, 4) * 8 + to_z) * 2 + to_core, lax.rem(at, 4))

    partner = device(place, z, 1 - core)

    def above(step):
        return lax.rem(place + step, 16)

    def below(step):
        return lax.rem(place - step + 16, 16)

    def z_peer(step):
        return device(place, lax.rem(z + step, 8), core)

    barrier = pltpu.get_barrier_semaphore()
    pl.semaphore_signal(barrier, inc=1, device_id=partner, device_id_type=MESH)

    @pl.loop(1, 16)
    def _(step):
        pl.semaphore_signal(
            barrier, inc=1, device_id=device(above(step), z, core), device_id_type=MESH
        )

    @pl.loop(1, 8)
    def _(step):
        pl.semaphore_signal(barrier, inc=1, device_id=z_peer(step), device_id_type=MESH)

    pl.semaphore_wait(barrier, 23)

    swap = pltpu.make_async_remote_copy(
        src_ref=mine.at[1 - core], dst_ref=other, send_sem=core_send, recv_sem=core_recv,
        device_id=partner, device_id_type=MESH,
    )
    swap.start()
    swap.wait()

    @pl.loop(0, 16)
    def _(part):
        send_p[part] = (mine[core, part] + other[part]).astype(jnp.bfloat16)

    def plane_copy(step):
        return pltpu.make_async_remote_copy(
            src_ref=send_p.at[above(step)], dst_ref=recv_p.at[step], send_sem=p_send.at[step],
            recv_sem=p_recv.at[step], device_id=device(above(step), z, core), device_id_type=MESH,
        )

    @pl.loop(1, 16)
    def _(step):
        plane_copy(step).start()

    kept = mine[core, place] + other[place]

    @pl.loop(1, 16)
    def _(step):
        plane_copy(step).wait()

    def add_plane(step, value):
        return value + recv_p[step].astype(jnp.float32)

    send_z[...] = lax.fori_loop(1, 16, add_plane, kept).astype(jnp.bfloat16)

    def z_copy(step):
        return pltpu.make_async_remote_copy(
            src_ref=send_z, dst_ref=recv_z.at[step], send_sem=z_send.at[step],
            recv_sem=z_recv.at[step], device_id=z_peer(step), device_id_type=MESH,
        )

    @pl.loop(1, 8)
    def _(step):
        z_copy(step).start()

    recv_z[0] = send_z[...]

    @pl.loop(1, 8)
    def _(step):
        z_copy(step).wait()

    def add_z(of_z, value):
        step = lax.rem(z - of_z + 8, 8)
        return value + recv_z[step].astype(jnp.float32)

    total[core, place] = lax.fori_loop(0, 8, add_z, jnp.zeros_like(kept))

    def plane_back(step):
        return pltpu.make_async_remote_copy(
            src_ref=total.at[core, place], dst_ref=total.at[core, place], send_sem=g_send.at[step],
            recv_sem=g_recv.at[step], device_id=device(above(step), z, core), device_id_type=MESH,
        )

    def hand_on(step):
        return pltpu.make_async_remote_copy(
            src_ref=total.at[core, below(step)], dst_ref=total.at[core, below(step)],
            send_sem=h_send.at[step], recv_sem=h_recv.at[step], device_id=partner,
            device_id_type=MESH,
        )

    @pl.loop(1, 16)
    def _(step):
        plane_back(step).start()

    hand_on(0).start()

    @pl.loop(1, 16)
    def _(step):
        plane_back(step).wait()
        hand_on(step).start()

    @pl.loop(0, 16)
    def _(step):
        hand_on(step).wait()


def sum_all(packed):
    vmem = pl.BlockSpec(memory_space=pltpu.VMEM)
    dma = pltpu.SemaphoreType.DMA
    return pl.pallas_call(
        sum_kernel,
        out_shape=jax.ShapeDtypeStruct((2, 16, PIECE, 128), jnp.float32),
        in_specs=[vmem],
        out_specs=vmem,
        scratch_shapes=[
            pltpu.VMEM((16, PIECE, 128), jnp.float32),
            pltpu.VMEM((16, PIECE, 128), jnp.bfloat16),
            pltpu.VMEM((16, PIECE, 128), jnp.bfloat16),
            pltpu.VMEM((PIECE, 128), jnp.bfloat16),
            pltpu.VMEM((8, PIECE, 128), jnp.bfloat16),
            dma, dma, dma((16,)), dma((16,)), dma((8,)), dma((8,)),
            dma((16,)), dma((16,)), dma((16,)), dma((16,)),
        ],
        compiler_params=pltpu.CompilerParams(
            collective_id=1, has_side_effects=True, vmem_limit_bytes=SMALL_VMEM_LIMIT
        ),
        name="sum_all",
    )(packed)


def shards(
    features,
    partition_map,
    seed_ids,
    hop1_ids,
    hop2_ids,
    labels,
    self_one,
    neigh_one,
    bias_one,
    self_two,
    neigh_two,
    bias_two,
):
    ids = jnp.concatenate(
        [
            seed_ids[None, :],
            hop1_ids.T,
            hop2_ids.transpose(2, 1, 0).reshape(FAN2 * FAN1, SEEDS),
        ],
        axis=0,
    )
    place, returned, hubs = fetch(ids, partition_map, features)
    hubs = hubs.reshape(OWNERS * HOT_DEV, 128)
    seed_loss, packed = sage(
        place, returned, hubs, labels, self_one, neigh_one, bias_one, self_two, neigh_two, bias_two
    )
    total = sum_all(packed.reshape(2, 16, PIECE, 128))
    return (seed_loss, *unpack(total.reshape(ROWS, 128)))


def solution(mesh):
    return jax.shard_map(
        shards,
        mesh=mesh,
        in_specs=(
            P("dom", None),
            P(),
            P(("dom", "rep")),
            P(("dom", "rep"), None),
            P(("dom", "rep"), None, None),
            P(("dom", "rep")),
            P(),
            P(),
            P(),
            P(),
            P(),
            P(),
        ),
        out_specs=(P(("dom", "rep")), P(), P(), P(), P(), P(), P()),
        check_vma=False,
    )
```

```python
import functools

import jax
import jax.numpy as jnp
from jax import lax
from jax.experimental import pallas as pl
from jax.experimental.pallas import tpu as pltpu
from jax.sharding import PartitionSpec as P

MESH = pl.DeviceIdType.MESH
HOT_DEV = 256
NODE_DEV = 8192
OWNERS = 64
CAP = 83
SEEDS = 64
FAN1 = 15
FAN2 = 10
HOPS = SEEDS * FAN1
CLASSES = 172
BLOCK = 128
GROUP = 4
CHUNK = 16
ROWS = 1280
PIECE = ROWS // 32
VMEM_LIMIT = 30 * 1024 * 1024
SMALL_VMEM_LIMIT = 8 * 1024 * 1024


def fetch_kernel(blocks, lines, ids, table, features, place_out, returned, hubs, found, kept_place, counts, request, wide, picked, sending,
                 arrived, wanted, ask_send, ask_recv, row_send, row_recv, local_sem, z_send,
                 z_recv, x_send, x_recv, core_send, core_recv):
    dom = lax.axis_index("dom")
    y = lax.axis_index("rep")
    core = lax.rem(dom, 2)
    z = lax.rem(lax.div(dom, 2), 8)
    x = lax.div(dom, 16)

    def peer(step):
        return lax.rem(dom + step, OWNERS)

    def at_z(offset):
        return lax.rem(z + offset + 8, 8)

    def at_x(offset):
        return lax.rem(x + offset + 4, 4)

    barrier = pltpu.get_barrier_semaphore()

    @pl.loop(1, OWNERS)
    def _(step):
        pl.semaphore_signal(barrier, inc=1, device_id=(peer(step), y), device_id_type=MESH)

    hubs[core, x, z] = features[0:HOT_DEV]

    def hub_z(step, way):
        place = hubs.at[core, x, at_z(-way * (step - 1))]
        if step == 4:
            place = place.at[pl.ds(0 if way > 0 else HOT_DEV // 2, HOT_DEV // 2)]
        slot = step - 1 + (0 if way > 0 else 4)
        return pltpu.make_async_remote_copy(
            src_ref=place, dst_ref=place, send_sem=z_send.at[slot], recv_sem=z_recv.at[slot],
            device_id=((x * 8 + at_z(way)) * 2 + core, y), device_id_type=MESH,
        )

    def hub_x(offset, way, hop):
        place = hubs.at[core, at_x(-way * hop), at_z(offset)]
        slot = (offset + 3) + (0 if way > 0 else 8) + 16 * hop
        return pltpu.make_async_remote_copy(
            src_ref=place, dst_ref=place, send_sem=x_send.at[slot], recv_sem=x_recv.at[slot],
            device_id=((at_x(way) * 8 + z) * 2 + core, y), device_id_type=MESH,
        )

    def hub_core(offset):
        place = hubs.at[core, at_x(offset)]
        return pltpu.make_async_remote_copy(
            src_ref=place, dst_ref=place, send_sem=core_send.at[offset + 1],
            recv_sem=core_recv.at[offset + 1],
            device_id=((x * 8 + z) * 2 + 1 - core, y), device_id_type=MESH,
        )

    def turn(step):
        if step == 0:
            pl.semaphore_wait(barrier, OWNERS - 1)
        else:
            for way in (1, -1):
                hub_z(step, way).wait()
        if step < 4:
            for way in (1, -1):
                hub_z(step + 1, way).start()
        for offset in (0,) if step == 0 else (-step, step) if step < 4 else (4,):
            for way in (1, -1):
                hub_x(offset, way, 0).start()
        if step == 4:
            hub_core(0).start()

    square_row = lax.broadcasted_iota(jnp.int32, (BLOCK, BLOCK), 0)
    square_col = lax.broadcasted_iota(jnp.int32, (BLOCK, BLOCK), 1)
    diagonal = square_row == square_col
    before = jnp.concatenate(
        [(square_row < square_col).astype(jnp.bfloat16), jnp.ones((BLOCK, BLOCK), jnp.bfloat16)],
        axis=1,
    )
    owner_row = lax.broadcasted_iota(jnp.int32, (OWNERS, BLOCK), 0)
    groups = ids.shape[0] // GROUP
    found[...] = jnp.zeros_like(found)
    kept_place[...] = jnp.zeros_like(kept_place)
    counts[...] = jnp.zeros_like(counts)

    def spread(position, valid):
        owner = lax.shift_right_logical(position, 13)
        row = position & (NODE_DEV - 1)
        cold = (row >= HOT_DEV) & valid
        member = ((owner_row == owner) & cold).astype(jnp.float32)
        return owner, row, cold, member

    def step(group, base):
        old = [kept_place[pl.ds(8 * g, 2)] for g in range(GROUP)]
        rows = [found[BLOCK * g : BLOCK * (g + 1)] for g in range(GROUP)]
        from_row = jnp.minimum(group, groups - 1) * GROUP
        for g in range(GROUP):
            for at in range(BLOCK):
                found[pl.ds(BLOCK * g + at, 1)] = table[lines[from_row + g, at]]
        last_row = jnp.maximum(group - 1, 0) * GROUP
        ids_row = jnp.minimum(last_row, (groups - 1) * GROUP)
        spreads = []
        for g in range(GROUP):
            valid = (group >= 1) & (last_row + g < blocks)
            lane_row = ids[pl.ds(ids_row + g, 1)] & (BLOCK - 1)
            turned = rows[g].T
            position = jnp.sum(jnp.where(square_row == lane_row, turned, 0), axis=0, keepdims=True)
            spreads.append((position, *spread(position, valid)))
        members = jnp.concatenate([one[4].astype(jnp.bfloat16) for one in spreads], axis=0)
        counted_all = jnp.dot(members, before, preferred_element_type=jnp.float32)
        for g in range(GROUP):
            position, owner, row, cold, member = spreads[g]
            counted = counted_all[OWNERS * g : OWNERS * (g + 1)]
            rank = jnp.sum((counted[:, :BLOCK] + base) * member, axis=0, keepdims=True)
            slot = jnp.clip(rank.astype(jnp.int32), 0, CAP - 1)
            hub_place = (
                (owner & 1) * (OWNERS // 2 * HOT_DEV)
                + lax.shift_right_logical(owner, 1) * HOT_DEV
                + jnp.minimum(row, HOT_DEV - 1)
            )
            place = jnp.where(cold, owner * CAP + slot, OWNERS * CAP + hub_place)
            place_out[pl.ds(last_row + g, 1)] = place
            kept_place[pl.ds(8 * g, 1)] = position
            kept_place[pl.ds(8 * g + 1, 1)] = slot
            base = base + counted[:, BLOCK:]
        old_group = (group - 2) * GROUP
        boths = []
        picks = []
        for g in range(GROUP):
            valid = (group >= 2) & (old_group + g < blocks)
            _, row, _, member = spread(old[g][0:1], valid)
            picks.append((square_row == old[g][1:2]).astype(jnp.bfloat16))
            high = member * lax.shift_right_logical(row, 8).astype(jnp.float32)
            low = member * (row & 255).astype(jnp.float32)
            boths.append(jnp.concatenate([high, low], axis=0).astype(jnp.bfloat16))
        counts[...] += lax.dot_general(
            jnp.concatenate(boths, axis=1), jnp.concatenate(picks, axis=1),
            (((1,), (1,)), ((), ())), preferred_element_type=jnp.float32,
        )
        for at in range(3):
            pl.when(group == 8 + 6 * at)(functools.partial(turn, at))
        return base

    picked[...] = jnp.zeros_like(picked)
    lax.fori_loop(0, groups + 2, step, jnp.zeros((OWNERS, BLOCK), jnp.float32))
    flat = (counts[0:OWNERS] * 256.0 + counts[OWNERS:]).astype(jnp.int32) & (NODE_DEV - 1)
    for owner in range(OWNERS):
        request[owner] = flat[owner : owner + 1]

    def distance(slot):
        turn_z = lax.div(slot, 8)
        ahead = lax.div(turn_z + 1, 2)
        dz = jnp.where(lax.rem(turn_z, 2) == 1, ahead, 8 - ahead)
        return lax.div(lax.rem(slot, 8), 2), dz, lax.rem(slot, 2)

    def owner_at(slot):
        dx, dz, dc = distance(slot)
        return (lax.rem(x + dx, 4) * 8 + lax.rem(z + dz, 8)) * 2 + lax.rem(core + dc, 2)

    def asker_at(slot):
        dx, dz, dc = distance(slot)
        return (lax.rem(x - dx + 4, 4) * 8 + lax.rem(z - dz + 8, 8)) * 2 + lax.rem(core + dc, 2)

    def ask(slot):
        owner = owner_at(slot)
        return pltpu.make_async_remote_copy(
            src_ref=request.at[owner], dst_ref=arrived.at[slot], send_sem=ask_send.at[slot],
            recv_sem=ask_recv.at[slot], device_id=(owner, y), device_id_type=MESH,
        )

    @pl.loop(1, OWNERS)
    def _(slot):
        ask(slot).start()

    arrived[0] = request[dom]

    def down(near):
        first = near * 8
        return pltpu.make_async_copy(
            arrived.at[pl.ds(first, 8)], wanted.at[pl.ds(first, 8)], local_sem.at[near]
        )

    wide[...] = features[...].astype(jnp.float32)
    turn(3)
    first_near = 3

    @pl.loop(8 * first_near, 8 * first_near + 8)
    def _(slot):
        ask(slot).wait()

    down(first_near).start()
    order = (0, -1, 1, -2, 2, -3, 3, 4)

    def hub_on():
        for offset in order:
            for way in (1, -1):
                hub_x(offset, way, 0).wait()
            hub_x(offset, 1 if offset <= 0 else -1, 1).start()
        hub_core(-1).start()
        hub_core(1).start()

    def answer(slot):
        return pltpu.make_async_remote_copy(
            src_ref=sending.at[slot], dst_ref=returned.at[dom], send_sem=row_send.at[slot],
            recv_sem=row_recv.at[slot], device_id=(asker_at(slot), y), device_id_type=MESH,
        )

    def rounded():
        return picked[0:CAP].astype(jnp.bfloat16)

    @pl.loop(0, 8)
    def _(turn_at):
        near = lax.rem(turn_at + first_near, 8)
        then = lax.rem(near + 1, 8)
        down(near).wait()

        @pl.when(turn_at < 7)
        def _():
            @pl.loop(0, 8)
            def _(at):
                slot = then * 8 + at

                @pl.when(slot > 0)
                def _():
                    ask(slot).wait()

            down(then).start()

        @pl.loop(0, 8)
        def _(at):
            slot = near * 8 + at
            last = lax.rem(slot + OWNERS - 1, OWNERS)
            sending[last] = rounded()
            for of in range(CAP):
                picked[pl.ds(of, 1)] = wide[pl.ds(wanted[slot, 0, of], 1)]

            @pl.when((last > 0) & (slot != 8 * first_near))
            def _():
                answer(last).start()

        pl.when(turn_at == 1)(functools.partial(turn, 4))
        pl.when(turn_at == 6)(hub_on)

    sending[8 * first_near - 1] = rounded()
    answer(8 * first_near - 1).start()
    returned[dom] = sending[0]

    for offset in order:
        hub_x(offset, 1 if offset <= 0 else -1, 1).wait()
    hub_core(2).start()
    for offset in (0, -1, 1, 2):
        hub_core(offset).wait()

    @pl.loop(1, OWNERS)
    def _(slot):
        answer(slot).wait()


def fetch(ids, partition_map, features):
    blocks = ids.shape[0] * ids.shape[1] // BLOCK
    padded = -(-blocks // GROUP) * GROUP
    ids = jnp.pad(ids.reshape(blocks, BLOCK), ((0, padded - blocks), (0, 0)))
    lines = lax.shift_right_logical(ids, 7)
    vmem = pl.BlockSpec(memory_space=pltpu.VMEM)
    dma = pltpu.SemaphoreType.DMA
    return pl.pallas_call(
        functools.partial(fetch_kernel, blocks),
        out_shape=[
            jax.ShapeDtypeStruct((padded + GROUP, BLOCK), jnp.int32),
            jax.ShapeDtypeStruct((OWNERS, CAP, 128), jnp.bfloat16),
            jax.ShapeDtypeStruct((2, 4, 8, HOT_DEV, 128), jnp.bfloat16),
        ],
        in_specs=[pl.BlockSpec(memory_space=pltpu.SMEM), vmem, vmem, vmem],
        out_specs=[vmem, vmem, vmem],
        scratch_shapes=[
            pltpu.VMEM((GROUP * BLOCK, BLOCK), jnp.int32),
            pltpu.VMEM((GROUP * 8, BLOCK), jnp.int32),
            pltpu.VMEM((BLOCK, BLOCK), jnp.float32),
            pltpu.VMEM((OWNERS, 1, BLOCK), jnp.int32),
            pltpu.VMEM(features.shape, jnp.float32),
            pltpu.VMEM((88, 128), jnp.float32),
            pltpu.VMEM((OWNERS, CAP, 128), jnp.bfloat16),
            pltpu.VMEM((OWNERS, 1, BLOCK), jnp.int32),
            pltpu.SMEM((OWNERS, 1, BLOCK), jnp.int32),
            dma((OWNERS,)), dma((OWNERS,)), dma((OWNERS,)), dma((OWNERS,)), dma((8,)),
            dma((8,)), dma((8,)), dma((32,)), dma((32,)), dma((4,)), dma((4,)),
        ],
        compiler_params=pltpu.CompilerParams(
            collective_id=2, has_side_effects=True, vmem_limit_bytes=VMEM_LIMIT
        ),
        name="fetch",
    )(lines, ids, partition_map.reshape(-1, 1, BLOCK), features)


def dot(a, b, dims):
    return lax.dot_general(a, b, (dims, ((), ())), preferred_element_type=jnp.float32)


def gelu_parts(x):
    scale = 0.7978845608028654
    square = x * x
    t = jnp.tanh(scale * x * (1.0 + 0.044715 * square))
    half = 0.5 * (1.0 + t)
    slope = half + 0.5 * x * (1.0 - t * t) * (scale * (1.0 + 3.0 * 0.044715 * square))
    return x * half, slope


def sage_kernel(place, returned, hubs, labels, self_one, neigh_one, bias_one, self_two, neigh_two,
                bias_two, loss_out, packed, table, rows, far):
    for owner in range(OWNERS):
        table[CAP * owner : CAP * (owner + 1)] = returned[owner].astype(jnp.float32)
    table[CAP * OWNERS :] = hubs[...].astype(jnp.float32)

    @pl.loop(0, (SEEDS + HOPS) // 64)
    def _(block):
        first = pl.multiple_of(block * 64, 64)
        for at in range(64):
            rows[pl.ds(first + at, 1)] = table[pl.ds(place[first + at], 1)]

    @pl.loop(0, HOPS // CHUNK)
    def _(block):
        first = pl.multiple_of(block * CHUNK, CHUNK)
        for at in range(CHUNK):
            value = None
            for k in range(FAN2):
                row = table[pl.ds(place[first + (SEEDS + HOPS + k * HOPS + at)], 1)]
                value = row if value is None else value + row
            far[pl.ds(first + at, 1)] = value

    seed_rows = rows[0:SEEDS].astype(jnp.bfloat16)
    hop_rows = rows[SEEDS:].astype(jnp.bfloat16)
    far_mean = (far[...] * (1.0 / FAN2)).astype(jnp.bfloat16)
    seed_sum = rows[SEEDS : 2 * SEEDS]
    for f in range(1, FAN1):
        seed_sum = seed_sum + rows[SEEDS * (f + 1) : SEEDS * (f + 2)]
    seed_mean = (seed_sum * (1.0 / FAN1)).astype(jnp.bfloat16)

    own = jnp.concatenate([seed_rows, hop_rows], axis=0)
    near = jnp.concatenate([seed_mean, far_mean], axis=0)
    both = jnp.concatenate([own, near], axis=1)
    weight = jnp.concatenate([self_one[...], neigh_one[...]], axis=0)
    pre = dot(both, weight, ((1,), (0,))) + bias_one[...]
    act, slope = gelu_parts(pre)
    hid_seed = act[0:SEEDS].astype(jnp.bfloat16)
    hop_sum = act[SEEDS : 2 * SEEDS]
    for f in range(1, FAN1):
        hop_sum = hop_sum + act[SEEDS * (f + 1) : SEEDS * (f + 2)]
    hop_mean = (hop_sum * (1.0 / FAN1)).astype(jnp.bfloat16)

    logits = (
        dot(hid_seed, self_two[...], ((1,), (1,)))
        + dot(hop_mean, neigh_two[...], ((1,), (1,)))
        + bias_two[...]
    )
    shifted = logits - jnp.max(logits, axis=1, keepdims=True)
    exps = jnp.exp(shifted)
    sums = jnp.sum(exps, axis=1, keepdims=True)
    log_probs = shifted - jnp.log(sums)
    small_row = lax.broadcasted_iota(jnp.int32, (SEEDS, SEEDS), 0)
    small_col = lax.broadcasted_iota(jnp.int32, (SEEDS, SEEDS), 1)
    label = jnp.sum(
        jnp.where(small_row == small_col, labels[...].astype(jnp.float32), 0.0),
        axis=1, keepdims=True,
    ).astype(jnp.int32)
    target = lax.broadcasted_iota(jnp.int32, (SEEDS, CLASSES), 1) == label
    picked = jnp.sum(jnp.where(target, log_probs, 0.0), axis=1, keepdims=True)
    loss_out[...] = -jnp.sum(
        jnp.where(small_row == small_col, picked, 0.0), axis=0, keepdims=True
    )
    d_logits32 = (jnp.exp(log_probs) - target.astype(jnp.float32)) * (1.0 / SEEDS)
    d_logits = d_logits32.astype(jnp.bfloat16)

    zeros = jnp.zeros((8, 128), jnp.float32)
    packed[512 + 168 : 512 + 176] = zeros
    packed[688 + 168 : 688 + 176] = zeros
    packed[864 + 168 : 864 + 176] = zeros
    packed[1040 + 168 : 1040 + 176] = zeros
    packed[1216:] = jnp.zeros((ROWS - 1216, 128), jnp.float32)
    grad_self_two = dot(d_logits, hid_seed, ((0,), (0,)))
    packed[512:684] = grad_self_two[:, :128]
    packed[688:860] = grad_self_two[:, 128:]
    grad_neigh_two = dot(d_logits, hop_mean, ((0,), (0,)))
    packed[864:1036] = grad_neigh_two[:, :128]
    packed[1040:1212] = grad_neigh_two[:, 128:]
    grad_bias_two = jnp.sum(d_logits32, axis=0, keepdims=True)
    packed[1218:1219] = grad_bias_two[:, :128]
    packed[1219:1220, 0 : CLASSES - 128] = grad_bias_two[:, 128:]

    d_hid_seed = dot(d_logits, self_two[...], ((1,), (0,)))
    d_hop_mean = dot(d_logits, neigh_two[...], ((1,), (0,))) * (1.0 / FAN1)
    d_hid = jnp.concatenate([d_hid_seed] + [d_hop_mean] * FAN1, axis=0)
    d_pre32 = d_hid * slope
    d_pre = d_pre32.astype(jnp.bfloat16)
    grad_one = dot(both, d_pre, ((0,), (0,)))
    packed[0:128] = grad_one[0:128, :128]
    packed[128:256] = grad_one[0:128, 128:]
    packed[256:384] = grad_one[128:256, :128]
    packed[384:512] = grad_one[128:256, 128:]
    grad_bias_one = jnp.sum(d_pre32, axis=0, keepdims=True)
    packed[1216:1217] = grad_bias_one[:, :128]
    packed[1217:1218] = grad_bias_one[:, 128:]


def sage(place, returned, hubs, labels, self_one, neigh_one, bias_one, self_two, neigh_two, bias_two):
    vmem = pl.BlockSpec(memory_space=pltpu.VMEM)
    loss, packed = pl.pallas_call(
        sage_kernel,
        out_shape=[
            jax.ShapeDtypeStruct((1, SEEDS), jnp.float32),
            jax.ShapeDtypeStruct((ROWS, 128), jnp.float32),
        ],
        in_specs=[pl.BlockSpec(memory_space=pltpu.SMEM)] + [vmem] * 9,
        out_specs=[vmem, vmem],
        scratch_shapes=[
            pltpu.VMEM((OWNERS * (CAP + HOT_DEV), 128), jnp.float32),
            pltpu.VMEM((SEEDS + HOPS, 128), jnp.float32),
            pltpu.VMEM((HOPS, 128), jnp.float32),
        ],
        compiler_params=pltpu.CompilerParams(vmem_limit_bytes=VMEM_LIMIT),
        name="sage",
    )(
        place.reshape(-1), returned, hubs, labels[None, :], self_one, neigh_one, bias_one[None, :],
        self_two.T, neigh_two.T, bias_two[None, :],
    )
    return loss.reshape(-1), packed


def unpack_kernel(packed, self_one, neigh_one, bias_one, self_two, neigh_two, bias_two):
    self_one[:, :128] = packed[0:128]
    self_one[:, 128:] = packed[128:256]
    neigh_one[:, :128] = packed[256:384]
    neigh_one[:, 128:] = packed[384:512]
    self_two[:, :128] = packed[512:684]
    self_two[:, 128:] = packed[688:860]
    neigh_two[:, :128] = packed[864:1036]
    neigh_two[:, 128:] = packed[1040:1212]
    bias_one[:, :128] = packed[1216:1217]
    bias_one[:, 128:] = packed[1217:1218]
    bias_two[:, :128] = packed[1218:1219]
    bias_two[:, 128:] = packed[1219:1220, 0 : CLASSES - 128]


def unpack(packed):
    shapes = ((128, 256), (128, 256), (1, 256), (CLASSES, 256), (CLASSES, 256), (1, CLASSES))
    self_one, neigh_one, bias_one, self_two, neigh_two, bias_two = pl.pallas_call(
        unpack_kernel,
        out_shape=[jax.ShapeDtypeStruct(shape, jnp.float32) for shape in shapes],
        compiler_params=pltpu.CompilerParams(vmem_limit_bytes=SMALL_VMEM_LIMIT),
        name="unpack",
    )(packed)
    return self_one, neigh_one, bias_one.reshape(-1), self_two.T, neigh_two.T, bias_two.reshape(-1)


def sum_kernel(mine, total, other, send_p, recv_p, send_z, recv_z, core_send, core_recv,
               p_send, p_recv, z_send, z_recv, g_send, g_recv, h_send, h_recv):
    dom = lax.axis_index("dom")
    y = lax.axis_index("rep")
    core = lax.rem(dom, 2)
    z = lax.rem(lax.div(dom, 2), 8)
    x = lax.div(dom, 16)
    place = x * 4 + y

    def device(at, to_z, to_core):
        return ((lax.div(at, 4) * 8 + to_z) * 2 + to_core, lax.rem(at, 4))

    partner = device(place, z, 1 - core)

    def above(step):
        return lax.rem(place + step, 16)

    def below(step):
        return lax.rem(place - step + 16, 16)

    def z_peer(step):
        return device(place, lax.rem(z + step, 8), core)

    barrier = pltpu.get_barrier_semaphore()
    pl.semaphore_signal(barrier, inc=1, device_id=partner, device_id_type=MESH)

    @pl.loop(1, 16)
    def _(step):
        pl.semaphore_signal(
            barrier, inc=1, device_id=device(above(step), z, core), device_id_type=MESH
        )

    @pl.loop(1, 8)
    def _(step):
        pl.semaphore_signal(barrier, inc=1, device_id=z_peer(step), device_id_type=MESH)

    pl.semaphore_wait(barrier, 23)

    swap = pltpu.make_async_remote_copy(
        src_ref=mine.at[1 - core], dst_ref=other, send_sem=core_send, recv_sem=core_recv,
        device_id=partner, device_id_type=MESH,
    )
    swap.start()
    swap.wait()

    @pl.loop(0, 16)
    def _(part):
        send_p[part] = (mine[core, part] + other[part]).astype(jnp.bfloat16)

    def plane_copy(step):
        return pltpu.make_async_remote_copy(
            src_ref=send_p.at[above(step)], dst_ref=recv_p.at[step], send_sem=p_send.at[step],
            recv_sem=p_recv.at[step], device_id=device(above(step), z, core), device_id_type=MESH,
        )

    @pl.loop(1, 16)
    def _(step):
        plane_copy(step).start()

    kept = mine[core, place] + other[place]

    @pl.loop(1, 16)
    def _(step):
        plane_copy(step).wait()

    def add_plane(step, value):
        return value + recv_p[step].astype(jnp.float32)

    send_z[...] = lax.fori_loop(1, 16, add_plane, kept).astype(jnp.bfloat16)

    def z_copy(step):
        return pltpu.make_async_remote_copy(
            src_ref=send_z, dst_ref=recv_z.at[step], send_sem=z_send.at[step],
            recv_sem=z_recv.at[step], device_id=z_peer(step), device_id_type=MESH,
        )

    @pl.loop(1, 8)
    def _(step):
        z_copy(step).start()

    recv_z[0] = send_z[...]

    @pl.loop(1, 8)
    def _(step):
        z_copy(step).wait()

    def add_z(of_z, value):
        step = lax.rem(z - of_z + 8, 8)
        return value + recv_z[step].astype(jnp.float32)

    total[core, place] = lax.fori_loop(0, 8, add_z, jnp.zeros_like(kept))

    def plane_back(step):
        return pltpu.make_async_remote_copy(
            src_ref=total.at[core, place], dst_ref=total.at[core, place], send_sem=g_send.at[step],
            recv_sem=g_recv.at[step], device_id=device(above(step), z, core), device_id_type=MESH,
        )

    def hand_on(step):
        return pltpu.make_async_remote_copy(
            src_ref=total.at[core, below(step)], dst_ref=total.at[core, below(step)],
            send_sem=h_send.at[step], recv_sem=h_recv.at[step], device_id=partner,
            device_id_type=MESH,
        )

    @pl.loop(1, 16)
    def _(step):
        plane_back(step).start()

    hand_on(0).start()

    @pl.loop(1, 16)
    def _(step):
        plane_back(step).wait()
        hand_on(step).start()

    @pl.loop(0, 16)
    def _(step):
        hand_on(step).wait()


def sum_all(packed):
    vmem = pl.BlockSpec(memory_space=pltpu.VMEM)
    dma = pltpu.SemaphoreType.DMA
    return pl.pallas_call(
        sum_kernel,
        out_shape=jax.ShapeDtypeStruct((2, 16, PIECE, 128), jnp.float32),
        in_specs=[vmem],
        out_specs=vmem,
        scratch_shapes=[
            pltpu.VMEM((16, PIECE, 128), jnp.float32),
            pltpu.VMEM((16, PIECE, 128), jnp.bfloat16),
            pltpu.VMEM((16, PIECE, 128), jnp.bfloat16),
            pltpu.VMEM((PIECE, 128), jnp.bfloat16),
            pltpu.VMEM((8, PIECE, 128), jnp.bfloat16),
            dma, dma, dma((16,)), dma((16,)), dma((8,)), dma((8,)),
            dma((16,)), dma((16,)), dma((16,)), dma((16,)),
        ],
        compiler_params=pltpu.CompilerParams(
            collective_id=1, has_side_effects=True, vmem_limit_bytes=SMALL_VMEM_LIMIT
        ),
        name="sum_all",
    )(packed)


def shards(
    features,
    partition_map,
    seed_ids,
    hop1_ids,
    hop2_ids,
    labels,
    self_one,
    neigh_one,
    bias_one,
    self_two,
    neigh_two,
    bias_two,
):
    ids = jnp.concatenate(
        [
            seed_ids[None, :],
            hop1_ids.T,
            hop2_ids.transpose(2, 1, 0).reshape(FAN2 * FAN1, SEEDS),
        ],
        axis=0,
    )
    place, returned, hubs = fetch(ids, partition_map, features)
    hubs = hubs.reshape(OWNERS * HOT_DEV, 128)
    seed_loss, packed = sage(
        place, returned, hubs, labels, self_one, neigh_one, bias_one, self_two, neigh_two, bias_two
    )
    total = sum_all(packed.reshape(2, 16, PIECE, 128))
    return (seed_loss, *unpack(total.reshape(ROWS, 128)))


def solution(mesh):
    return jax.shard_map(
        shards,
        mesh=mesh,
        in_specs=(
            P("dom", None),
            P(),
            P(("dom", "rep")),
            P(("dom", "rep"), None),
            P(("dom", "rep"), None, None),
            P(("dom", "rep")),
            P(),
            P(),
            P(),
            P(),
            P(),
            P(),
        ),
        out_specs=(P(("dom", "rep")), P(), P(), P(), P(), P(), P()),
        check_vma=False,
    )
```

```python
import functools

import jax
import jax.numpy as jnp
from jax import lax
from jax.experimental import pallas as pl
from jax.experimental.pallas import tpu as pltpu
from jax.sharding import PartitionSpec as P

MESH = pl.DeviceIdType.MESH
HOT_DEV = 256
NODE_DEV = 8192
OWNERS = 64
CAP = 83
CAP_ROWS = 88
SEEDS = 64
FAN1 = 15
FAN2 = 10
HOPS = SEEDS * FAN1
CLASSES = 172
BLOCK = 128
GROUP = 4
CHUNK = 64
ROWS = 1280
PIECE = ROWS // 32
VMEM_LIMIT = 30 * 1024 * 1024
SMALL_VMEM_LIMIT = 8 * 1024 * 1024


def fetch_kernel(blocks, lines, ids, table, features, place_out, returned, hubs, found, kept_place, counts, request, wide, picked, sending,
                 arrived, wanted, ask_send, ask_recv, row_send, row_recv, local_sem, z_send,
                 z_recv, x_send, x_recv, core_send, core_recv):
    dom = lax.axis_index("dom")
    y = lax.axis_index("rep")
    core = lax.rem(dom, 2)
    z = lax.rem(lax.div(dom, 2), 8)
    x = lax.div(dom, 16)

    def peer(step):
        return lax.rem(dom + step, OWNERS)

    def at_z(offset):
        return lax.rem(z + offset + 8, 8)

    def at_x(offset):
        return lax.rem(x + offset + 4, 4)

    barrier = pltpu.get_barrier_semaphore()

    @pl.loop(1, OWNERS)
    def _(step):
        pl.semaphore_signal(barrier, inc=1, device_id=(peer(step), y), device_id_type=MESH)

    hubs[core, x, z] = features[0:HOT_DEV]

    def hub_z(step, way):
        place = hubs.at[core, x, at_z(-way * (step - 1))]
        if step == 4:
            place = place.at[pl.ds(0 if way > 0 else HOT_DEV // 2, HOT_DEV // 2)]
        slot = step - 1 + (0 if way > 0 else 4)
        return pltpu.make_async_remote_copy(
            src_ref=place, dst_ref=place, send_sem=z_send.at[slot], recv_sem=z_recv.at[slot],
            device_id=((x * 8 + at_z(way)) * 2 + core, y), device_id_type=MESH,
        )

    def hub_x(offset, way, hop):
        place = hubs.at[core, at_x(-way * hop), at_z(offset)]
        slot = (offset + 3) + (0 if way > 0 else 8) + 16 * hop
        return pltpu.make_async_remote_copy(
            src_ref=place, dst_ref=place, send_sem=x_send.at[slot], recv_sem=x_recv.at[slot],
            device_id=((at_x(way) * 8 + z) * 2 + core, y), device_id_type=MESH,
        )

    def hub_core(offset):
        place = hubs.at[core, at_x(offset)]
        return pltpu.make_async_remote_copy(
            src_ref=place, dst_ref=place, send_sem=core_send.at[offset + 1],
            recv_sem=core_recv.at[offset + 1],
            device_id=((x * 8 + z) * 2 + 1 - core, y), device_id_type=MESH,
        )

    def turn(step):
        if step == 0:
            pl.semaphore_wait(barrier, OWNERS - 1)
        else:
            for way in (1, -1):
                hub_z(step, way).wait()
        if step < 4:
            for way in (1, -1):
                hub_z(step + 1, way).start()
        for offset in (0,) if step == 0 else (-step, step) if step < 4 else (4,):
            for way in (1, -1):
                hub_x(offset, way, 0).start()
        if step == 4:
            hub_core(0).start()

    square_row = lax.broadcasted_iota(jnp.int32, (BLOCK, BLOCK), 0)
    square_col = lax.broadcasted_iota(jnp.int32, (BLOCK, BLOCK), 1)
    diagonal = square_row == square_col
    before = jnp.concatenate(
        [(square_row < square_col).astype(jnp.bfloat16), jnp.ones((BLOCK, BLOCK), jnp.bfloat16)],
        axis=1,
    )
    owner_row = lax.broadcasted_iota(jnp.int32, (OWNERS, BLOCK), 0)
    groups = ids.shape[0] // GROUP
    found[...] = jnp.zeros_like(found)
    kept_place[...] = jnp.zeros_like(kept_place)
    counts[...] = jnp.zeros_like(counts)

    def spread(position, valid):
        owner = lax.shift_right_logical(position, 13)
        row = position & (NODE_DEV - 1)
        cold = (row >= HOT_DEV) & valid
        member = ((owner_row == owner) & cold).astype(jnp.float32)
        return owner, row, cold, member

    def step(group, base):
        old = [kept_place[pl.ds(8 * g, 2)] for g in range(GROUP)]
        rows = [found[BLOCK * g : BLOCK * (g + 1)] for g in range(GROUP)]
        from_row = jnp.minimum(group, groups - 1) * GROUP
        for g in range(GROUP):
            for at in range(BLOCK):
                found[pl.ds(BLOCK * g + at, 1)] = table[lines[from_row + g, at]]
        last_row = jnp.maximum(group - 1, 0) * GROUP
        ids_row = jnp.minimum(last_row, (groups - 1) * GROUP)
        spreads = []
        for g in range(GROUP):
            valid = (group >= 1) & (last_row + g < blocks)
            lane_row = ids[pl.ds(ids_row + g, 1)] & (BLOCK - 1)
            turned = rows[g].T
            position = jnp.sum(jnp.where(square_row == lane_row, turned, 0), axis=0, keepdims=True)
            spreads.append((position, *spread(position, valid)))
        members = jnp.concatenate([one[4].astype(jnp.bfloat16) for one in spreads], axis=0)
        counted_all = jnp.dot(members, before, preferred_element_type=jnp.float32)
        for g in range(GROUP):
            position, owner, row, cold, member = spreads[g]
            counted = counted_all[OWNERS * g : OWNERS * (g + 1)]
            rank = jnp.sum((counted[:, :BLOCK] + base) * member, axis=0, keepdims=True)
            slot = jnp.clip(rank.astype(jnp.int32), 0, CAP - 1)
            hub_place = (
                (owner & 1) * (OWNERS // 2 * HOT_DEV)
                + lax.shift_right_logical(owner, 1) * HOT_DEV
                + jnp.minimum(row, HOT_DEV - 1)
            )
            place = jnp.where(cold, owner * CAP_ROWS + slot, OWNERS * CAP_ROWS + hub_place)
            place_out[pl.ds(last_row + g, 1)] = place
            kept_place[pl.ds(8 * g, 1)] = position
            kept_place[pl.ds(8 * g + 1, 1)] = slot
            base = base + counted[:, BLOCK:]
        old_group = (group - 2) * GROUP
        boths = []
        picks = []
        for g in range(GROUP):
            valid = (group >= 2) & (old_group + g < blocks)
            _, row, _, member = spread(old[g][0:1], valid)
            picks.append((square_row == old[g][1:2]).astype(jnp.bfloat16))
            high = member * lax.shift_right_logical(row, 8).astype(jnp.float32)
            low = member * (row & 255).astype(jnp.float32)
            boths.append(jnp.concatenate([high, low], axis=0).astype(jnp.bfloat16))
        counts[...] += lax.dot_general(
            jnp.concatenate(boths, axis=1), jnp.concatenate(picks, axis=1),
            (((1,), (1,)), ((), ())), preferred_element_type=jnp.float32,
        )
        for at in range(3):
            pl.when(group == 8 + 6 * at)(functools.partial(turn, at))
        return base

    picked[...] = jnp.zeros_like(picked)
    lax.fori_loop(0, groups + 2, step, jnp.zeros((OWNERS, BLOCK), jnp.float32))
    flat = (counts[0:OWNERS] * 256.0 + counts[OWNERS:]).astype(jnp.int32) & (NODE_DEV - 1)
    for owner in range(OWNERS):
        request[owner] = flat[owner : owner + 1]

    def distance(slot):
        turn_z = lax.div(slot, 8)
        ahead = lax.div(turn_z + 1, 2)
        dz = jnp.where(lax.rem(turn_z, 2) == 1, ahead, 8 - ahead)
        return lax.div(lax.rem(slot, 8), 2), dz, lax.rem(slot, 2)

    def owner_at(slot):
        dx, dz, dc = distance(slot)
        return (lax.rem(x + dx, 4) * 8 + lax.rem(z + dz, 8)) * 2 + lax.rem(core + dc, 2)

    def asker_at(slot):
        dx, dz, dc = distance(slot)
        return (lax.rem(x - dx + 4, 4) * 8 + lax.rem(z - dz + 8, 8)) * 2 + lax.rem(core + dc, 2)

    def ask(slot):
        owner = owner_at(slot)
        return pltpu.make_async_remote_copy(
            src_ref=request.at[owner], dst_ref=arrived.at[slot], send_sem=ask_send.at[slot],
            recv_sem=ask_recv.at[slot], device_id=(owner, y), device_id_type=MESH,
        )

    @pl.loop(1, OWNERS)
    def _(slot):
        ask(slot).start()

    arrived[0] = request[dom]

    def down(near):
        first = near * 8
        return pltpu.make_async_copy(
            arrived.at[pl.ds(first, 8)], wanted.at[pl.ds(first, 8)], local_sem.at[near]
        )

    wide[...] = features[...].astype(jnp.float32)
    turn(3)
    first_near = 3

    @pl.loop(8 * first_near, 8 * first_near + 8)
    def _(slot):
        ask(slot).wait()

    down(first_near).start()
    order = (0, -1, 1, -2, 2, -3, 3, 4)

    def hub_on():
        for offset in order:
            for way in (1, -1):
                hub_x(offset, way, 0).wait()
            hub_x(offset, 1 if offset <= 0 else -1, 1).start()
        hub_core(-1).start()
        hub_core(1).start()

    def answer(slot):
        return pltpu.make_async_remote_copy(
            src_ref=sending.at[slot], dst_ref=returned.at[dom], send_sem=row_send.at[slot],
            recv_sem=row_recv.at[slot], device_id=(asker_at(slot), y), device_id_type=MESH,
        )

    def rounded():
        return picked[0:CAP].astype(jnp.bfloat16)

    @pl.loop(0, 8)
    def _(turn_at):
        near = lax.rem(turn_at + first_near, 8)
        then = lax.rem(near + 1, 8)
        down(near).wait()

        @pl.when(turn_at < 7)
        def _():
            @pl.loop(0, 8)
            def _(at):
                slot = then * 8 + at

                @pl.when(slot > 0)
                def _():
                    ask(slot).wait()

            down(then).start()

        @pl.loop(0, 8)
        def _(at):
            slot = near * 8 + at
            last = lax.rem(slot + OWNERS - 1, OWNERS)
            sending[last] = rounded()
            for of in range(CAP):
                picked[pl.ds(of, 1)] = wide[pl.ds(wanted[slot, 0, of], 1)]

            @pl.when((last > 0) & (slot != 8 * first_near))
            def _():
                answer(last).start()

        pl.when(turn_at == 1)(functools.partial(turn, 4))
        pl.when(turn_at == 6)(hub_on)

    sending[8 * first_near - 1] = rounded()
    answer(8 * first_near - 1).start()
    returned[dom] = sending[0]

    for offset in order:
        hub_x(offset, 1 if offset <= 0 else -1, 1).wait()
    hub_core(2).start()
    for offset in (0, -1, 1, 2):
        hub_core(offset).wait()

    @pl.loop(1, OWNERS)
    def _(slot):
        answer(slot).wait()


def fetch(ids, partition_map, features):
    blocks = ids.shape[0] * ids.shape[1] // BLOCK
    padded = -(-blocks // GROUP) * GROUP
    ids = jnp.pad(ids.reshape(blocks, BLOCK), ((0, padded - blocks), (0, 0)))
    lines = lax.shift_right_logical(ids, 7)
    vmem = pl.BlockSpec(memory_space=pltpu.VMEM)
    dma = pltpu.SemaphoreType.DMA
    return pl.pallas_call(
        functools.partial(fetch_kernel, blocks),
        out_shape=[
            jax.ShapeDtypeStruct((padded + GROUP, BLOCK), jnp.int32),
            jax.ShapeDtypeStruct((OWNERS, CAP, 128), jnp.bfloat16),
            jax.ShapeDtypeStruct((2, 4, 8, HOT_DEV, 128), jnp.bfloat16),
        ],
        in_specs=[pl.BlockSpec(memory_space=pltpu.SMEM), vmem, vmem, vmem],
        out_specs=[vmem, vmem, vmem],
        scratch_shapes=[
            pltpu.VMEM((GROUP * BLOCK, BLOCK), jnp.int32),
            pltpu.VMEM((GROUP * 8, BLOCK), jnp.int32),
            pltpu.VMEM((BLOCK, BLOCK), jnp.float32),
            pltpu.VMEM((OWNERS, 1, BLOCK), jnp.int32),
            pltpu.VMEM(features.shape, jnp.float32),
            pltpu.VMEM((CAP_ROWS, 128), jnp.float32),
            pltpu.VMEM((OWNERS, CAP, 128), jnp.bfloat16),
            pltpu.VMEM((OWNERS, 1, BLOCK), jnp.int32),
            pltpu.SMEM((OWNERS, 1, BLOCK), jnp.int32),
            dma((OWNERS,)), dma((OWNERS,)), dma((OWNERS,)), dma((OWNERS,)), dma((8,)),
            dma((8,)), dma((8,)), dma((32,)), dma((32,)), dma((4,)), dma((4,)),
        ],
        compiler_params=pltpu.CompilerParams(
            collective_id=2, has_side_effects=True, vmem_limit_bytes=VMEM_LIMIT
        ),
        name="fetch",
    )(lines, ids, partition_map.reshape(-1, 1, BLOCK), features)


def dot(a, b, dims):
    return lax.dot_general(a, b, (dims, ((), ())), preferred_element_type=jnp.float32)


def gelu_parts(x):
    scale = 0.7978845608028654
    square = x * x
    t = jnp.tanh(scale * x * (1.0 + 0.044715 * square))
    half = 0.5 * (1.0 + t)
    slope = half + 0.5 * x * (1.0 - t * t) * (scale * (1.0 + 3.0 * 0.044715 * square))
    return x * half, slope


def sage_kernel(place, returned, hubs, labels, self_one, neigh_one, bias_one, self_two, neigh_two,
                bias_two, loss_out, packed, table, rows, far):
    for owner in range(OWNERS):
        first = CAP_ROWS * owner
        table[first : first + CAP] = returned[owner].astype(jnp.float32)
    table[CAP_ROWS * OWNERS :] = hubs[...].astype(jnp.float32)

    @pl.loop(0, (SEEDS + HOPS) // 64)
    def _(block):
        first = pl.multiple_of(block * 64, 64)
        for at in range(64):
            rows[pl.ds(first + at, 1)] = table[pl.ds(place[first + at], 1)]

    @pl.loop(0, HOPS // CHUNK)
    def _(block):
        first = pl.multiple_of(block * CHUNK, CHUNK)
        for at in range(CHUNK):
            value = None
            for k in range(FAN2):
                row = table[pl.ds(place[first + (SEEDS + HOPS + k * HOPS + at)], 1)]
                value = row if value is None else value + row
            far[pl.ds(first + at, 1)] = value

    seed_rows = rows[0:SEEDS].astype(jnp.bfloat16)
    hop_rows = rows[SEEDS:].astype(jnp.bfloat16)
    far_mean = (far[...] * (1.0 / FAN2)).astype(jnp.bfloat16)
    seed_sum = rows[SEEDS : 2 * SEEDS]
    for f in range(1, FAN1):
        seed_sum = seed_sum + rows[SEEDS * (f + 1) : SEEDS * (f + 2)]
    seed_mean = (seed_sum * (1.0 / FAN1)).astype(jnp.bfloat16)

    own = jnp.concatenate([seed_rows, hop_rows], axis=0)
    near = jnp.concatenate([seed_mean, far_mean], axis=0)
    both = jnp.concatenate([own, near], axis=1)
    weight = jnp.concatenate([self_one[...], neigh_one[...]], axis=0)
    pre = dot(both, weight, ((1,), (0,))) + bias_one[...]
    act, slope = gelu_parts(pre)
    hid_seed = act[0:SEEDS].astype(jnp.bfloat16)
    hop_sum = act[SEEDS : 2 * SEEDS]
    for f in range(1, FAN1):
        hop_sum = hop_sum + act[SEEDS * (f + 1) : SEEDS * (f + 2)]
    hop_mean = (hop_sum * (1.0 / FAN1)).astype(jnp.bfloat16)

    logits = (
        dot(hid_seed, self_two[...], ((1,), (1,)))
        + dot(hop_mean, neigh_two[...], ((1,), (1,)))
        + bias_two[...]
    )
    shifted = logits - jnp.max(logits, axis=1, keepdims=True)
    exps = jnp.exp(shifted)
    sums = jnp.sum(exps, axis=1, keepdims=True)
    log_probs = shifted - jnp.log(sums)
    small_row = lax.broadcasted_iota(jnp.int32, (SEEDS, SEEDS), 0)
    small_col = lax.broadcasted_iota(jnp.int32, (SEEDS, SEEDS), 1)
    label = jnp.sum(
        jnp.where(small_row == small_col, labels[...].astype(jnp.float32), 0.0),
        axis=1, keepdims=True,
    ).astype(jnp.int32)
    target = lax.broadcasted_iota(jnp.int32, (SEEDS, CLASSES), 1) == label
    picked = jnp.sum(jnp.where(target, log_probs, 0.0), axis=1, keepdims=True)
    loss_out[...] = -jnp.sum(
        jnp.where(small_row == small_col, picked, 0.0), axis=0, keepdims=True
    )
    d_logits32 = (jnp.exp(log_probs) - target.astype(jnp.float32)) * (1.0 / SEEDS)
    d_logits = d_logits32.astype(jnp.bfloat16)

    zeros = jnp.zeros((8, 128), jnp.float32)
    packed[512 + 168 : 512 + 176] = zeros
    packed[688 + 168 : 688 + 176] = zeros
    packed[864 + 168 : 864 + 176] = zeros
    packed[1040 + 168 : 1040 + 176] = zeros
    packed[1216:] = jnp.zeros((ROWS - 1216, 128), jnp.float32)
    grad_self_two = dot(d_logits, hid_seed, ((0,), (0,)))
    packed[512:684] = grad_self_two[:, :128]
    packed[688:860] = grad_self_two[:, 128:]
    grad_neigh_two = dot(d_logits, hop_mean, ((0,), (0,)))
    packed[864:1036] = grad_neigh_two[:, :128]
    packed[1040:1212] = grad_neigh_two[:, 128:]
    grad_bias_two = jnp.sum(d_logits32, axis=0, keepdims=True)
    packed[1218:1219] = grad_bias_two[:, :128]
    packed[1219:1220, 0 : CLASSES - 128] = grad_bias_two[:, 128:]

    d_hid_seed = dot(d_logits, self_two[...], ((1,), (0,)))
    d_hop_mean = dot(d_logits, neigh_two[...], ((1,), (0,))) * (1.0 / FAN1)
    d_hid = jnp.concatenate([d_hid_seed] + [d_hop_mean] * FAN1, axis=0)
    d_pre32 = d_hid * slope
    d_pre = d_pre32.astype(jnp.bfloat16)
    grad_one = dot(both, d_pre, ((0,), (0,)))
    packed[0:128] = grad_one[0:128, :128]
    packed[128:256] = grad_one[0:128, 128:]
    packed[256:384] = grad_one[128:256, :128]
    packed[384:512] = grad_one[128:256, 128:]
    grad_bias_one = jnp.sum(d_pre32, axis=0, keepdims=True)
    packed[1216:1217] = grad_bias_one[:, :128]
    packed[1217:1218] = grad_bias_one[:, 128:]


def sage(place, returned, hubs, labels, self_one, neigh_one, bias_one, self_two, neigh_two, bias_two):
    vmem = pl.BlockSpec(memory_space=pltpu.VMEM)
    loss, packed = pl.pallas_call(
        sage_kernel,
        out_shape=[
            jax.ShapeDtypeStruct((1, SEEDS), jnp.float32),
            jax.ShapeDtypeStruct((ROWS, 128), jnp.float32),
        ],
        in_specs=[pl.BlockSpec(memory_space=pltpu.SMEM)] + [vmem] * 9,
        out_specs=[vmem, vmem],
        scratch_shapes=[
            pltpu.VMEM((OWNERS * (CAP_ROWS + HOT_DEV), 128), jnp.float32),
            pltpu.VMEM((SEEDS + HOPS, 128), jnp.float32),
            pltpu.VMEM((HOPS, 128), jnp.float32),
        ],
        compiler_params=pltpu.CompilerParams(vmem_limit_bytes=VMEM_LIMIT),
        name="sage",
    )(
        place.reshape(-1), returned, hubs, labels[None, :], self_one, neigh_one, bias_one[None, :],
        self_two.T, neigh_two.T, bias_two[None, :],
    )
    return loss.reshape(-1), packed


def unpack_kernel(packed, self_one, neigh_one, bias_one, self_two, neigh_two, bias_two):
    self_one[:, :128] = packed[0:128]
    self_one[:, 128:] = packed[128:256]
    neigh_one[:, :128] = packed[256:384]
    neigh_one[:, 128:] = packed[384:512]
    self_two[:, :128] = packed[512:684]
    self_two[:, 128:] = packed[688:860]
    neigh_two[:, :128] = packed[864:1036]
    neigh_two[:, 128:] = packed[1040:1212]
    bias_one[:, :128] = packed[1216:1217]
    bias_one[:, 128:] = packed[1217:1218]
    bias_two[:, :128] = packed[1218:1219]
    bias_two[:, 128:] = packed[1219:1220, 0 : CLASSES - 128]


def unpack(packed):
    shapes = ((128, 256), (128, 256), (1, 256), (CLASSES, 256), (CLASSES, 256), (1, CLASSES))
    self_one, neigh_one, bias_one, self_two, neigh_two, bias_two = pl.pallas_call(
        unpack_kernel,
        out_shape=[jax.ShapeDtypeStruct(shape, jnp.float32) for shape in shapes],
        compiler_params=pltpu.CompilerParams(vmem_limit_bytes=SMALL_VMEM_LIMIT),
        name="unpack",
    )(packed)
    return self_one, neigh_one, bias_one.reshape(-1), self_two.T, neigh_two.T, bias_two.reshape(-1)


def sum_kernel(mine, total, other, send_p, recv_p, send_z, recv_z, core_send, core_recv,
               p_send, p_recv, z_send, z_recv, g_send, g_recv, h_send, h_recv):
    dom = lax.axis_index("dom")
    y = lax.axis_index("rep")
    core = lax.rem(dom, 2)
    z = lax.rem(lax.div(dom, 2), 8)
    x = lax.div(dom, 16)
    place = x * 4 + y

    def device(at, to_z, to_core):
        return ((lax.div(at, 4) * 8 + to_z) * 2 + to_core, lax.rem(at, 4))

    partner = device(place, z, 1 - core)

    def above(step):
        return lax.rem(place + step, 16)

    def below(step):
        return lax.rem(place - step + 16, 16)

    def z_peer(step):
        return device(place, lax.rem(z + step, 8), core)

    barrier = pltpu.get_barrier_semaphore()
    pl.semaphore_signal(barrier, inc=1, device_id=partner, device_id_type=MESH)

    @pl.loop(1, 16)
    def _(step):
        pl.semaphore_signal(
            barrier, inc=1, device_id=device(above(step), z, core), device_id_type=MESH
        )

    @pl.loop(1, 8)
    def _(step):
        pl.semaphore_signal(barrier, inc=1, device_id=z_peer(step), device_id_type=MESH)

    pl.semaphore_wait(barrier, 23)

    swap = pltpu.make_async_remote_copy(
        src_ref=mine.at[1 - core], dst_ref=other, send_sem=core_send, recv_sem=core_recv,
        device_id=partner, device_id_type=MESH,
    )
    swap.start()
    swap.wait()

    @pl.loop(0, 16)
    def _(part):
        send_p[part] = (mine[core, part] + other[part]).astype(jnp.bfloat16)

    def plane_copy(step):
        return pltpu.make_async_remote_copy(
            src_ref=send_p.at[above(step)], dst_ref=recv_p.at[step], send_sem=p_send.at[step],
            recv_sem=p_recv.at[step], device_id=device(above(step), z, core), device_id_type=MESH,
        )

    @pl.loop(1, 16)
    def _(step):
        plane_copy(step).start()

    kept = mine[core, place] + other[place]

    @pl.loop(1, 16)
    def _(step):
        plane_copy(step).wait()

    def add_plane(step, value):
        return value + recv_p[step].astype(jnp.float32)

    send_z[...] = lax.fori_loop(1, 16, add_plane, kept).astype(jnp.bfloat16)

    def z_copy(step):
        return pltpu.make_async_remote_copy(
            src_ref=send_z, dst_ref=recv_z.at[step], send_sem=z_send.at[step],
            recv_sem=z_recv.at[step], device_id=z_peer(step), device_id_type=MESH,
        )

    @pl.loop(1, 8)
    def _(step):
        z_copy(step).start()

    recv_z[0] = send_z[...]

    @pl.loop(1, 8)
    def _(step):
        z_copy(step).wait()

    def add_z(of_z, value):
        step = lax.rem(z - of_z + 8, 8)
        return value + recv_z[step].astype(jnp.float32)

    total[core, place] = lax.fori_loop(0, 8, add_z, jnp.zeros_like(kept))

    def plane_back(step):
        return pltpu.make_async_remote_copy(
            src_ref=total.at[core, place], dst_ref=total.at[core, place], send_sem=g_send.at[step],
            recv_sem=g_recv.at[step], device_id=device(above(step), z, core), device_id_type=MESH,
        )

    def hand_on(step):
        return pltpu.make_async_remote_copy(
            src_ref=total.at[core, below(step)], dst_ref=total.at[core, below(step)],
            send_sem=h_send.at[step], recv_sem=h_recv.at[step], device_id=partner,
            device_id_type=MESH,
        )

    @pl.loop(1, 16)
    def _(step):
        plane_back(step).start()

    hand_on(0).start()

    @pl.loop(1, 16)
    def _(step):
        plane_back(step).wait()
        hand_on(step).start()

    @pl.loop(0, 16)
    def _(step):
        hand_on(step).wait()


def sum_all(packed):
    vmem = pl.BlockSpec(memory_space=pltpu.VMEM)
    dma = pltpu.SemaphoreType.DMA
    return pl.pallas_call(
        sum_kernel,
        out_shape=jax.ShapeDtypeStruct((2, 16, PIECE, 128), jnp.float32),
        in_specs=[vmem],
        out_specs=vmem,
        scratch_shapes=[
            pltpu.VMEM((16, PIECE, 128), jnp.float32),
            pltpu.VMEM((16, PIECE, 128), jnp.bfloat16),
            pltpu.VMEM((16, PIECE, 128), jnp.bfloat16),
            pltpu.VMEM((PIECE, 128), jnp.bfloat16),
            pltpu.VMEM((8, PIECE, 128), jnp.bfloat16),
            dma, dma, dma((16,)), dma((16,)), dma((8,)), dma((8,)),
            dma((16,)), dma((16,)), dma((16,)), dma((16,)),
        ],
        compiler_params=pltpu.CompilerParams(
            collective_id=1, has_side_effects=True, vmem_limit_bytes=SMALL_VMEM_LIMIT
        ),
        name="sum_all",
    )(packed)


def shards(
    features,
    partition_map,
    seed_ids,
    hop1_ids,
    hop2_ids,
    labels,
    self_one,
    neigh_one,
    bias_one,
    self_two,
    neigh_two,
    bias_two,
):
    ids = jnp.concatenate(
        [
            seed_ids[None, :],
            hop1_ids.T,
            hop2_ids.transpose(2, 1, 0).reshape(FAN2 * FAN1, SEEDS),
        ],
        axis=0,
    )
    place, returned, hubs = fetch(ids, partition_map, features)
    hubs = hubs.reshape(OWNERS * HOT_DEV, 128)
    seed_loss, packed = sage(
        place, returned, hubs, labels, self_one, neigh_one, bias_one, self_two, neigh_two, bias_two
    )
    total = sum_all(packed.reshape(2, 16, PIECE, 128))
    return (seed_loss, *unpack(total.reshape(ROWS, 128)))


def solution(mesh):
    return jax.shard_map(
        shards,
        mesh=mesh,
        in_specs=(
            P("dom", None),
            P(),
            P(("dom", "rep")),
            P(("dom", "rep"), None),
            P(("dom", "rep"), None, None),
            P(("dom", "rep")),
            P(),
            P(),
            P(),
            P(),
            P(),
            P(),
        ),
        out_specs=(P(("dom", "rep")), P(), P(), P(), P(), P(), P()),
        check_vma=False,
    )
```
